32 devices in a mesh: dp: 1 (over z), tp: 4 (over y), sp: 8 (over x, core).
Axes of the slice: x: 4, y: 4, z: 1, core: 2. Of those that a mesh axis runs over, the one named last changes fastest.
The devices are a block of a 4x4x8 slice.
Arguments:
- encoded: bfloat16 [64, 256, 1536], P('dp', 'sp')
- enc_gain: float32 [1536], replicated
- enc_bias: float32 [1536], replicated
- probe: float32 [1536], replicated
- w_query: bfloat16 [1536, 16, 96], P(None, 'tp')
- b_query: float32 [16, 96], P('tp')
- w_key: bfloat16 [1536, 16, 96], P(None, 'tp')
- w_value: bfloat16 [1536, 16, 96], P(None, 'tp')
- b_value: float32 [16, 96], P('tp')
- w_out: bfloat16 [16, 96, 1536], P('tp')
- b_out: float32 [1536], replicated
- head_gain: float32 [1536], replicated
- head_bias: float32 [1536], replicated
- w_up: bfloat16 [1536, 6144], P(None, 'tp')
- b_up: float32 [6144], P('tp')
- w_down: bfloat16 [6144, 1536], P('tp')
- b_down: float32 [1536], replicated
- out_grad: bfloat16 [64, 1536], P('dp')
Outputs:
- output 1: bfloat16 [64, 1536], P('dp')
- output 2: bfloat16 [64, 256, 1536], P('dp', 'sp')
- output 3: float32 [1536], P('dp')
- output 4: float32 [1536, 16, 96], P('dp', 'tp')
- output 5: float32 [1536, 16, 96], P('dp', 'tp')
- output 6: float32 [1536, 16, 96], P('dp', 'tp')
- output 7: float32 [16, 96, 1536], P(('dp', 'tp'))
- output 8: float32 [1536, 6144], P('dp', 'tp')
- output 9: float32 [6144, 1536], P(('dp', 'tp'))
All inputs are finite; a program needn't handle non-finite values.
Results may differ from the reference program's by a relative error of at most 0.0186865.
Values sent between devices are 32-bit elements.
A program may use at most 768 MiB of HBM per device.

```python
import jax
import jax.numpy as jnp
from jax import lax

IMAGES = 64
TOKENS = 256
MODEL_WIDTH = 1536
NUM_HEADS = 16
MLP_WIDTH = 6144
HEAD_DIM = MODEL_WIDTH // NUM_HEADS
NORM_EPS = 1e-6


def normal_weight(key_in, shape_in, fan_in):
    return (jax.random.normal(key_in, shape_in, jnp.float32) * fan_in ** -0.5).astype(jnp.bfloat16)


def normal_vector(key_in, shape_in, center, spread):
    return center + spread * jax.random.normal(key_in, shape_in, jnp.float32)


def setup_inputs(seed: int = 0, part: int = 0) -> dict:
    base_key = jax.random.key(seed)
    shared_keys = jax.random.split(base_key, 16)
    part_keys = jax.random.split(jax.random.fold_in(base_key, part), 4)
    head_shape = (MODEL_WIDTH, NUM_HEADS, HEAD_DIM)
    positions = jnp.linspace(-1.5, 1.5, TOKENS, dtype=jnp.float32)
    token_noise = jax.random.normal(part_keys[0], (IMAGES, TOKENS, MODEL_WIDTH), jnp.float32)
    common = jax.random.normal(part_keys[1], (IMAGES, 1, MODEL_WIDTH), jnp.float32)
    trend_dir = jax.random.normal(part_keys[2], (IMAGES, 1, MODEL_WIDTH), jnp.float32)
    encoded = (token_noise + common + positions[None, :, None] * trend_dir).astype(jnp.bfloat16)
    out_grad = jax.random.normal(part_keys[3], (IMAGES, MODEL_WIDTH), jnp.float32).astype(jnp.bfloat16)
    return {
        'encoded': encoded,
        'enc_gain': normal_vector(shared_keys[0], (MODEL_WIDTH,), 1.0, 0.3),
        'enc_bias': normal_vector(shared_keys[1], (MODEL_WIDTH,), 0.0, 0.5),
        'probe': normal_vector(shared_keys[2], (MODEL_WIDTH,), 0.0, 1.0),
        'w_query': normal_weight(shared_keys[3], head_shape, MODEL_WIDTH),
        'b_query': normal_vector(shared_keys[4], (NUM_HEADS, HEAD_DIM), 0.0, 0.5),
        'w_key': normal_weight(shared_keys[5], head_shape, MODEL_WIDTH),
        'w_value': normal_weight(shared_keys[6], head_shape, MODEL_WIDTH),
        'b_value': normal_vector(shared_keys[7], (NUM_HEADS, HEAD_DIM), 0.0, 0.5),
        'w_out': normal_weight(shared_keys[8], (NUM_HEADS, HEAD_DIM, MODEL_WIDTH), MODEL_WIDTH),
        'b_out': normal_vector(shared_keys[9], (MODEL_WIDTH,), 0.0, 0.5),
        'head_gain': normal_vector(shared_keys[10], (MODEL_WIDTH,), 1.0, 0.3),
        'head_bias': normal_vector(shared_keys[11], (MODEL_WIDTH,), 0.0, 0.5),
        'w_up': normal_weight(shared_keys[12], (MODEL_WIDTH, MLP_WIDTH), MODEL_WIDTH),
        'b_up': normal_vector(shared_keys[13], (MLP_WIDTH,), 0.0, 0.5),
        'w_down': normal_weight(shared_keys[14], (MLP_WIDTH, MODEL_WIDTH), MLP_WIDTH),
        'b_down': normal_vector(shared_keys[15], (MODEL_WIDTH,), 0.0, 0.5),
        'out_grad': out_grad,
    }


def layer_norm(rows_in, norm_gain, norm_bias):
    row_mean = jnp.mean(rows_in, axis=-1, keepdims=True)
    centred = rows_in - row_mean
    inv_std = lax.rsqrt(jnp.mean(centred * centred, axis=-1, keepdims=True) + NORM_EPS)
    return centred * inv_std * norm_gain + norm_bias


def keep_exact(array_in):
    return array_in


def store_bf16(array_in):
    return array_in.astype(jnp.bfloat16).astype(jnp.float32)


def head_forward(store, encoded, enc_gain, enc_bias, probe, w_query, b_query, w_key, w_value, b_value, w_out, b_out, head_gain, head_bias, w_up, b_up, w_down, b_down):
    normed = store(layer_norm(encoded, enc_gain, enc_bias))
    query_heads = store(jnp.einsum('w,whd->hd', store(probe), w_query) + b_query)
    key_heads = store(jnp.einsum('bnw,whd->bnhd', normed, w_key))
    value_heads = store(jnp.einsum('bnw,whd->bnhd', normed, w_value) + b_value)
    scores = jnp.einsum('bnhd,hd->bhn', key_heads, query_heads) * HEAD_DIM ** -0.5
    weights = jax.nn.softmax(scores, axis=-1)
    pooled_heads = store(jnp.einsum('bhn,bnhd->bhd', weights, value_heads))
    attn_out = jnp.einsum('bhd,hdw->bw', pooled_heads, w_out) + b_out
    normed_out = store(layer_norm(attn_out, head_gain, head_bias))
    hidden = store(jax.nn.gelu(jnp.dot(normed_out, w_up) + b_up, approximate=True))
    return attn_out + jnp.dot(hidden, w_down) + b_down


def reference(encoded, enc_gain, enc_bias, probe, w_query, b_query, w_key, w_value, b_value, w_out, b_out, head_gain, head_bias, w_up, b_up, w_down, b_down, out_grad):
    exact_args = [array_in.astype(jnp.float32) for array_in in (encoded, enc_gain, enc_bias, probe, w_query, b_query, w_key, w_value, b_value, w_out, b_out, head_gain, head_bias, w_up, b_up, w_down, b_down)]
    pooled = head_forward(store_bf16, *exact_args).astype(jnp.bfloat16)

    def grad_target(enc_in, probe_in, query_in, key_in, value_in, out_in, up_in, down_in):
        return head_forward(keep_exact, enc_in, exact_args[1], exact_args[2], probe_in, query_in, exact_args[5], key_in, value_in, exact_args[8], out_in, exact_args[10], exact_args[11], exact_args[12], up_in, exact_args[14], down_in, exact_args[16])

    pull_back = jax.vjp(grad_target, exact_args[0], exact_args[3], exact_args[4], exact_args[6], exact_args[7], exact_args[9], exact_args[13], exact_args[15])[1]
    grad_list = pull_back(out_grad.astype(jnp.float32))
    return (pooled, grad_list[0].astype(jnp.bfloat16), grad_list[1], grad_list[2], grad_list[3], grad_list[4], grad_list[5], grad_list[6], grad_list[7])
```

```python
import functools
import jax
import jax.numpy as jnp
from jax import lax
from jax.experimental import pallas as pl
from jax.experimental.pallas import tpu as pltpu
from jax.sharding import PartitionSpec as P

NORM_EPS = 1e-6
MESH = pl.DeviceIdType.MESH
F32, BF16 = jnp.float32, jnp.bfloat16
IN_SPECS = (P('dp', 'sp', None), P(), P(), P(), P(None, 'tp', None), P('tp', None), P(None, 'tp', None), P(None, 'tp', None), P('tp', None), P('tp', None, None), P(), P(), P(), P(None, 'tp'), P('tp'), P('tp', None), P(), P('dp', None))
OUT_SPECS = (P('dp', None), P('dp', 'sp', None), P('dp'), P('dp', 'tp', None), P('dp', 'tp', None), P('dp', 'tp', None), P(('dp', 'tp'), None, None), P('dp', 'tp'), P(('dp', 'tp'), None))
LANES = 128
SUB = 8
GELU_C = 0.7978845608028654
GELU_A = 0.044715


def nn(a, b):
    return lax.dot_general(a, b, (((1,), (0,)), ((), ())), preferred_element_type=F32)


def nt(a, b):
    return lax.dot_general(a, b, (((1,), (1,)), ((), ())), preferred_element_type=F32)


def tn(a, b):
    return lax.dot_general(a, b, (((0,), (0,)), ((), ())), preferred_element_type=F32)


def hi_lo(a):
    hi = a.astype(BF16)
    return hi, (a - hi.astype(F32)).astype(BF16)


def iota(shape, dim):
    return lax.broadcasted_iota(jnp.int32, shape, dim)


def by_head(parts, width):
    rows, cols = parts[0].shape[0], len(parts) * width
    block = iota((rows, cols), 1) // width
    out = jnp.zeros((rows, cols), F32)
    for h, part in enumerate(parts):
        out = jnp.where(block == h, part, out)
    return out


def gelu_parts(pre):
    t = jnp.tanh(GELU_C * (pre + GELU_A * pre * pre * pre))
    value = 0.5 * pre * (1.0 + t)
    slope = 0.5 * (1.0 + t) + 0.5 * pre * (1.0 - t * t) * (GELU_C * (1.0 + 3.0 * GELU_A * pre * pre))
    return value, slope


def centre(rows):
    mean = jnp.mean(rows, axis=-1, keepdims=True)
    centred = rows - mean
    inv = lax.rsqrt(jnp.mean(centred * centred, axis=-1, keepdims=True) + NORM_EPS)
    return centred * inv, inv


def norm_back(hat, inv, cot):
    return inv * (cot - jnp.mean(cot, axis=-1, keepdims=True) - hat * jnp.mean(cot * hat, axis=-1, keepdims=True))


def barrier_all(peers):
    sem = pltpu.get_barrier_semaphore()
    for axis, dev in peers:
        pl.semaphore_signal(sem, inc=1, device_id={axis: dev}, device_id_type=MESH)
    pl.semaphore_wait(sem, len(peers))


def peers_of(axis, n):
    me = lax.axis_index(axis)
    return me, [lax.rem(me + k, n) for k in range(1, n)]


def remote(src, dst, send_sem, recv_sem, axis, dev):
    return pltpu.make_async_remote_copy(src_ref=src, dst_ref=dst, send_sem=send_sem, recv_sem=recv_sem, device_id={axis: dev}, device_id_type=MESH)


def gather_start(buf, me, peers, send_sems, recv_sems, axis):
    for k, dev in enumerate(peers):
        remote(buf.at[me], buf.at[me], send_sems.at[k], recv_sems.at[me], axis, dev).start()


def gather_wait(buf, me, peers, send_sems, recv_sems, axis):
    for k, dev in enumerate(peers):
        remote(buf.at[dev], buf.at[dev], send_sems.at[k], recv_sems.at[dev], axis, dev).wait_recv()
    for k, dev in enumerate(peers):
        remote(buf.at[me], buf.at[me], send_sems.at[k], recv_sems.at[me], axis, dev).wait_send()


def scan_kernel(heads, scale, x_ref, gain_ref, bias_ref, probe_ref, wq_ref, bq_ref, wk_ref, wv_ref, bv_ref, pk_ref, hb_ref, qk_ref, q_ref, qkr):
    rows = heads * SUB
    width = wq_ref.shape[0] // heads

    @pl.when(pl.program_id(0) == 0)
    def _():
        probe8 = jnp.broadcast_to(probe_ref[...].astype(BF16), (SUB, probe_ref.shape[1]))
        q8 = (nt(probe8, wq_ref[...]) + bq_ref[...]).astype(BF16)
        q_ref[...] = q8.astype(F32)
        qs = jnp.concatenate([q8.astype(F32)] * heads, axis=0)
        qs = jnp.where(iota(qs.shape, 0) // SUB == iota(qs.shape, 1) // width, qs, 0.0).astype(BF16)
        qk = nn(qs, wk_ref[...])
        hi, lo = hi_lo(qk)
        qkr[...] = jnp.zeros(qkr.shape, BF16)
        qkr[0:rows, :] = hi
        qkr[LANES // 2:LANES // 2 + rows, :] = lo
        for h in range(heads):
            qk_ref[h:h + 1, :] = qk[SUB * h:SUB * h + 1, :]

    images, tokens = SUB, x_ref.shape[0] // SUB
    hat, _ = centre(x_ref[...].astype(F32))
    hid = (hat * gain_ref[...] + bias_ref[...]).astype(BF16)
    r = nt(hid, qkr[...])
    s = ((r + pltpu.roll(r, LANES // 2, 1)) * scale).reshape(images, tokens, LANES)
    m = jnp.max(s, axis=1)
    e = jnp.exp(s - m[:, None, :])
    l = jnp.sum(e, axis=1)
    lane, img = iota(e.shape, 2), iota(e.shape, 0)
    ebd = jnp.where((lane % SUB == img) & (lane < rows), e, 0.0).astype(BF16).reshape(images * tokens, LANES)
    hb = tn(ebd, hid)[0:rows, :]
    hb_ref[0, :, :] = hb
    hi, lo = hi_lo(hb)
    v = nt(jnp.concatenate([hi, lo], axis=0), wv_ref[...])
    v = v[0:rows] + v[rows:2 * rows]
    cols = wq_ref.shape[0]
    vs = by_head([v[SUB * h:SUB * h + SUB] for h in range(heads)], width)
    vs = vs + by_head([l[:, SUB * h:SUB * h + 1] for h in range(heads)], width) * bv_ref[...]
    pk_ref[:, 0:cols] = vs
    pk_ref[:, cols:cols + LANES] = m
    pk_ref[:, cols + LANES:cols + 2 * LANES] = l


def scan_tokens(heads, images, scale, x, gain, bias, probe, wq, bq, wk, wv, bv):
    tokens_all, width = x.shape
    hd = wq.shape[0]
    groups = images // SUB
    block = tokens_all // groups
    full = lambda a: pl.BlockSpec(a.shape, lambda g: (0,) * a.ndim)
    return pl.pallas_call(
        functools.partial(scan_kernel, heads, scale),
        grid=(groups,),
        in_specs=[pl.BlockSpec((block, width), lambda g: (g, 0))] + [full(a) for a in (gain, bias, probe, wq, bq, wk, wv, bv)],
        out_specs=[pl.BlockSpec((SUB, hd + 2 * LANES), lambda g: (g, 0)), pl.BlockSpec((1, heads * SUB, width), lambda g: (g, 0, 0)), pl.BlockSpec((heads, width), lambda g: (0, 0)), pl.BlockSpec((SUB, hd), lambda g: (0, 0))],
        out_shape=[jax.ShapeDtypeStruct((images, hd + 2 * LANES), F32), jax.ShapeDtypeStruct((groups, heads * SUB, width), F32), jax.ShapeDtypeStruct((heads, width), F32), jax.ShapeDtypeStruct((SUB, hd), F32)],
        scratch_shapes=[pltpu.VMEM((LANES, width), BF16)],
        cost_estimate=pl.CostEstimate(flops=2 * tokens_all * width * 3 * LANES, bytes_accessed=tokens_all * width * 2, transcendentals=0),
        name='scan_tokens',
    )(x, gain, bias, probe, wq, bq, wk, wv, bv)


def head_kernel(heads, nsp, ntp, pk_ref, wo_hbm, wu_hbm, wd_hbm, og_ref, bo_ref, hg_ref, hb_ref, bu_ref, bd_ref, bv_ref,
                y_out, ga_out, pool_out, pb_out, st_out,
                wo, wu, wd, rbuf, ta, tg, td, ag, wsem, rs_send, rs_recv, ta_s, ta_r, tg_s, tg_r, td_s, td_r, ag_s, ag_r):
    sp, sp_peers = peers_of('sp', nsp)
    tp, tp_peers = peers_of('tp', ntp)
    loads = [pltpu.make_async_copy(a, b, wsem.at[i]) for i, (a, b) in enumerate(((wd_hbm, wd), (wo_hbm, wo), (wu_hbm, wu)))]
    for load in loads:
        load.start()
    barrier_all([('sp', d) for d in sp_peers] + [('tp', d) for d in tp_peers])
    sends = []
    for k, dev in enumerate(sp_peers):
        sends.append(remote(pk_ref.at[dev], rbuf.at[sp], rs_send.at[k], rs_recv.at[sp], 'sp', dev))
        sends[-1].start()
    rbuf[sp] = pk_ref[sp]
    hd = wo.shape[0]
    width = hd // heads
    model = wu.shape[0]
    og = og_ref[sp]
    loads[0].wait()
    gh = nt(og, wd[...])
    for k, dev in enumerate(sp_peers):
        remote(rbuf.at[dev], rbuf.at[dev], rs_send.at[k], rs_recv.at[dev], 'sp', dev).wait_recv()
    for send in sends:
        send.wait_send()
    m = rbuf[0, :, hd:hd + LANES]
    for j in range(1, nsp):
        m = jnp.maximum(m, rbuf[j, :, hd:hd + LANES])
    l = jnp.zeros_like(m)
    v = jnp.zeros((SUB, hd), F32)
    for j in range(nsp):
        w = jnp.exp(rbuf[j, :, hd:hd + LANES] - m)
        l = l + w * rbuf[j, :, hd + LANES:hd + 2 * LANES]
        v = v + by_head([w[:, SUB * h:SUB * h + 1] for h in range(heads)], width) * rbuf[j, :, 0:hd]
    o = v / by_head([l[:, SUB * h:SUB * h + 1] for h in range(heads)], width)
    pooled_bf = o.astype(BF16)
    lse = m + jnp.log(l)
    loads[1].wait()
    ta[tp] = nn(pooled_bf, wo[...])
    gather_start(ta, tp, tp_peers, ta_s, ta_r, 'tp')
    loads[2].wait()
    gather_wait(ta, tp, tp_peers, ta_s, ta_r, 'tp')
    attn = bo_ref[...] + ((ta[0] + ta[1]) + (ta[2] + ta[3])) if ntp == 4 else bo_ref[...] + sum(ta[t] for t in range(ntp))
    hat, inv = centre(attn)
    y = (hat * hg_ref[...] + hb_ref[...]).astype(BF16)
    value, slope = gelu_parts(nn(y, wu[...]) + bu_ref[...])
    hidden = value.astype(BF16)
    tg[tp] = nt((gh * slope).astype(BF16), wu[...])
    gather_start(tg, tp, tp_peers, tg_s, tg_r, 'tp')
    td[tp] = nn(hidden, wd[...])
    gather_start(td, tp, tp_peers, td_s, td_r, 'tp')
    gather_wait(tg, tp, tp_peers, tg_s, tg_r, 'tp')
    gno = tg[0]
    for t in range(1, ntp):
        gno = gno + tg[t]
    ga = (og.astype(F32) + norm_back(hat, inv, gno * hg_ref[...])).astype(BF16)
    gp = nt(ga, wo[...]).astype(BF16).astype(F32)
    prod = gp * (o - bv_ref[...])
    head_of = iota(prod.shape, 1) // width
    delta = by_head([jnp.sum(jnp.where(head_of == h, prod, 0.0), axis=1, keepdims=True) for h in range(heads)], SUB)
    gather_wait(td, tp, tp_peers, td_s, td_r, 'tp')
    down = td[0]
    for t in range(1, ntp):
        down = down + td[t]
    ag[sp, :, 0:model] = y.astype(F32)
    ag[sp, :, model:2 * model] = ga.astype(F32)
    ag[sp, :, 2 * model:3 * model] = (attn + down + bd_ref[...]).astype(BF16).astype(F32)
    base = 3 * model
    ag[sp, :, base:base + hd] = pooled_bf.astype(F32)
    ag[sp, :, base + hd:base + hd + LANES] = lse
    ag[sp, :, base + hd + LANES:base + hd + 2 * LANES] = jnp.concatenate([delta, jnp.zeros((SUB, LANES - heads * SUB), F32)], axis=1)
    gather_start(ag, sp, sp_peers, ag_s, ag_r, 'sp')
    gather_wait(ag, sp, sp_peers, ag_s, ag_r, 'sp')
    y_out[...] = ag[:, :, 0:model].astype(BF16)
    ga_out[...] = ag[:, :, model:2 * model].astype(BF16)
    pool_out[...] = ag[:, :, 2 * model:3 * model].astype(BF16)
    pb_out[...] = ag[:, :, base:base + hd].astype(BF16)
    st_out[...] = ag[:, :, base + hd:base + hd + 2 * LANES]


def head(heads, nsp, ntp, pk, wo, wu, wd, og, bo, hg, hb, bu, bd, bv):
    images, model = og.shape
    hd = wo.shape[0]
    own = images // nsp
    pk3 = pk.reshape(nsp, own, pk.shape[1])
    og3 = og.reshape(nsp, own, model)
    vm, hbm = pl.BlockSpec(memory_space=pltpu.VMEM), pl.BlockSpec(memory_space=pl.ANY)
    dma = pltpu.SemaphoreType.DMA
    cols = 3 * model + hd + 2 * LANES
    part = pltpu.VMEM((ntp, own, model), F32)
    shapes = [(model, BF16), (model, BF16), (model, BF16), (hd, BF16), (2 * LANES, F32)]
    return pl.pallas_call(
        functools.partial(head_kernel, heads, nsp, ntp),
        in_specs=[vm, hbm, hbm, hbm] + [vm] * 7,
        out_specs=[vm] * 5,
        out_shape=[jax.ShapeDtypeStruct((nsp, own, c), d) for c, d in shapes],
        scratch_shapes=[pltpu.VMEM(wo.shape, BF16), pltpu.VMEM(wu.shape, BF16), pltpu.VMEM(wd.shape, BF16), pltpu.VMEM(pk3.shape, F32), part, part, part, pltpu.VMEM((nsp, own, cols), F32),
                        dma((3,)), dma((nsp - 1,)), dma((nsp,)), dma((ntp - 1,)), dma((ntp,)), dma((ntp - 1,)), dma((ntp,)), dma((ntp - 1,)), dma((ntp,)), dma((nsp - 1,)), dma((nsp,))],
        compiler_params=pltpu.CompilerParams(collective_id=0, has_side_effects=True),
        name='head',
    )(pk3, wo, wu, wd, og3, bo, hg, hb, bu, bd, bv)


def spread_kernel(heads, nsp, ntp, ga_ref, wo_ref, wv_ref, hb_ref, pk_ref, st_ref, qk_ref,
                  gv_out, hbar_out, st_out, qk_out,
                  hs, hr, ha, gv_s, gv_r, fw_s, fw_r, hs_s, hs_r, ha_s, ha_r, st_s, st_r, qk_s, qk_r):
    sp, sp_peers = peers_of('sp', nsp)
    tp, tp_peers = peers_of('tp', ntp)
    core = lax.rem(sp, 2)
    mate = sp + 1 - 2 * core
    half = nsp // 2
    hd = wo_ref.shape[0]
    width = hd // heads
    model = wo_ref.shape[1]
    rows = heads * SUB

    def make_gv(i, _):
        g = lax.rem(core * half + i, nsp)
        gp = nt(ga_ref[g], wo_ref[...]).astype(BF16).astype(F32)
        gp = jnp.concatenate([gp] * heads, axis=0)
        gp = jnp.where(iota(gp.shape, 0) // SUB == iota(gp.shape, 1) // width, gp, 0.0).astype(BF16)
        gv_out[tp, g] = nn(gp, wv_ref[...])
        return 0

    lax.fori_loop(0, half, make_gv, 0)

    def make_hs(g, _):
        w = jnp.exp(pk_ref[g, :, hd:hd + LANES] - st_ref[g, :, 0:LANES])
        col = jnp.concatenate([w[:, SUB * h:SUB * h + 1] for h in range(heads)], axis=0)
        hs[g] = hb_ref[g] * col
        return 0

    lax.fori_loop(0, nsp, make_hs, 0)
    st_out[tp] = st_ref[...]
    qk_out[tp] = qk_ref[...]
    barrier_all([('sp', d) for d in sp_peers] + [('tp', d) for d in tp_peers])
    for i in range(half):
        g = core * half + i
        for k, dev in enumerate(tp_peers):
            remote(gv_out.at[tp, g], gv_out.at[tp, g], gv_s.at[k, i], gv_r.at[tp, i], 'tp', dev).start()
    for k, dev in enumerate(sp_peers):
        remote(hs.at[dev], hr.at[sp], hs_s.at[k], hs_r.at[sp], 'sp', dev).start()
    gather_start(st_out, tp, tp_peers, st_s, st_r, 'tp')
    gather_start(qk_out, tp, tp_peers, qk_s, qk_r, 'tp')
    lax.fori_loop(half, nsp, make_gv, 0)
    for k, dev in enumerate(sp_peers):
        remote(hr.at[dev], hr.at[dev], hs_s.at[k], hs_r.at[dev], 'sp', dev).wait_recv()
    for k, dev in enumerate(sp_peers):
        remote(hs.at[dev], hr.at[sp], hs_s.at[k], hs_r.at[sp], 'sp', dev).wait_send()
    hr[sp] = hs[sp]
    total = hr[0]
    for j in range(1, nsp):
        total = total + hr[j]
    ha[sp] = total
    gather_start(ha, sp, sp_peers, ha_s, ha_r, 'sp')
    for i in range(half):
        g = core * half + i
        for k, dev in enumerate(tp_peers):
            remote(gv_out.at[dev, g], gv_out.at[dev, g], gv_s.at[k, i], gv_r.at[dev, i], 'tp', dev).wait_recv()
            remote(gv_out.at[dev, g], gv_out.at[dev, g], fw_s.at[k, i], fw_r.at[dev, i], 'sp', mate).start()
    for i in range(half):
        g = core * half + i
        other = (1 - core) * half + i
        for k, dev in enumerate(tp_peers):
            remote(gv_out.at[tp, g], gv_out.at[tp, g], gv_s.at[k, i], gv_r.at[tp, i], 'tp', dev).wait_send()
            remote(gv_out.at[dev, g], gv_out.at[dev, g], fw_s.at[k, i], fw_r.at[dev, i], 'sp', mate).wait_send()
            remote(gv_out.at[dev, other], gv_out.at[dev, other], fw_s.at[k, i], fw_r.at[dev, i], 'sp', mate).wait_recv()
    gather_wait(st_out, tp, tp_peers, st_s, st_r, 'tp')
    gather_wait(qk_out, tp, tp_peers, qk_s, qk_r, 'tp')
    gather_wait(ha, sp, sp_peers, ha_s, ha_r, 'sp')
    hbar_out[...] = ha[...].astype(BF16)


def spread(heads, nsp, ntp, ga3, wo, wv, hb, pk, st, qk):
    groups, rows, model = hb.shape
    vm = pl.BlockSpec(memory_space=pltpu.VMEM)
    dma = pltpu.SemaphoreType.DMA
    half = nsp // 2
    pk3 = pk.reshape(nsp, -1, pk.shape[1])
    slots = pltpu.VMEM((nsp, rows, model), F32)
    return pl.pallas_call(
        functools.partial(spread_kernel, heads, nsp, ntp),
        in_specs=[vm] * 7,
        out_specs=[vm] * 4,
        out_shape=[jax.ShapeDtypeStruct((ntp, nsp, rows, model), F32), jax.ShapeDtypeStruct((nsp, rows, model), BF16), jax.ShapeDtypeStruct((ntp,) + st.shape, F32), jax.ShapeDtypeStruct((ntp,) + qk.shape, F32)],
        scratch_shapes=[slots, slots, slots, dma((ntp - 1, half)), dma((ntp, half)), dma((ntp - 1, half)), dma((ntp, half)), dma((nsp - 1,)), dma((nsp,)), dma((nsp - 1,)), dma((nsp,)), dma((ntp - 1,)), dma((ntp,)), dma((ntp - 1,)), dma((ntp,))],
        compiler_params=pltpu.CompilerParams(collective_id=1, has_side_effects=True),
        name='spread',
    )(ga3, wo, wv, hb, pk3, st, qk)


def back_kernel(heads, ntp, scale, x_ref, gain_ref, bias_ref, gv_ref, qk_ref, st_ref, gx_ref, u_ref, qkr, uacc):
    step = pl.program_id(0)
    rows = heads * SUB
    model = x_ref.shape[1]

    @pl.when(step == 0)
    def _():
        for t in range(ntp):
            for h in range(heads):
                hi, lo = hi_lo(jnp.broadcast_to(qk_ref[t, h:h + 1, :], (SUB, model)))
                at = (t * heads + h) * SUB
                qkr[at:at + SUB, :] = hi.astype(F32)
                qkr[LANES + at:LANES + at + SUB, :] = lo.astype(F32)
        uacc[...] = jnp.zeros(uacc.shape, F32)

    images, tokens = SUB, x_ref.shape[0] // SUB
    hat, inv = centre(x_ref[...].astype(F32))
    gain = gain_ref[...]
    hid = (hat * gain + bias_ref[...]).astype(BF16)
    qkb = qkr[...].astype(BF16)
    gv_hi, gv_lo = hi_lo(gv_ref[...].reshape(ntp * rows, model))
    r = nt(hid, qkb)
    s = (r[:, 0:LANES] + r[:, LANES:2 * LANES]) * scale
    d = nt(hid, jnp.concatenate([gv_hi, gv_lo], axis=0))
    d = d[:, 0:LANES] + d[:, LANES:2 * LANES]
    lse = jnp.concatenate([st_ref[t, 0, :, 0:rows] for t in range(ntp)], axis=1)
    delta = jnp.concatenate([st_ref[t, 0, :, LANES:LANES + rows] for t in range(ntp)], axis=1)
    shape = (images, tokens, LANES)
    keep = iota(shape, 2) % SUB == iota(shape, 0)
    p = jnp.where(keep, jnp.exp(s.reshape(shape) - lse[:, None, :]), 0.0)
    ds = p * (d.reshape(shape) - delta[:, None, :]) * scale
    pb = p.astype(BF16).reshape(images * tokens, LANES)
    db = ds.astype(BF16).reshape(images * tokens, LANES)
    gh = nn(jnp.concatenate([pb, db], axis=1), jnp.concatenate([gv_hi, qkb[0:LANES]], axis=0))
    uacc[...] += tn(db, hid)
    gx_ref[...] = norm_back(hat, inv, gh * gain).astype(BF16)

    @pl.when(step == pl.num_programs(0) - 1)
    def _():
        tp = lax.axis_index('tp')
        for h in range(heads):
            mine = uacc[pl.ds(pl.multiple_of(tp * rows + h * SUB, SUB), SUB), :]
            u_ref[h:h + 1, :] = jnp.sum(mine, axis=0, keepdims=True)


def back_tokens(heads, ntp, scale, x, gain, bias, gv, qk, st):
    tokens_all, model = x.shape
    groups, rows = gv.shape[1], gv.shape[2]
    block = tokens_all // groups
    full = lambda a: pl.BlockSpec(a.shape, lambda g: (0,) * a.ndim)
    return pl.pallas_call(
        functools.partial(back_kernel, heads, ntp, scale),
        grid=(groups,),
        in_specs=[pl.BlockSpec((block, model), lambda g: (g, 0)), full(gain), full(bias), pl.BlockSpec((ntp, 1, rows, model), lambda g: (0, g, 0, 0)), full(qk), pl.BlockSpec((ntp, 1) + st.shape[2:], lambda g: (0, g, 0, 0))],
        out_specs=[pl.BlockSpec((block, model), lambda g: (g, 0)), pl.BlockSpec((heads, model), lambda g: (0, 0))],
        out_shape=[jax.ShapeDtypeStruct((tokens_all, model), BF16), jax.ShapeDtypeStruct((heads, model), F32)],
        scratch_shapes=[pltpu.VMEM((2 * LANES, model), F32), pltpu.VMEM((LANES, model), F32)],
        name='back_tokens',
    )(x, gain, bias, gv, qk, st)


def query_kernel(heads, nsp, ntp, u_ref, q_ref, probe_ref, wq_ref, wk_ref, gwq_out, gwk_out, gpr_out, ub, pb, u_s, u_r, p_s, p_r):
    sp, sp_peers = peers_of('sp', nsp)
    tp, tp_peers = peers_of('tp', ntp)
    ub[sp] = u_ref[...]
    barrier_all([('sp', d) for d in sp_peers] + [('tp', d) for d in tp_peers])
    gather_start(ub, sp, sp_peers, u_s, u_r, 'sp')
    gather_wait(ub, sp, sp_peers, u_s, u_r, 'sp')
    u = ub[0]
    for j in range(1, nsp):
        u = u + ub[j]
    hd = wk_ref.shape[0]
    width = hd // heads
    hi, lo = hi_lo(u)
    g = nt(jnp.concatenate([hi, lo], axis=0), wk_ref[...])
    g = g[0:heads] + g[heads:2 * heads]
    gq = jnp.sum(jnp.where(iota(g.shape, 0) == iota(g.shape, 1) // width, g, 0.0), axis=0, keepdims=True)
    hi, lo = hi_lo(gq)
    gpr = nn(jnp.concatenate([hi, lo], axis=0), wq_ref[...])
    pb[tp] = gpr[0:1] + gpr[1:2]
    gather_start(pb, tp, tp_peers, p_s, p_r, 'tp')
    qcol = jnp.transpose(q_ref[...])[:, 0:1]
    gcol = jnp.transpose(jnp.broadcast_to(gq, (SUB, hd)))[:, 0:1]
    for h in range(heads):
        at = slice(width * h, width * h + width)
        gwk_out[at, :] = qcol[at, :] * u[h:h + 1, :]
        gwq_out[at, :] = gcol[at, :] * probe_ref[...]
    gather_wait(pb, tp, tp_peers, p_s, p_r, 'tp')
    total = pb[0]
    for t in range(1, ntp):
        total = total + pb[t]
    gpr_out[...] = total


def query_grads(heads, nsp, ntp, u, q, probe, wq, wk):
    hd, model = wq.shape
    vm = pl.BlockSpec(memory_space=pltpu.VMEM)
    dma = pltpu.SemaphoreType.DMA
    return pl.pallas_call(
        functools.partial(query_kernel, heads, nsp, ntp),
        in_specs=[vm] * 5,
        out_specs=[vm] * 3,
        out_shape=[jax.ShapeDtypeStruct((hd, model), F32), jax.ShapeDtypeStruct((hd, model), F32), jax.ShapeDtypeStruct((1, model), F32)],
        scratch_shapes=[pltpu.VMEM((nsp, heads, model), F32), pltpu.VMEM((ntp, 1, model), F32), dma((nsp - 1,)), dma((nsp,)), dma((ntp - 1,)), dma((ntp,))],
        compiler_params=pltpu.CompilerParams(collective_id=2, has_side_effects=True),
        name='query_grads',
    )(u, q, probe, wq, wk)


def local_head(nsp, ntp, encoded, enc_gain, enc_bias, probe, w_query, b_query, w_key, w_value, b_value, w_out, b_out, head_gain, head_bias, w_up, b_up, w_down, b_down, out_grad):
    images, tokens, model = encoded.shape
    heads, head_dim = b_query.shape
    hd = heads * head_dim
    scale = head_dim ** -0.5
    x = encoded.reshape(images * tokens, model)
    wq, wk, wv = (jnp.transpose(w, (1, 2, 0)).reshape(hd, model) for w in (w_query, w_key, w_value))
    wo = w_out.reshape(hd, model)
    row = lambda a: a.reshape(1, -1)
    bv = row(b_value)
    pk, hb, qk, q8 = scan_tokens(heads, images, scale, x, row(enc_gain), row(enc_bias), row(probe), wq, row(b_query), wk, wv, bv)
    y3, ga3, pool3, pb3, st = head(heads, nsp, ntp, pk, wo, w_up, w_down, out_grad, row(b_out), row(head_gain), row(head_bias), row(b_up), row(b_down), bv)
    gv, hbar, st_all, qk_all = spread(heads, nsp, ntp, ga3, wo, wv, hb, pk, st, qk)
    gx, u = back_tokens(heads, ntp, scale, x, row(enc_gain), row(enc_bias), gv, qk_all, st_all)
    gwq, gwk, gpr = query_grads(heads, nsp, ntp, u, q8, row(probe), wq, wk)

    y, ga, pooled_bf = (a.reshape(images, -1) for a in (y3, ga3, pb3))
    pre = jnp.dot(y, w_up, preferred_element_type=F32) + b_up
    value, slope = gelu_parts(pre)
    grad_w_down = jnp.einsum('bf,bw->fw', value.astype(BF16), out_grad, preferred_element_type=F32)
    grad_hidden = jnp.einsum('bw,fw->bf', out_grad, w_down, preferred_element_type=F32)
    grad_w_up = jnp.einsum('bw,bf->wf', y, (grad_hidden * slope).astype(BF16), preferred_element_type=F32)
    grad_w_out = jnp.einsum('bk,bw->kw', pooled_bf, ga, preferred_element_type=F32).reshape(heads, head_dim, model)
    grad_pooled = jnp.einsum('bw,kw->bk', ga, wo, preferred_element_type=F32).astype(BF16)
    gp5 = grad_pooled.reshape(nsp, images // nsp, heads, head_dim)
    hbar4 = hbar.reshape(nsp, heads, images // nsp, model)
    grad_wv = jnp.einsum('gihd,ghiw->hdw', gp5, hbar4, preferred_element_type=F32)
    back = lambda a: jnp.transpose(a.reshape(heads, head_dim, model), (2, 0, 1))
    return (pool3.reshape(images, model), gx.reshape(encoded.shape), gpr.reshape(model), back(gwq), back(gwk), back(grad_wv), grad_w_out, grad_w_up, grad_w_down)


def solution(mesh):
    body = functools.partial(local_head, mesh.shape['sp'], mesh.shape['tp'])
    return jax.shard_map(body, mesh=mesh, in_specs=IN_SPECS, out_specs=OUT_SPECS, check_vma=False)
```

```python
import functools
import jax
import jax.numpy as jnp
from jax import lax
from jax.experimental import pallas as pl
from jax.experimental.pallas import tpu as pltpu
from jax.sharding import PartitionSpec as P

NORM_EPS = 1e-6
MESH = pl.DeviceIdType.MESH
F32, BF16 = jnp.float32, jnp.bfloat16
IN_SPECS = (P('dp', 'sp', None), P(), P(), P(), P(None, 'tp', None), P('tp', None), P(None, 'tp', None), P(None, 'tp', None), P('tp', None), P('tp', None, None), P(), P(), P(), P(None, 'tp'), P('tp'), P('tp', None), P(), P('dp', None))
OUT_SPECS = (P('dp', None), P('dp', 'sp', None), P('dp'), P('dp', 'tp', None), P('dp', 'tp', None), P('dp', 'tp', None), P(('dp', 'tp'), None, None), P('dp', 'tp'), P(('dp', 'tp'), None))
LANES = 128
SUB = 8
GELU_C = 0.7978845608028654
GELU_A = 0.044715


def nn(a, b):
    return lax.dot_general(a, b, (((1,), (0,)), ((), ())), preferred_element_type=F32)


def nt(a, b):
    return lax.dot_general(a, b, (((1,), (1,)), ((), ())), preferred_element_type=F32)


def tn(a, b):
    return lax.dot_general(a, b, (((0,), (0,)), ((), ())), preferred_element_type=F32)


def hi_lo(a):
    hi = a.astype(BF16)
    return hi, (a - hi.astype(F32)).astype(BF16)


def iota(shape, dim):
    return lax.broadcasted_iota(jnp.int32, shape, dim)


def by_head(parts, width):
    rows, cols = parts[0].shape[0], len(parts) * width
    block = iota((rows, cols), 1) // width
    out = jnp.zeros((rows, cols), F32)
    for h, part in enumerate(parts):
        out = jnp.where(block == h, part, out)
    return out


def row(ref):
    return ref[...].reshape(1, -1)


def flat(ref):
    heads, width = ref.shape
    wide = jnp.concatenate([ref[...]] * heads, axis=1)
    keep = iota(wide.shape, 0) == iota(wide.shape, 1) // width
    return jnp.sum(jnp.where(keep, wide, 0.0), axis=0, keepdims=True)


def gelu_parts(pre):
    t = jnp.tanh(GELU_C * (pre + GELU_A * pre * pre * pre))
    value = 0.5 * pre * (1.0 + t)
    slope = 0.5 * (1.0 + t) + 0.5 * pre * (1.0 - t * t) * (GELU_C * (1.0 + 3.0 * GELU_A * pre * pre))
    return value, slope


def centre(rows):
    mean = jnp.mean(rows, axis=-1, keepdims=True)
    centred = rows - mean
    inv = lax.rsqrt(jnp.mean(centred * centred, axis=-1, keepdims=True) + NORM_EPS)
    return centred * inv, inv


def norm_back(hat, inv, cot):
    return inv * (cot - jnp.mean(cot, axis=-1, keepdims=True) - hat * jnp.mean(cot * hat, axis=-1, keepdims=True))


def barrier_all(peers):
    sem = pltpu.get_barrier_semaphore()
    for axis, dev in peers:
        pl.semaphore_signal(sem, inc=1, device_id={axis: dev}, device_id_type=MESH)
    pl.semaphore_wait(sem, len(peers))


def peers_of(axis, n):
    me = lax.axis_index(axis)
    return me, [lax.rem(me + k, n) for k in range(1, n)]


def remote(src, dst, send_sem, recv_sem, axis, dev):
    return pltpu.make_async_remote_copy(src_ref=src, dst_ref=dst, send_sem=send_sem, recv_sem=recv_sem, device_id={axis: dev}, device_id_type=MESH)


def gather_start(buf, me, peers, send_sems, recv_sems, axis):
    for k, dev in enumerate(peers):
        remote(buf.at[me], buf.at[me], send_sems.at[k], recv_sems.at[me], axis, dev).start()


def gather_wait(buf, me, peers, send_sems, recv_sems, axis):
    for k, dev in enumerate(peers):
        remote(buf.at[dev], buf.at[dev], send_sems.at[k], recv_sems.at[dev], axis, dev).wait_recv()
    for k, dev in enumerate(peers):
        remote(buf.at[me], buf.at[me], send_sems.at[k], recv_sems.at[me], axis, dev).wait_send()


def scan_kernel(heads, scale, x_ref, gain_ref, bias_ref, probe_ref, wq_ref, bq_ref, wk_ref, wv_ref, bv_ref, pk_ref, hb_ref, qk_ref, q_ref, qkr):
    rows = heads * SUB
    width = wq_ref.shape[0] // heads

    @pl.when(pl.program_id(0) == 0)
    def _():
        probe8 = jnp.broadcast_to(row(probe_ref), (SUB, probe_ref.shape[0])).astype(BF16)
        q8 = (nt(probe8, wq_ref[...]) + flat(bq_ref)).astype(BF16)
        q_ref[...] = q8.astype(F32)
        qs = jnp.concatenate([q8.astype(F32)] * heads, axis=0)
        qs = jnp.where(iota(qs.shape, 0) // SUB == iota(qs.shape, 1) // width, qs, 0.0).astype(BF16)
        qk = nn(qs, wk_ref[...])
        hi, lo = hi_lo(qk)
        qkr[...] = jnp.zeros(qkr.shape, BF16)
        qkr[0:rows, :] = hi
        qkr[LANES // 2:LANES // 2 + rows, :] = lo
        for h in range(heads):
            qk_ref[h:h + 1, :] = qk[SUB * h:SUB * h + 1, :]

    images, tokens = SUB, x_ref.shape[0] // SUB
    hat, _ = centre(x_ref[...].astype(F32))
    hid = (hat * row(gain_ref) + row(bias_ref)).astype(BF16)
    r = nt(hid, qkr[...])
    s = ((r + pltpu.roll(r, LANES // 2, 1)) * scale).reshape(images, tokens, LANES)
    m = jnp.max(s, axis=1)
    e = jnp.exp(s - m[:, None, :])
    l = jnp.sum(e, axis=1)
    lane, img = iota(e.shape, 2), iota(e.shape, 0)
    ebd = jnp.where((lane % SUB == img) & (lane < rows), e, 0.0).astype(BF16).reshape(images * tokens, LANES)
    hb = tn(ebd, hid)[0:rows, :]
    hb_ref[0, :, :] = hb
    hi, lo = hi_lo(hb)
    v = nt(jnp.concatenate([hi, lo], axis=0), wv_ref[...])
    v = v[0:rows] + v[rows:2 * rows]
    cols = wq_ref.shape[0]
    vs = by_head([v[SUB * h:SUB * h + SUB] for h in range(heads)], width)
    vs = vs + by_head([l[:, SUB * h:SUB * h + 1] for h in range(heads)], width) * flat(bv_ref)
    pk_ref[:, 0:cols] = vs
    pk_ref[:, cols:cols + LANES] = m
    pk_ref[:, cols + LANES:cols + 2 * LANES] = l


def scan_tokens(heads, images, scale, x, gain, bias, probe, wq, bq, wk, wv, bv):
    tokens_all, width = x.shape
    hd = wq.shape[0]
    groups = images // SUB
    block = tokens_all // groups
    full = lambda a: pl.BlockSpec(a.shape, lambda g: (0,) * a.ndim)
    return pl.pallas_call(
        functools.partial(scan_kernel, heads, scale),
        grid=(groups,),
        in_specs=[pl.BlockSpec((block, width), lambda g: (g, 0))] + [full(a) for a in (gain, bias, probe, wq, bq, wk, wv, bv)],
        out_specs=[pl.BlockSpec((SUB, hd + 2 * LANES), lambda g: (g, 0)), pl.BlockSpec((1, heads * SUB, width), lambda g: (g, 0, 0)), pl.BlockSpec((heads, width), lambda g: (0, 0)), pl.BlockSpec((SUB, hd), lambda g: (0, 0))],
        out_shape=[jax.ShapeDtypeStruct((images, hd + 2 * LANES), F32), jax.ShapeDtypeStruct((groups, heads * SUB, width), F32), jax.ShapeDtypeStruct((heads, width), F32), jax.ShapeDtypeStruct((SUB, hd), F32)],
        scratch_shapes=[pltpu.VMEM((LANES, width), BF16)],
        cost_estimate=pl.CostEstimate(flops=2 * tokens_all * width * 3 * LANES, bytes_accessed=tokens_all * width * 2, transcendentals=0),
        name='scan_tokens',
    )(x, gain, bias, probe, wq, bq, wk, wv, bv)


def head_kernel(heads, nsp, ntp, pk_ref, hb_hbm, wo_hbm, wu_hbm, wd_hbm, og_ref, bo_ref, hg_ref, hb_ref, bu_ref, bd_ref, bv_ref,
                ga_out, st_out, own_out, hbar_out,
                wo, wu, wd, rbuf, ta, tg, td, ag, hr, wsem, rs_send, rs_recv, ta_s, ta_r, tg_s, tg_r, td_s, td_r, ag_s, ag_r, hr_s, hr_r):
    sp, sp_peers = peers_of('sp', nsp)
    tp, tp_peers = peers_of('tp', ntp)
    loads = [pltpu.make_async_copy(a, b, wsem.at[i]) for i, (a, b) in enumerate(((wd_hbm, wd), (wo_hbm, wo), (wu_hbm, wu), (hb_hbm.at[sp], hr.at[sp])))]
    for load in loads:
        load.start()
    barrier_all([('sp', d) for d in sp_peers] + [('tp', d) for d in tp_peers])
    sends = []
    for k, dev in enumerate(sp_peers):
        sends.append(remote(pk_ref.at[dev], rbuf.at[sp], rs_send.at[k], rs_recv.at[sp], 'sp', dev))
        sends[-1].start()
    late = []
    for k, dev in enumerate(sp_peers):
        late.append(remote(hb_hbm.at[dev], hr.at[sp], hr_s.at[k], hr_r.at[sp], 'sp', dev))
        late[-1].start()
    rbuf[sp] = pk_ref[sp]
    hd = wo.shape[0]
    width = hd // heads
    model = wu.shape[0]
    og = og_ref[sp]
    loads[0].wait()
    gh = nt(og, wd[...])
    for k, dev in enumerate(sp_peers):
        remote(rbuf.at[dev], rbuf.at[dev], rs_send.at[k], rs_recv.at[dev], 'sp', dev).wait_recv()
    for send in sends:
        send.wait_send()
    m = rbuf[0, :, hd:hd + LANES]
    for j in range(1, nsp):
        m = jnp.maximum(m, rbuf[j, :, hd:hd + LANES])
    l = jnp.zeros_like(m)
    v = jnp.zeros((SUB, hd), F32)
    for j in range(nsp):
        w = jnp.exp(rbuf[j, :, hd:hd + LANES] - m)
        l = l + w * rbuf[j, :, hd + LANES:hd + 2 * LANES]
        v = v + by_head([w[:, SUB * h:SUB * h + 1] for h in range(heads)], width) * rbuf[j, :, 0:hd]
    o = v / by_head([l[:, SUB * h:SUB * h + 1] for h in range(heads)], width)
    pooled_bf = o.astype(BF16)
    lse = m + jnp.log(l)
    loads[1].wait()
    ta[tp] = nn(pooled_bf, wo[...])
    gather_start(ta, tp, tp_peers, ta_s, ta_r, 'tp')
    loads[2].wait()
    gather_wait(ta, tp, tp_peers, ta_s, ta_r, 'tp')
    attn = ta[0]
    for t in range(1, ntp):
        attn = attn + ta[t]
    attn = attn + row(bo_ref)
    hat, inv = centre(attn)
    gain = row(hg_ref)
    y = (hat * gain + row(hb_ref)).astype(BF16)
    value, slope = gelu_parts(nn(y, wu[...]) + row(bu_ref))
    tg[tp] = nt((gh * slope).astype(BF16), wu[...])
    gather_start(tg, tp, tp_peers, tg_s, tg_r, 'tp')
    td[tp] = nn(value.astype(BF16), wd[...])
    gather_start(td, tp, tp_peers, td_s, td_r, 'tp')
    gather_wait(tg, tp, tp_peers, tg_s, tg_r, 'tp')
    gno = tg[0]
    for t in range(1, ntp):
        gno = gno + tg[t]
    ga = (og.astype(F32) + norm_back(hat, inv, gno * gain)).astype(BF16)
    gp = nt(ga, wo[...]).astype(BF16).astype(F32)
    prod = gp * (o - flat(bv_ref))
    head_of = iota(prod.shape, 1) // width
    delta = by_head([jnp.sum(jnp.where(head_of == h, prod, 0.0), axis=1, keepdims=True) for h in range(heads)], SUB)
    ag[sp, :, 0:model] = ga.astype(F32)
    ag[sp, :, model:model + LANES] = lse
    ag[sp, :, model + LANES:model + 2 * LANES] = jnp.concatenate([delta, jnp.zeros((SUB, LANES - heads * SUB), F32)], axis=1)
    gather_start(ag, sp, sp_peers, ag_s, ag_r, 'sp')
    gather_wait(td, tp, tp_peers, td_s, td_r, 'tp')
    down = td[0]
    for t in range(1, ntp):
        down = down + td[t]
    own_out[:, 0:model] = y.astype(F32)
    own_out[:, model:2 * model] = (attn + down + row(bd_ref)).astype(BF16).astype(F32)
    own_out[:, 2 * model:2 * model + hd] = pooled_bf.astype(F32)
    loads[3].wait()
    for k, dev in enumerate(sp_peers):
        remote(hr.at[dev], hr.at[dev], hr_s.at[k], hr_r.at[dev], 'sp', dev).wait_recv()
    for send in late:
        send.wait_send()
    hbar = jnp.zeros(hbar_out.shape, F32)
    for j in range(nsp):
        w = jnp.exp(rbuf[j, :, hd:hd + LANES] - lse)
        hbar = hbar + hr[j] * jnp.concatenate([w[:, SUB * h:SUB * h + 1] for h in range(heads)], axis=0)
    hbar_out[...] = hbar
    gather_wait(ag, sp, sp_peers, ag_s, ag_r, 'sp')
    ga_out[...] = ag[:, :, 0:model].astype(BF16)
    st_out[...] = ag[:, :, model:model + 2 * LANES]


def head(heads, nsp, ntp, pk, hb, wo, wu, wd, og3, vectors):
    own, model = og3.shape[1:]
    hd = wo.shape[0]
    pk3 = pk.reshape(nsp, own, pk.shape[1])
    vm, hbm = pl.BlockSpec(memory_space=pltpu.VMEM), pl.BlockSpec(memory_space=pl.ANY)
    dma = pltpu.SemaphoreType.DMA
    part = pltpu.VMEM((ntp, own, model), F32)
    return pl.pallas_call(
        functools.partial(head_kernel, heads, nsp, ntp),
        in_specs=[vm, hbm, hbm, hbm, hbm] + [vm] * 7,
        out_specs=[vm] * 4,
        out_shape=[jax.ShapeDtypeStruct((nsp, own, model), BF16), jax.ShapeDtypeStruct((nsp, own, 2 * LANES), F32), jax.ShapeDtypeStruct((own, 2 * model + hd), F32), jax.ShapeDtypeStruct(hb.shape[1:], F32)],
        scratch_shapes=[pltpu.VMEM(wo.shape, BF16), pltpu.VMEM(wu.shape, BF16), pltpu.VMEM(wd.shape, BF16), pltpu.VMEM(pk3.shape, F32), part, part, part, pltpu.VMEM((nsp, own, model + 2 * LANES), F32), pltpu.VMEM(hb.shape, F32),
                        dma((4,)), dma((nsp - 1,)), dma((nsp,)), dma((ntp - 1,)), dma((ntp,)), dma((ntp - 1,)), dma((ntp,)), dma((ntp - 1,)), dma((ntp,)), dma((nsp - 1,)), dma((nsp,)), dma((nsp - 1,)), dma((nsp,))],
        compiler_params=pltpu.CompilerParams(collective_id=0, has_side_effects=True),
        name='head',
    )(pk3, hb, wo, wu, wd, og3, *vectors)


def chip_start(buf, sp, mate, sames, send_sems, recv_sems):
    for k, dev in enumerate([mate] + sames):
        remote(buf.at[sp], buf.at[sp], send_sems.at[k], recv_sems.at[sp], 'sp', dev).start()


def chip_forward(buf, sp, mate, sames, send_sems, recv_sems):
    for k, dev in enumerate(sames):
        remote(buf.at[dev], buf.at[dev], send_sems.at[k + 1], recv_sems.at[dev], 'sp', dev).wait_recv()
        remote(buf.at[dev], buf.at[dev], send_sems.at[len(sames) + 1 + k], recv_sems.at[dev], 'sp', mate).start()


def chip_finish(buf, sp, mate, sames, others, send_sems, recv_sems):
    for dev in [mate] + others:
        remote(buf.at[dev], buf.at[dev], send_sems.at[0], recv_sems.at[dev], 'sp', mate).wait_recv()
    for k, dev in enumerate([mate] + sames):
        remote(buf.at[sp], buf.at[sp], send_sems.at[k], recv_sems.at[sp], 'sp', dev).wait_send()
    for k, dev in enumerate(sames):
        remote(buf.at[dev], buf.at[dev], send_sems.at[len(sames) + 1 + k], recv_sems.at[dev], 'sp', mate).wait_send()


def spread_kernel(heads, nsp, ntp, ga_ref, wo_ref, wv_ref, own_ref, hbar_ref, st_ref, qk_ref, og_ref, bu_ref, wu_hbm, wd_hbm,
                  gv_out, hbar_out, st_out, qk_out, gp_out, y_out, pool_out, pb_out, hid_out, gpre_out,
                  wu, wd, pa, ha, wsem, gv_s, gv_r, fw_s, fw_r, pa_s, pa_r, ha_s, ha_r, st_s, st_r, qk_s, qk_r):
    sp, sp_peers = peers_of('sp', nsp)
    tp, tp_peers = peers_of('tp', ntp)
    core = lax.rem(sp, 2)
    mate = sp + 1 - 2 * core
    sames = [lax.rem(sp + 2 * k, nsp) for k in range(1, nsp // 2)]
    others = [lax.rem(mate + 2 * k, nsp) for k in range(1, nsp // 2)]
    half = nsp // 2
    hd = wo_ref.shape[0]
    width = hd // heads
    model = wo_ref.shape[1]
    images = nsp * SUB
    loads = [pltpu.make_async_copy(a, b, wsem.at[i]) for i, (a, b) in enumerate(((wd_hbm, wd), (wu_hbm, wu)))]
    for load in loads:
        load.start()
    sem = pltpu.get_barrier_semaphore()
    for axis, devs in (('sp', sp_peers), ('tp', tp_peers)):
        for dev in devs:
            pl.semaphore_signal(sem, inc=1, device_id={axis: dev}, device_id_type=MESH)
    pa[sp] = own_ref[...]
    ha[sp] = hbar_ref[...]
    st_out[tp] = st_ref[...]
    qk_out[tp] = qk_ref[...]
    gp_all = nt(ga_ref[...].reshape(images, model), wo_ref[...]).astype(BF16)
    gp_out[...] = gp_all.reshape(nsp, SUB, hd)

    def make_gv(i, _):
        g = lax.rem(core * half + i, nsp)
        gp = gp_out[g].astype(F32)
        gp = jnp.concatenate([gp] * heads, axis=0)
        gp = jnp.where(iota(gp.shape, 0) // SUB == iota(gp.shape, 1) // width, gp, 0.0).astype(BF16)
        gv_out[tp, g] = nn(gp, wv_ref[...])
        return 0

    lax.fori_loop(0, half, make_gv, 0)
    pl.semaphore_wait(sem, len(sp_peers) + len(tp_peers))
    for i in range(half):
        g = core * half + i
        for k, dev in enumerate(tp_peers):
            remote(gv_out.at[tp, g], gv_out.at[tp, g], gv_s.at[k, i], gv_r.at[tp, i], 'tp', dev).start()
        if i == 0:
            gather_start(st_out, tp, tp_peers, st_s, st_r, 'tp')
            gather_start(qk_out, tp, tp_peers, qk_s, qk_r, 'tp')
    chip_start(pa, sp, mate, sames, pa_s, pa_r)
    chip_start(ha, sp, mate, sames, ha_s, ha_r)
    lax.fori_loop(half, nsp, make_gv, 0)
    loads[0].wait()
    og = og_ref[...].reshape(images, model)
    gh = nt(og, wd[...])
    chip_forward(pa, sp, mate, sames, pa_s, pa_r)
    chip_finish(pa, sp, mate, sames, others, pa_s, pa_r)
    y = pa[:, :, 0:model].astype(BF16)
    y_out[...] = y
    pool_out[...] = pa[:, :, model:2 * model].astype(BF16)
    pb_out[...] = pa[:, :, 2 * model:2 * model + hd].astype(BF16)
    loads[1].wait()
    value, slope = gelu_parts(nn(y.reshape(images, model), wu[...]) + row(bu_ref))
    hid_out[...] = value.astype(BF16)
    gpre_out[...] = (gh * slope).astype(BF16)
    for i in range(half):
        g = core * half + i
        for k, dev in enumerate(tp_peers):
            remote(gv_out.at[dev, g], gv_out.at[dev, g], gv_s.at[k, i], gv_r.at[dev, i], 'tp', dev).wait_recv()
            remote(gv_out.at[dev, g], gv_out.at[dev, g], fw_s.at[k, i], fw_r.at[dev, i], 'sp', mate).start()
        if i == 1:
            chip_forward(ha, sp, mate, sames, ha_s, ha_r)
    chip_finish(ha, sp, mate, sames, others, ha_s, ha_r)
    hbar_out[...] = ha[...].astype(BF16)
    for i in range(half):
        g = core * half + i
        other = (1 - core) * half + i
        for k, dev in enumerate(tp_peers):
            remote(gv_out.at[tp, g], gv_out.at[tp, g], gv_s.at[k, i], gv_r.at[tp, i], 'tp', dev).wait_send()
            remote(gv_out.at[dev, g], gv_out.at[dev, g], fw_s.at[k, i], fw_r.at[dev, i], 'sp', mate).wait_send()
            remote(gv_out.at[dev, other], gv_out.at[dev, other], fw_s.at[k, i], fw_r.at[dev, i], 'sp', mate).wait_recv()
    gather_wait(st_out, tp, tp_peers, st_s, st_r, 'tp')
    gather_wait(qk_out, tp, tp_peers, qk_s, qk_r, 'tp')


def spread(heads, nsp, ntp, ga3, wo, wv, own, hbar, st, qk, og3, bu, wu, wd):
    rows, model = hbar.shape
    hd = wo.shape[0]
    images = nsp * SUB
    vm, hbm = pl.BlockSpec(memory_space=pltpu.VMEM), pl.BlockSpec(memory_space=pl.ANY)
    dma = pltpu.SemaphoreType.DMA
    half = nsp // 2
    sds = jax.ShapeDtypeStruct
    chip = 2 * half
    return pl.pallas_call(
        functools.partial(spread_kernel, heads, nsp, ntp),
        in_specs=[vm] * 9 + [hbm] * 2,
        out_specs=[vm] * 10,
        out_shape=[sds((ntp, nsp, rows, model), F32), sds((nsp, rows, model), BF16), sds((ntp,) + st.shape, F32), sds((ntp,) + qk.shape, F32), sds((nsp, SUB, hd), BF16),
                   sds((nsp, SUB, model), BF16), sds((nsp, SUB, model), BF16), sds((nsp, SUB, hd), BF16), sds((images, model), BF16), sds((images, model), BF16)],
        scratch_shapes=[pltpu.VMEM(wu.shape, BF16), pltpu.VMEM(wd.shape, BF16), pltpu.VMEM((nsp,) + own.shape, F32), pltpu.VMEM((nsp, rows, model), F32), dma((2,)),
                        dma((ntp - 1, half)), dma((ntp, half)), dma((ntp - 1, half)), dma((ntp, half)), dma((chip,)), dma((nsp,)), dma((chip,)), dma((nsp,)), dma((ntp - 1,)), dma((ntp,)), dma((ntp - 1,)), dma((ntp,))],
        compiler_params=pltpu.CompilerParams(collective_id=1, has_side_effects=True),
        name='spread',
    )(ga3, wo, wv, own, hbar, st, qk, og3, bu, wu, wd)


def products_kernel(y_ref, gpre_ref, hid_ref, og_ref, gup_ref, gdown_ref):
    gup_ref[...] = tn(y_ref[...], gpre_ref[...])
    gdown_ref[...] = tn(hid_ref[...], og_ref[...])


def products(y, gpre, hid, og):
    images, model = y.shape
    cols = gpre.shape[1]
    tile = 2 * LANES
    part = pl.BlockSpec((images, tile), lambda i: (0, i))
    whole = pl.BlockSpec((images, cols), lambda i: (0, 0))
    out = pl.BlockSpec((tile, cols), lambda i: (i, 0))
    return pl.pallas_call(
        products_kernel,
        grid=(model // tile,),
        in_specs=[part, whole, part, whole],
        out_specs=[out, out],
        out_shape=[jax.ShapeDtypeStruct((model, cols), F32), jax.ShapeDtypeStruct((cols, model), F32)],
        name='products',
    )(y, gpre, hid, og)


def back_kernel(heads, ntp, scale, x_ref, gain_ref, bias_ref, gv_ref, qk_ref, st_ref, gx_ref, u_ref, qkr, uacc):
    step = pl.program_id(0)
    rows = heads * SUB
    model = x_ref.shape[1]

    @pl.when(step == 0)
    def _():
        for t in range(ntp):
            for h in range(heads):
                hi, lo = hi_lo(jnp.broadcast_to(qk_ref[t, h:h + 1, :], (SUB, model)))
                at = (t * heads + h) * SUB
                qkr[at:at + SUB, :] = hi.astype(F32)
                qkr[LANES + at:LANES + at + SUB, :] = lo.astype(F32)
        uacc[...] = jnp.zeros(uacc.shape, F32)

    images, tokens = SUB, x_ref.shape[0] // SUB
    hat, inv = centre(x_ref[...].astype(F32))
    gain = row(gain_ref)
    hid = (hat * gain + row(bias_ref)).astype(BF16)
    qkb = qkr[...].astype(BF16)
    gv_hi, gv_lo = hi_lo(gv_ref[...].reshape(ntp * rows, model))
    r = nt(hid, qkb)
    s = (r[:, 0:LANES] + r[:, LANES:2 * LANES]) * scale
    d = nt(hid, jnp.concatenate([gv_hi, gv_lo], axis=0))
    d = d[:, 0:LANES] + d[:, LANES:2 * LANES]
    lse = jnp.concatenate([st_ref[t, 0, :, 0:rows] for t in range(ntp)], axis=1)
    delta = jnp.concatenate([st_ref[t, 0, :, LANES:LANES + rows] for t in range(ntp)], axis=1)
    shape = (images, tokens, LANES)
    keep = iota(shape, 2) % SUB == iota(shape, 0)
    p = jnp.where(keep, jnp.exp(s.reshape(shape) - lse[:, None, :]), 0.0)
    ds = p * (d.reshape(shape) - delta[:, None, :]) * scale
    pb = p.astype(BF16).reshape(images * tokens, LANES)
    db = ds.astype(BF16).reshape(images * tokens, LANES)
    gh = nn(jnp.concatenate([pb, db], axis=1), jnp.concatenate([gv_hi, qkb[0:LANES]], axis=0))
    uacc[...] += tn(db, hid)
    gx_ref[...] = norm_back(hat, inv, gh * gain).astype(BF16)

    @pl.when(step == pl.num_programs(0) - 1)
    def _():
        tp = lax.axis_index('tp')
        for h in range(heads):
            mine = uacc[pl.ds(pl.multiple_of(tp * rows + h * SUB, SUB), SUB), :]
            u_ref[h:h + 1, :] = jnp.sum(mine, axis=0, keepdims=True)


def back_tokens(heads, ntp, scale, x, gain, bias, gv, qk, st):
    tokens_all, model = x.shape
    groups, rows = gv.shape[1], gv.shape[2]
    block = tokens_all // groups
    full = lambda a: pl.BlockSpec(a.shape, lambda g: (0,) * a.ndim)
    return pl.pallas_call(
        functools.partial(back_kernel, heads, ntp, scale),
        grid=(groups,),
        in_specs=[pl.BlockSpec((block, model), lambda g: (g, 0)), full(gain), full(bias), pl.BlockSpec((ntp, 1, rows, model), lambda g: (0, g, 0, 0)), full(qk), pl.BlockSpec((ntp, 1) + st.shape[2:], lambda g: (0, g, 0, 0))],
        out_specs=[pl.BlockSpec((block, model), lambda g: (g, 0)), pl.BlockSpec((heads, model), lambda g: (0, 0))],
        out_shape=[jax.ShapeDtypeStruct((tokens_all, model), BF16), jax.ShapeDtypeStruct((heads, model), F32)],
        scratch_shapes=[pltpu.VMEM((2 * LANES, model), F32), pltpu.VMEM((LANES, model), F32)],
        name='back_tokens',
    )(x, gain, bias, gv, qk, st)


def query_kernel(heads, nsp, ntp, u_ref, wq_ref, wk_ref, u_out, gq_out, gpr_out, ub, pb, u_s, u_r, p_s, p_r):
    sp, sp_peers = peers_of('sp', nsp)
    tp = lax.axis_index('tp')
    hd = wk_ref.shape[0]
    width = hd // heads
    everyone = [(lax.rem(tp + a, ntp), lax.rem(sp + b, nsp)) for a in range(ntp) for b in range(nsp) if a or b]
    sem = pltpu.get_barrier_semaphore()
    for t, j in everyone:
        pl.semaphore_signal(sem, inc=1, device_id={'tp': t, 'sp': j}, device_id_type=MESH)
    ub[sp] = u_ref[...]

    def query_grad(u):
        hi, lo = hi_lo(u)
        g = nt(jnp.concatenate([hi, lo], axis=0), wk_ref[...])
        g = g[0:heads] + g[heads:2 * heads]
        return jnp.sum(jnp.where(iota(g.shape, 0) == iota(g.shape, 1) // width, g, 0.0), axis=0, keepdims=True)

    hi, lo = hi_lo(query_grad(u_ref[...]))
    gpr = nn(jnp.concatenate([hi, lo], axis=0), wq_ref[...])
    mine = tp * nsp + sp
    pb[mine] = gpr[0:1] + gpr[1:2]
    pl.semaphore_wait(sem, len(everyone))
    gather_start(ub, sp, sp_peers, u_s, u_r, 'sp')
    sends = []
    for k, (t, j) in enumerate(everyone):
        sends.append(pltpu.make_async_remote_copy(src_ref=pb.at[mine], dst_ref=pb.at[mine], send_sem=p_s.at[k], recv_sem=p_r.at[mine], device_id={'tp': t, 'sp': j}, device_id_type=MESH))
        sends[-1].start()
    gather_wait(ub, sp, sp_peers, u_s, u_r, 'sp')
    u = ub[0]
    for j in range(1, nsp):
        u = u + ub[j]
    u_out[...] = u
    gq_out[...] = query_grad(u)
    for k, (t, j) in enumerate(everyone):
        slot = t * nsp + j
        pltpu.make_async_remote_copy(src_ref=pb.at[slot], dst_ref=pb.at[slot], send_sem=p_s.at[k], recv_sem=p_r.at[slot], device_id={'tp': t, 'sp': j}, device_id_type=MESH).wait_recv()
    for send in sends:
        send.wait_send()
    total = pb[0]
    for j in range(1, ntp * nsp):
        total = total + pb[j]
    gpr_out[...] = total


def query_grads(heads, nsp, ntp, u, wq, wk):
    hd, model = wq.shape
    vm = pl.BlockSpec(memory_space=pltpu.VMEM)
    dma = pltpu.SemaphoreType.DMA
    return pl.pallas_call(
        functools.partial(query_kernel, heads, nsp, ntp),
        in_specs=[vm] * 3,
        out_specs=[vm] * 3,
        out_shape=[jax.ShapeDtypeStruct((heads, model), F32), jax.ShapeDtypeStruct((1, hd), F32), jax.ShapeDtypeStruct((1, model), F32)],
        scratch_shapes=[pltpu.VMEM((nsp, heads, model), F32), pltpu.VMEM((ntp * nsp, 1, model), F32), dma((nsp - 1,)), dma((nsp,)), dma((ntp * nsp - 1,)), dma((ntp * nsp,))],
        compiler_params=pltpu.CompilerParams(collective_id=2, has_side_effects=True),
        name='query_grads',
    )(u, wq, wk)


def local_head(nsp, ntp, encoded, enc_gain, enc_bias, probe, w_query, b_query, w_key, w_value, b_value, w_out, b_out, head_gain, head_bias, w_up, b_up, w_down, b_down, out_grad):
    images, tokens, model = encoded.shape
    heads, head_dim = b_query.shape
    hd = heads * head_dim
    scale = head_dim ** -0.5
    x = encoded.reshape(images * tokens, model)
    wq, wk, wv = (jnp.transpose(w, (1, 2, 0)).reshape(hd, model) for w in (w_query, w_key, w_value))
    wo = w_out.reshape(hd, model)
    og3 = out_grad.reshape(nsp, images // nsp, model)
    pk, hb, qk, q8 = scan_tokens(heads, images, scale, x, enc_gain, enc_bias, probe, wq, b_query, wk, wv, b_value)
    ga3, st, own, hbar_own = head(heads, nsp, ntp, pk, hb, wo, w_up, w_down, og3, (b_out, head_gain, head_bias, b_up, b_down, b_value))
    gv, hbar, st_all, qk_all, gp3, y3, pool3, pb3, hidden, grad_pre = spread(heads, nsp, ntp, ga3, wo, wv, own, hbar_own, st, qk, og3, b_up, w_up, w_down)
    gx, u = back_tokens(heads, ntp, scale, x, enc_gain, enc_bias, gv, qk_all, st_all)
    u, gq, gpr = query_grads(heads, nsp, ntp, u, wq, wk)
    y, ga, pooled_bf = (a.reshape(images, -1) for a in (y3, ga3, pb3))
    grad_w_up, grad_w_down = products(y, grad_pre, hidden, out_grad)
    grad_w_out = jnp.einsum('bk,bw->kw', pooled_bf, ga, preferred_element_type=F32).reshape(heads, head_dim, model)
    gp4 = gp3.reshape(nsp, images // nsp, heads, head_dim)
    hbar4 = hbar.reshape(nsp, heads, images // nsp, model)
    grad_wv = jnp.einsum('gihd,ghiw->hdw', gp4, hbar4, preferred_element_type=F32)
    grad_wk = q8[0].reshape(heads, head_dim, 1) * u[:, None, :]
    grad_wq = gq.reshape(heads, head_dim, 1) * probe[None, None, :]
    back = lambda a: jnp.transpose(a, (2, 0, 1))
    return (pool3.reshape(images, model), gx.reshape(encoded.shape), gpr.reshape(model), back(grad_wq), back(grad_wk), back(grad_wv), grad_w_out, grad_w_up, grad_w_down)


def solution(mesh):
    body = functools.partial(local_head, mesh.shape['sp'], mesh.shape['tp'])
    return jax.shard_map(body, mesh=mesh, in_specs=IN_SPECS, out_specs=OUT_SPECS, check_vma=False)
```

```python
import functools
import jax
import jax.numpy as jnp
from jax import lax
from jax.experimental import pallas as pl
from jax.experimental.pallas import tpu as pltpu
from jax.sharding import PartitionSpec as P

NORM_EPS = 1e-6
MESH = pl.DeviceIdType.MESH
F32, BF16 = jnp.float32, jnp.bfloat16
IN_SPECS = (P('dp', 'sp', None), P(), P(), P(), P(None, 'tp', None), P('tp', None), P(None, 'tp', None), P(None, 'tp', None), P('tp', None), P('tp', None, None), P(), P(), P(), P(None, 'tp'), P('tp'), P('tp', None), P(), P('dp', None))
OUT_SPECS = (P('dp', None), P('dp', 'sp', None), P('dp'), P('dp', 'tp', None), P('dp', 'tp', None), P('dp', 'tp', None), P(('dp', 'tp'), None, None), P('dp', 'tp'), P(('dp', 'tp'), None))
LANES = 128
SUB = 8
GELU_C = 0.7978845608028654
GELU_A = 0.044715


def nn(a, b):
    return lax.dot_general(a, b, (((1,), (0,)), ((), ())), preferred_element_type=F32)


def nt(a, b):
    return lax.dot_general(a, b, (((1,), (1,)), ((), ())), preferred_element_type=F32)


def tn(a, b):
    return lax.dot_general(a, b, (((0,), (0,)), ((), ())), preferred_element_type=F32)


def hi_lo(a):
    hi = a.astype(BF16)
    return hi, (a - hi.astype(F32)).astype(BF16)


def iota(shape, dim):
    return lax.broadcasted_iota(jnp.int32, shape, dim)


def by_head(parts, width):
    rows, cols = parts[0].shape[0], len(parts) * width
    block = iota((rows, cols), 1) // width
    out = jnp.zeros((rows, cols), F32)
    for h, part in enumerate(parts):
        out = jnp.where(block == h, part, out)
    return out


def row(ref):
    return ref[...].reshape(1, -1)


def flat(ref):
    heads, width = ref.shape
    wide = jnp.concatenate([ref[...]] * heads, axis=1)
    keep = iota(wide.shape, 0) == iota(wide.shape, 1) // width
    return jnp.sum(jnp.where(keep, wide, 0.0), axis=0, keepdims=True)


def gelu_parts(pre):
    t = jnp.tanh(GELU_C * (pre + GELU_A * pre * pre * pre))
    value = 0.5 * pre * (1.0 + t)
    slope = 0.5 * (1.0 + t) + 0.5 * pre * (1.0 - t * t) * (GELU_C * (1.0 + 3.0 * GELU_A * pre * pre))
    return value, slope


def centre(rows):
    mean = jnp.mean(rows, axis=-1, keepdims=True)
    centred = rows - mean
    inv = lax.rsqrt(jnp.mean(centred * centred, axis=-1, keepdims=True) + NORM_EPS)
    return centred * inv, inv


def norm_back(hat, inv, cot):
    return inv * (cot - jnp.mean(cot, axis=-1, keepdims=True) - hat * jnp.mean(cot * hat, axis=-1, keepdims=True))


def barrier_all(peers):
    sem = pltpu.get_barrier_semaphore()
    for axis, dev in peers:
        pl.semaphore_signal(sem, inc=1, device_id={axis: dev}, device_id_type=MESH)
    pl.semaphore_wait(sem, len(peers))


def peers_of(axis, n):
    me = lax.axis_index(axis)
    return me, [lax.rem(me + k, n) for k in range(1, n)]


def remote(src, dst, send_sem, recv_sem, axis, dev):
    return pltpu.make_async_remote_copy(src_ref=src, dst_ref=dst, send_sem=send_sem, recv_sem=recv_sem, device_id={axis: dev}, device_id_type=MESH)


def gather_start(buf, me, peers, send_sems, recv_sems, axis):
    for k, dev in enumerate(peers):
        remote(buf.at[me], buf.at[me], send_sems.at[k], recv_sems.at[me], axis, dev).start()


def gather_wait(buf, me, peers, send_sems, recv_sems, axis):
    for k, dev in enumerate(peers):
        remote(buf.at[dev], buf.at[dev], send_sems.at[k], recv_sems.at[dev], axis, dev).wait_recv()
    for k, dev in enumerate(peers):
        remote(buf.at[me], buf.at[me], send_sems.at[k], recv_sems.at[me], axis, dev).wait_send()


class ChipRing:
    def __init__(self, nsp):
        me = lax.axis_index('sp')
        self.me, self.core = me, lax.rem(me, 2)
        self.mate = me + 1 - 2 * self.core
        self.up, self.down, self.far = (lax.rem(me + k, nsp) for k in (2, nsp - 2, 4))
        self.mates = [lax.rem(self.mate + k, nsp) for k in (2, nsp - 2, 4)]
        self.around = [self.mate, self.up, self.down, self.far] + self.mates

    def start(self, buf, send, recv):
        for k, dev in enumerate((self.mate, self.up, self.down)):
            remote(buf.at[self.me], buf.at[self.me], send.at[k], recv.at[self.me], 'sp', dev).start()

    def relay(self, buf, send, recv, upward):
        for k, dev in ((3, self.down), (4, self.up)):
            remote(buf.at[dev], buf.at[dev], send.at[k], recv.at[dev], 'sp', dev).wait_recv()
            if upward == (k == 3):
                remote(buf.at[dev], buf.at[dev], send.at[5], recv.at[dev], 'sp', self.up if upward else self.down).start()
            remote(buf.at[dev], buf.at[dev], send.at[k], recv.at[dev], 'sp', self.mate).start()

    def finish(self, buf, send, recv, upward):
        far = self.far
        remote(buf.at[far], buf.at[far], send.at[6], recv.at[far], 'sp', self.mate).wait_recv()
        remote(buf.at[far], buf.at[far], send.at[6], recv.at[far], 'sp', self.mate).start()
        for dev in [self.mate] + self.mates:
            remote(buf.at[dev], buf.at[dev], send.at[0], recv.at[dev], 'sp', self.mate).wait_recv()
        via = self.down if upward else self.up
        for k, slot in ((0, self.me), (1, self.me), (2, self.me), (3, self.down), (4, self.up), (5, via), (6, far)):
            remote(buf.at[slot], buf.at[slot], send.at[k], recv.at[slot], 'sp', self.mate).wait_send()


RING_SEMS = 7


def scan_kernel(heads, scale, x_ref, gain_ref, bias_ref, probe_ref, wq_ref, bq_ref, wk_ref, wv_ref, bv_ref, pk_ref, hb_ref, qk_ref, q_ref, qkr, hball):
    rows = heads * SUB
    width = wq_ref.shape[0] // heads

    @pl.when(pl.program_id(0) == 0)
    def _():
        probe8 = jnp.broadcast_to(row(probe_ref), (SUB, probe_ref.shape[0])).astype(BF16)
        q8 = (nt(probe8, wq_ref[...]) + flat(bq_ref)).astype(BF16)
        q_ref[...] = q8.astype(F32)
        qs = jnp.concatenate([q8.astype(F32)] * heads, axis=0)
        qs = jnp.where(iota(qs.shape, 0) // SUB == iota(qs.shape, 1) // width, qs, 0.0).astype(BF16)
        qk = nn(qs, wk_ref[...])
        hi, lo = hi_lo(qk)
        qkr[...] = jnp.zeros(qkr.shape, BF16)
        qkr[0:rows, :] = hi
        qkr[LANES // 2:LANES // 2 + rows, :] = lo
        for h in range(heads):
            qk_ref[h:h + 1, :] = qk[SUB * h:SUB * h + 1, :]

    step = pl.program_id(0)
    images, tokens = SUB, x_ref.shape[0] // SUB
    hat, _ = centre(x_ref[...].astype(F32))
    hid = (hat * row(gain_ref) + row(bias_ref)).astype(BF16)
    r = nt(hid, qkr[...])
    s = ((r + pltpu.roll(r, LANES // 2, 1)) * scale).reshape(images, tokens, LANES)
    m = jnp.max(s, axis=1)
    e = jnp.exp(s - m[:, None, :])
    l = jnp.sum(e, axis=1)
    lane, img = iota(e.shape, 2), iota(e.shape, 0)
    ebd = jnp.where((lane % SUB == img) & (lane < rows), e, 0.0).astype(BF16).reshape(images * tokens, LANES)
    hb = tn(ebd, hid)[0:rows, :]
    hb_ref[0, :, :] = hb
    hball[step] = hb
    cols = wq_ref.shape[0]
    mine = pl.ds(pl.multiple_of(step * SUB, SUB), SUB)
    pk_ref[mine, cols:cols + LANES] = m
    pk_ref[mine, cols + LANES:cols + 2 * LANES] = l

    @pl.when(step == pl.num_programs(0) - 1)
    def _():
        groups = hball.shape[0]
        every = groups * rows
        hi, lo = hi_lo(hball[...].reshape(every, hball.shape[2]))
        v = nt(hi, wv_ref[...]) + nt(lo, wv_ref[...])
        bias = flat(bv_ref)
        for g in range(groups):
            vs = by_head([v[g * rows + SUB * h:g * rows + SUB * h + SUB] for h in range(heads)], width)
            tot = pk_ref[g * SUB:g * SUB + SUB, cols + LANES:cols + 2 * LANES]
            pk_ref[g * SUB:g * SUB + SUB, 0:cols] = vs + by_head([tot[:, SUB * h:SUB * h + 1] for h in range(heads)], width) * bias


def scan_tokens(heads, images, scale, x, gain, bias, probe, wq, bq, wk, wv, bv):
    tokens_all, width = x.shape
    hd = wq.shape[0]
    groups = images // SUB
    block = tokens_all // groups
    full = lambda a: pl.BlockSpec(a.shape, lambda g: (0,) * a.ndim)
    return pl.pallas_call(
        functools.partial(scan_kernel, heads, scale),
        grid=(groups,),
        in_specs=[pl.BlockSpec((block, width), lambda g: (g, 0))] + [full(a) for a in (gain, bias, probe, wq, bq, wk, wv, bv)],
        out_specs=[pl.BlockSpec((images, hd + 2 * LANES), lambda g: (0, 0)), pl.BlockSpec((1, heads * SUB, width), lambda g: (g, 0, 0)), pl.BlockSpec((heads, width), lambda g: (0, 0)), pl.BlockSpec((SUB, hd), lambda g: (0, 0))],
        out_shape=[jax.ShapeDtypeStruct((images, hd + 2 * LANES), F32), jax.ShapeDtypeStruct((groups, heads * SUB, width), F32), jax.ShapeDtypeStruct((heads, width), F32), jax.ShapeDtypeStruct((SUB, hd), F32)],
        scratch_shapes=[pltpu.VMEM((LANES, width), BF16), pltpu.VMEM((groups, heads * SUB, width), F32)],
        name='scan_tokens',
    )(x, gain, bias, probe, wq, bq, wk, wv, bv)


def middle_kernel(heads, nsp, ntp, scale, pk_ref, og_ref, qk_ref, bo_ref, hg_ref, hb_ref, bu_ref, bd_ref, bv_ref, eg_ref, eb_ref, hb_hbm, x_hbm, wo_hbm, wu_hbm, wd_hbm, wv_hbm, wk_hbm, wq_hbm,
                  gv_out, hbar_out, st_out, qk_out, gp_out, y_out, ga_out, pool_out, pb_out, hid_out, gpre_out, u_out, gq_out, gpr_out,
                  wo, wu, wd, wv, wk, wq, rbuf, ta, tg, td, ag, hr, relay, pa, ha, xb, rhs, uacc, ub, prb, ghb,
                  wsem, xsem, rs_send, rs_recv, ta_s, ta_r, tg_s, tg_r, td_s, td_r, ag_s, ag_r, hr_s, hr_r, rl_r, gv_s, gv_r, fw_s, fw_r, pa_s, pa_r, ha_s, ha_r, st_s, st_r, qk_s, qk_r, ub_s, ub_r, pr_s, pr_r):
    sp, sp_peers = peers_of('sp', nsp)
    tp, tp_peers = peers_of('tp', ntp)
    ring = ChipRing(nsp)
    core, mate = ring.core, ring.mate
    loads = [pltpu.make_async_copy(a, b, wsem.at[i]) for i, (a, b) in enumerate(((wd_hbm, wd), (wo_hbm, wo), (wu_hbm, wu), (hb_hbm.at[sp], hr.at[sp]), (wv_hbm, wv), (wk_hbm, wk), (wq_hbm, wq)))]
    for load in loads:
        load.start()
    sem = pltpu.get_barrier_semaphore()
    for axis, devs in (('sp', sp_peers), ('tp', tp_peers)):
        for dev in devs:
            pl.semaphore_signal(sem, inc=1, device_id={axis: dev}, device_id_type=MESH)

    def x_load(g):
        return pltpu.make_async_copy(x_hbm.at[g], xb.at[g % 2], xsem.at[g % 2])

    x_load(0).start()
    x_load(1).start()
    hd = wo.shape[0]
    width = hd // heads
    model = wu.shape[0]
    rows = heads * SUB
    images = nsp * SUB
    qk_out[tp] = qk_ref[...]
    rbuf[sp] = pk_ref[sp]
    for h in range(heads):
        hi, lo = hi_lo(jnp.broadcast_to(qk_ref[h:h + 1, :], (SUB, model)))
        rhs[h * SUB:h * SUB + SUB, :] = hi.astype(F32)
        rhs[2 * rows + h * SUB:2 * rows + h * SUB + SUB, :] = lo.astype(F32)
    og = og_ref[sp]
    pl.semaphore_wait(sem, len(sp_peers) + len(tp_peers))

    sends = []
    for k, dev in enumerate(sp_peers):
        sends.append(remote(pk_ref.at[dev], rbuf.at[sp], rs_send.at[k], rs_recv.at[sp], 'sp', dev))
        sends[-1].start()
    far0, far1 = ring.far - core, ring.far - core + 1
    late = [remote(hb_hbm.at[far0], relay.at[0], hr_s.at[0], rl_r.at[0], 'sp', ring.up), remote(hb_hbm.at[far1], relay.at[1], hr_s.at[1], rl_r.at[1], 'sp', ring.down)]
    for k, dev in enumerate((ring.up, ring.down, ring.mates[0], ring.mates[1], mate)):
        late.append(remote(hb_hbm.at[dev], hr.at[sp], hr_s.at[2 + k], hr_r.at[sp], 'sp', dev))
    for send in late:
        send.start()
    gather_start(qk_out, tp, tp_peers, qk_s, qk_r, 'tp')
    loads[0].wait()
    gh = nt(og, wd[...])
    for k, dev in enumerate(sp_peers):
        remote(rbuf.at[dev], rbuf.at[dev], rs_send.at[k], rs_recv.at[dev], 'sp', dev).wait_recv()
    for send in sends:
        send.wait_send()
    m = rbuf[0, :, hd:hd + LANES]
    for j in range(1, nsp):
        m = jnp.maximum(m, rbuf[j, :, hd:hd + LANES])
    l = jnp.zeros_like(m)
    v = jnp.zeros((SUB, hd), F32)
    for j in range(nsp):
        w = jnp.exp(rbuf[j, :, hd:hd + LANES] - m)
        l = l + w * rbuf[j, :, hd + LANES:hd + 2 * LANES]
        v = v + by_head([w[:, SUB * h:SUB * h + 1] for h in range(heads)], width) * rbuf[j, :, 0:hd]
    o = v / by_head([l[:, SUB * h:SUB * h + 1] for h in range(heads)], width)
    pooled_bf = o.astype(BF16)
    lse = m + jnp.log(l)

    loads[1].wait()
    ta[tp] = nn(pooled_bf, wo[...])
    gather_start(ta, tp, tp_peers, ta_s, ta_r, 'tp')
    for k, (src, dst) in enumerate(((ring.down, ring.up - core), (ring.up, ring.down - core + 1))):
        remote(relay.at[k], relay.at[k], hr_s.at[k], rl_r.at[k], 'sp', src).wait_recv()
        late.append(remote(relay.at[k], hr.at[src], hr_s.at[7 + k], hr_r.at[src], 'sp', dst))
        late[-1].start()
    loads[2].wait()
    gather_wait(ta, tp, tp_peers, ta_s, ta_r, 'tp')
    attn = ta[0]
    for t in range(1, ntp):
        attn = attn + ta[t]
    attn = attn + row(bo_ref)
    hat, inv = centre(attn)
    gain = row(hg_ref)
    y = (hat * gain + row(hb_ref)).astype(BF16)
    value, slope = gelu_parts(nn(y, wu[...]) + row(bu_ref))
    tg[tp] = nt((gh * slope).astype(BF16), wu[...])
    gather_start(tg, tp, tp_peers, tg_s, tg_r, 'tp')
    td[tp] = nn(value.astype(BF16), wd[...])
    gather_start(td, tp, tp_peers, td_s, td_r, 'tp')
    gather_wait(tg, tp, tp_peers, tg_s, tg_r, 'tp')
    gno = tg[0]
    for t in range(1, ntp):
        gno = gno + tg[t]
    ga = (og.astype(F32) + norm_back(hat, inv, gno * gain)).astype(BF16)
    gp = nt(ga, wo[...]).astype(BF16).astype(F32)
    prod = gp * (o - flat(bv_ref))
    head_of = iota(prod.shape, 1) // width
    delta = by_head([jnp.sum(jnp.where(head_of == h, prod, 0.0), axis=1, keepdims=True) for h in range(heads)], SUB)
    ag[sp, :, 0:model] = ga.astype(F32)
    ag[sp, :, model:model + LANES] = jnp.concatenate([lse[:, 0:rows], delta, jnp.zeros((SUB, LANES - 2 * rows), F32)], axis=1)
    ring.start(ag, ag_s, ag_r)

    gather_wait(td, tp, tp_peers, td_s, td_r, 'tp')
    down = td[0]
    for t in range(1, ntp):
        down = down + td[t]
    pa[sp, :, 0:model] = y.astype(F32)
    pa[sp, :, model:2 * model] = (attn + down + row(bd_ref)).astype(BF16).astype(F32)
    pa[sp, :, 2 * model:2 * model + hd] = pooled_bf.astype(F32)
    ring.start(pa, pa_s, pa_r)
    ring.relay(ag, ag_s, ag_r, True)
    loads[3].wait()
    for k, dev in enumerate(sp_peers):
        remote(hr.at[dev], hr.at[dev], hr_s.at[k], hr_r.at[dev], 'sp', dev).wait_recv()
    for send in late:
        send.wait_send()
    hbar = jnp.zeros(hr.shape[1:], F32)
    for j in range(nsp):
        w = jnp.exp(rbuf[j, :, hd:hd + LANES] - lse)
        hbar = hbar + hr[j] * jnp.concatenate([w[:, SUB * h:SUB * h + 1] for h in range(heads)], axis=0)
    ha[sp] = hbar
    ring.start(ha, ha_s, ha_r)
    loads[4].wait()
    ring.finish(ag, ag_s, ag_r, True)

    ga_out[...] = ag[:, :, 0:model].astype(BF16)
    st_out[tp] = ag[:, :, model:model + LANES]
    near_up, near_down, far_tp = lax.rem(tp + 1, ntp), lax.rem(tp + ntp - 1, ntp), lax.rem(tp + 2, ntp)
    half = nsp // 2
    gp_all = nt(ga_out[...].reshape(images, model), wo[...]).astype(BF16)
    gp_out[...] = gp_all.reshape(nsp, SUB, hd)

    def make_gv(i):
        g = lax.rem(core * half + i, nsp)
        part = gp_out[g].astype(F32)
        part = jnp.concatenate([part] * heads, axis=0)
        part = jnp.where(iota(part.shape, 0) // SUB == iota(part.shape, 1) // width, part, 0.0).astype(BF16)
        gv_out[tp, g] = nn(part, wv[...])

    def piece(i, owner):
        return gv_out.at[owner, core * half + i]

    def send_gv(i, k, owner, dev):
        return remote(piece(i, owner), piece(i, owner), gv_s.at[k, i], gv_r.at[owner, i], 'tp', dev)

    def forward(i, k, owner):
        return remote(piece(i, owner), piece(i, owner), fw_s.at[k, i], fw_r.at[owner, i], 'sp', mate)

    def near(i):
        for k, owner in ((0, near_down), (1, near_up)):
            send_gv(i, k, owner, owner).wait_recv()
            if k == i % 2:
                send_gv(i, 2, owner, near_down if k else near_up).start()
            forward(i, k, owner).start()

    def beyond(i):
        send_gv(i, 2, far_tp, far_tp).wait_recv()
        forward(i, 2, far_tp).start()

    for i in range(half):
        make_gv(i)
        send_gv(i, 0, tp, near_up).start()
        send_gv(i, 1, tp, near_down).start()
        if i == 0:
            gather_start(st_out, tp, tp_peers, st_s, st_r, 'tp')

    def rest_gv(i, _):
        make_gv(i)
        return 0

    lax.fori_loop(half, nsp, rest_gv, 0)

    uacc[...] = jnp.zeros(uacc.shape, F32)

    def u_step(g):
        x_load(g).wait()
        tokens = xb.shape[1] // SUB
        xhat, _ = centre(xb[g % 2].astype(F32))
        if g + 2 < nsp:
            x_load(g + 2).start()
        hidden = (xhat * row(eg_ref) + row(eb_ref)).astype(BF16)
        hi, lo = hi_lo(gv_out[tp, g])
        rhs[rows:2 * rows, :] = hi.astype(F32)
        rhs[3 * rows:4 * rows, :] = lo.astype(F32)
        r = nt(hidden, rhs[...].astype(BF16))
        r = (r + pltpu.roll(r, LANES // 2, 1)).reshape(SUB, tokens, LANES)
        lane, img = iota(r.shape, 2), iota(r.shape, 0)
        r = r * jnp.where(lane < rows, scale, 1.0) - ag[g, :, model:model + LANES][:, None, :]
        r = r.reshape(SUB * tokens, LANES)
        grad = (jnp.exp(r) * pltpu.roll(r, LANES - rows, 1) * scale).reshape(SUB, tokens, LANES)
        ds = jnp.where((lane % SUB == img) & (lane < rows), grad, 0.0).astype(BF16).reshape(SUB * tokens, LANES)
        uacc[...] += tn(ds, hidden)[0:rows, :]

    u_step(0)
    u_step(1)
    ring.relay(pa, pa_s, pa_r, True)
    near(0)
    u_step(2)
    ring.finish(pa, pa_s, pa_r, True)
    ring.relay(ha, ha_s, ha_r, False)
    u_step(3)
    near(1)
    beyond(0)
    u_step(4)
    u_step(5)
    near(2)
    beyond(1)
    ring.finish(ha, ha_s, ha_r, False)
    u_step(6)
    u_step(7)
    for h in range(heads):
        ub[sp, h:h + 1, :] = jnp.sum(uacc[SUB * h:SUB * h + SUB, :], axis=0, keepdims=True)
    gather_start(ub, sp, sp_peers, ub_s, ub_r, 'sp')

    y_all = pa[:, :, 0:model].astype(BF16)
    y_out[...] = y_all
    pool_out[...] = pa[:, :, model:2 * model].astype(BF16)
    pb_out[...] = pa[:, :, 2 * model:2 * model + hd].astype(BF16)
    hbar_out[...] = ha[...].astype(BF16)
    near(3)
    beyond(2)
    ghb[...] = nt(og_ref[...].reshape(images, model), wd[...])
    value, slope = gelu_parts(nn(y_all.reshape(images, model), wu[...]) + row(bu_ref))
    gpre_out[...] = (ghb[...] * slope).astype(BF16)
    hid_out[...] = value.astype(BF16)

    gather_wait(ub, sp, sp_peers, ub_s, ub_r, 'sp')
    u = ub[0]
    for j in range(1, nsp):
        u = u + ub[j]
    u_out[...] = u
    loads[5].wait()
    loads[6].wait()
    hi, lo = hi_lo(u)
    gq = nt(jnp.concatenate([hi, lo], axis=0), wk[...])
    gq = gq[0:heads] + gq[heads:2 * heads]
    gq = jnp.sum(jnp.where(iota(gq.shape, 0) == iota(gq.shape, 1) // width, gq, 0.0), axis=0, keepdims=True)
    gq_out[...] = gq
    hi, lo = hi_lo(gq)
    gpr = nn(jnp.concatenate([hi, lo], axis=0), wq[...])
    prb[tp] = gpr[0:1] + gpr[1:2]
    gather_start(prb, tp, tp_peers, pr_s, pr_r, 'tp')
    beyond(3)
    for i in range(half):
        other = (1 - core) * half + i
        for k, (owner, dev) in enumerate(((tp, near_up), (tp, near_down), (near_up if i % 2 else near_down, near_down if i % 2 else near_up))):
            send_gv(i, k, owner, dev).wait_send()
        for k, owner in enumerate((near_down, near_up, far_tp)):
            forward(i, k, owner).wait_send()
            remote(gv_out.at[owner, other], gv_out.at[owner, other], fw_s.at[k, i], fw_r.at[owner, i], 'sp', mate).wait_recv()
    gather_wait(st_out, tp, tp_peers, st_s, st_r, 'tp')
    gather_wait(qk_out, tp, tp_peers, qk_s, qk_r, 'tp')
    gather_wait(prb, tp, tp_peers, pr_s, pr_r, 'tp')
    total = prb[0]
    for t in range(1, ntp):
        total = total + prb[t]
    gpr_out[...] = total


def middle(heads, nsp, ntp, scale, pk, og3, qk, vectors, hb, x3, wo, wu, wd, wv, wk, wq):
    own, model = og3.shape[1:]
    hd = wo.shape[0]
    rows = hb.shape[1]
    images = nsp * own
    half = nsp // 2
    pk3 = pk.reshape(nsp, own, pk.shape[1])
    vm, hbm = pl.BlockSpec(memory_space=pltpu.VMEM), pl.BlockSpec(memory_space=pl.ANY)
    dma = pltpu.SemaphoreType.DMA
    sds = jax.ShapeDtypeStruct
    part = pltpu.VMEM((ntp, own, model), F32)
    wide = [pltpu.VMEM(w.shape, BF16) for w in (wo, wu, wd, wv, wk, wq)]
    ring, tps, tpr = [dma((RING_SEMS,)), dma((nsp,))], dma((ntp - 1,)), dma((ntp,))
    return pl.pallas_call(
        functools.partial(middle_kernel, heads, nsp, ntp, scale),
        in_specs=[vm] * 11 + [hbm] * 8,
        out_specs=[vm] * 14,
        out_shape=[sds((ntp, nsp, rows, model), F32), sds((nsp, rows, model), BF16), sds((ntp, nsp, own, LANES), F32), sds((ntp,) + qk.shape, F32), sds((nsp, own, hd), BF16),
                   sds((nsp, own, model), BF16), sds((nsp, own, model), BF16), sds((nsp, own, model), BF16), sds((nsp, own, hd), BF16), sds((images, model), BF16), sds((images, model), BF16), sds(qk.shape, F32), sds((1, hd), F32), sds((1, model), F32)],
        scratch_shapes=wide + [pltpu.VMEM(pk3.shape, F32), part, part, part, pltpu.VMEM((nsp, own, model + LANES), F32), pltpu.VMEM(hb.shape, F32), pltpu.VMEM((2,) + hb.shape[1:], F32), pltpu.VMEM((nsp, own, 2 * model + hd), F32), pltpu.VMEM(hb.shape, F32),
                               pltpu.VMEM((2,) + x3.shape[1:], BF16), pltpu.VMEM((LANES, model), F32), pltpu.VMEM((rows, model), F32), pltpu.VMEM((nsp,) + qk.shape, F32), pltpu.VMEM((ntp, 1, model), F32), pltpu.VMEM((images, model), F32),
                               dma((7,)), dma((2,)), dma((nsp - 1,)), dma((nsp,)), tps, tpr, tps, tpr, tps, tpr] + ring + [dma((9,)), dma((nsp,)), dma((2,)), dma((3, half)), dma((ntp, half)), dma((3, half)), dma((ntp, half))] + ring + ring + [tps, tpr, tps, tpr, dma((nsp - 1,)), dma((nsp,)), tps, tpr],
        compiler_params=pltpu.CompilerParams(collective_id=0, has_side_effects=True),
        name='middle',
    )(pk3, og3, qk, *vectors, hb, x3, wo, wu, wd, wv, wk, wq)


def products_kernel(heads, parts, y_ref, gpre_ref, hid_ref, og_ref, pb_ref, ga_ref, gp_ref, hbar_ref, q_ref, u_ref, gq_ref, probe_ref, pool_ref, gpr_ref, gup_ref, gdown_ref, gwo_ref, gwv_ref, gwk_ref, gwq_ref, pool_out, gpr_out):
    step = pl.program_id(0)
    gup_ref[...] = tn(y_ref[...], gpre_ref[...])
    gdown_ref[...] = tn(hid_ref[...], og_ref[...])
    tile, model = gwo_ref.shape
    width = parts * tile // heads
    part = lax.rem(step, parts)
    groups = gp_ref.shape[0]

    @pl.when(step == 0)
    def _():
        pool_out[...] = pool_ref[...]
        gpr_out[...] = gpr_ref[...].reshape(gpr_out.shape)

    @pl.when(step < parts)
    def _():
        gwo_ref[...] = tn(pb_ref[...], ga_ref[...])
        gp = jnp.concatenate([gp_ref[g].astype(F32) for g in range(groups) for _ in range(heads)], axis=0)
        keep = (iota(gp.shape, 0) // SUB) % heads == (part * tile + iota(gp.shape, 1)) // width
        gwv_ref[...] = tn(jnp.where(keep, gp, 0.0).astype(BF16), hbar_ref[...].reshape(gp.shape[0], model))

    @pl.when(step >= parts)
    def _():
        q = jnp.transpose(q_ref[...])[:, 0:1]
        head_of = (part * tile + iota((tile, model), 0)) // width
        u = jnp.zeros((tile, model), F32)
        for h in range(heads):
            u = jnp.where(head_of == h, u_ref[h:h + 1, :], u)
        gwk_ref[...] = q * u
        gq = jnp.transpose(jnp.broadcast_to(gq_ref[...], (SUB, tile)))[:, 0:1]
        gwq_ref[...] = gq * row(probe_ref)


def products(heads, y, gpre, hid, og, pb, ga, gp3, hbar, q8, u, gq, probe, pool, gpr):
    images, model = y.shape
    cols, hd = gpre.shape[1], pb.shape[1]
    parts = hd // LANES
    steps = 2 * parts
    tile = model // steps
    at = lambda a: lambda i: jnp.clip(i - parts * a, 0, parts - 1)
    lane = lambda i: lax.rem(i, parts)
    part = pl.BlockSpec((images, tile), lambda i: (0, i))
    full = lambda a: pl.BlockSpec(a.shape, lambda i: (0,) * a.ndim)
    out = pl.BlockSpec((tile, cols), lambda i: (i, 0))
    small = [pl.BlockSpec((LANES, model), lambda i, f=at(a): (f(i), 0)) for a in (0, 0, 1, 1)]
    sds = jax.ShapeDtypeStruct
    return pl.pallas_call(
        functools.partial(products_kernel, heads, parts),
        grid=(steps,),
        in_specs=[part, full(gpre), part, full(og), pl.BlockSpec((images, LANES), lambda i: (0, lane(i))), full(ga), pl.BlockSpec(gp3.shape[:2] + (LANES,), lambda i: (0, 0, lane(i))), full(hbar), pl.BlockSpec((SUB, LANES), lambda i: (0, lane(i))), full(u), pl.BlockSpec((1, LANES), lambda i: (0, lane(i))), full(probe), full(pool), full(gpr)],
        out_specs=[out, out] + small + [full(pool), full(probe)],
        out_shape=[sds((model, cols), F32), sds((cols, model), F32)] + [sds((hd, model), F32)] * 4 + [sds(pool.shape, pool.dtype), sds(probe.shape, F32)],
        name='products',
    )(y, gpre, hid, og, pb, ga, gp3, hbar, q8, u, gq, probe, pool, gpr)


def back_kernel(heads, ntp, scale, x_ref, gain_ref, bias_ref, gv_ref, qk_ref, st_ref, gx_ref, qkr):
    step = pl.program_id(0)
    rows = heads * SUB
    model = x_ref.shape[1]

    @pl.when(step == 0)
    def _():
        for t in range(ntp):
            for h in range(heads):
                hi, lo = hi_lo(jnp.broadcast_to(qk_ref[t, h:h + 1, :], (SUB, model)))
                at = (t * heads + h) * SUB
                qkr[at:at + SUB, :] = hi.astype(F32)
                qkr[LANES + at:LANES + at + SUB, :] = lo.astype(F32)

    images, tokens = SUB, x_ref.shape[0] // SUB
    hat, inv = centre(x_ref[...].astype(F32))
    gain = row(gain_ref)
    hid = (hat * gain + row(bias_ref)).astype(BF16)
    qkb = qkr[...].astype(BF16)
    gv_hi, gv_lo = hi_lo(gv_ref[...].reshape(ntp * rows, model))
    r = nt(hid, qkb)
    s = (r[:, 0:LANES] + r[:, LANES:2 * LANES]) * scale
    d = nt(hid, jnp.concatenate([gv_hi, gv_lo], axis=0))
    d = d[:, 0:LANES] + d[:, LANES:2 * LANES]
    lse = jnp.concatenate([st_ref[t, 0, :, 0:rows] for t in range(ntp)], axis=1)
    delta = jnp.concatenate([st_ref[t, 0, :, rows:2 * rows] for t in range(ntp)], axis=1)
    shape = (images, tokens, LANES)
    keep = iota(shape, 2) % SUB == iota(shape, 0)
    p = jnp.where(keep, jnp.exp(s.reshape(shape) - lse[:, None, :]), 0.0)
    ds = p * (d.reshape(shape) - delta[:, None, :]) * scale
    pb = p.astype(BF16).reshape(images * tokens, LANES)
    db = ds.astype(BF16).reshape(images * tokens, LANES)
    gh = nn(jnp.concatenate([pb, db], axis=1), jnp.concatenate([gv_hi, qkb[0:LANES]], axis=0))
    gx_ref[...] = norm_back(hat, inv, gh * gain).astype(BF16)


def back_tokens(heads, ntp, scale, x, gain, bias, gv, qk, st):
    tokens_all, model = x.shape
    groups, rows = gv.shape[1], gv.shape[2]
    block = tokens_all // groups
    full = lambda a: pl.BlockSpec(a.shape, lambda g: (0,) * a.ndim)
    return pl.pallas_call(
        functools.partial(back_kernel, heads, ntp, scale),
        grid=(groups,),
        in_specs=[pl.BlockSpec((block, model), lambda g: (g, 0)), full(gain), full(bias), pl.BlockSpec((ntp, 1, rows, model), lambda g: (0, g, 0, 0)), full(qk), pl.BlockSpec((ntp, 1) + st.shape[2:], lambda g: (0, g, 0, 0))],
        out_specs=pl.BlockSpec((block, model), lambda g: (g, 0)),
        out_shape=jax.ShapeDtypeStruct((tokens_all, model), BF16),
        scratch_shapes=[pltpu.VMEM((2 * LANES, model), F32)],
        name='back_tokens',
    )(x, gain, bias, gv, qk, st)


def local_head(nsp, ntp, encoded, enc_gain, enc_bias, probe, w_query, b_query, w_key, w_value, b_value, w_out, b_out, head_gain, head_bias, w_up, b_up, w_down, b_down, out_grad):
    images, tokens, model = encoded.shape
    heads, head_dim = b_query.shape
    hd = heads * head_dim
    scale = head_dim ** -0.5
    x = encoded.reshape(images * tokens, model)
    wq, wk, wv = (jnp.transpose(w, (1, 2, 0)).reshape(hd, model) for w in (w_query, w_key, w_value))
    wo = w_out.reshape(hd, model)
    og3 = out_grad.reshape(nsp, images // nsp, model)
    pk, hb, qk, q8 = scan_tokens(heads, images, scale, x, enc_gain, enc_bias, probe, wq, b_query, wk, wv, b_value)
    gv, hbar, st, qk_all, gp3, y3, ga3, pool3, pb3, hidden, grad_pre, u, gq, gpr = middle(heads, nsp, ntp, scale, pk, og3, qk, (b_out, head_gain, head_bias, b_up, b_down, b_value, enc_gain, enc_bias), hb, x.reshape(nsp, -1, model), wo, w_up, w_down, wv, wk, wq)
    gx = back_tokens(heads, ntp, scale, x, enc_gain, enc_bias, gv, qk_all, st)
    y, ga, pool, pooled_bf = (a.reshape(images, -1) for a in (y3, ga3, pool3, pb3))
    grad_w_up, grad_w_down, *small, pooled, grad_probe = products(heads, y, grad_pre, hidden, out_grad, pooled_bf, ga, gp3, hbar, q8, u, gq, probe, pool, gpr)
    grad_w_out, grad_wv, grad_wk, grad_wq = (a.reshape(heads, head_dim, model) for a in small)
    back = lambda a: jnp.transpose(a, (2, 0, 1))
    return (pooled, gx.reshape(encoded.shape), grad_probe, back(grad_wq), back(grad_wk), back(grad_wv), grad_w_out, grad_w_up, grad_w_down)


def solution(mesh):
    body = functools.partial(local_head, mesh.shape['sp'], mesh.shape['tp'])
    return jax.shard_map(body, mesh=mesh, in_specs=IN_SPECS, out_specs=OUT_SPECS, check_vma=False)
```

```python
import functools
import jax
import jax.numpy as jnp
from jax import lax
from jax.experimental import pallas as pl
from jax.experimental.pallas import tpu as pltpu
from jax.sharding import PartitionSpec as P

NORM_EPS = 1e-6
MESH = pl.DeviceIdType.MESH
F32, BF16 = jnp.float32, jnp.bfloat16
IN_SPECS = (P('dp', 'sp', None), P(), P(), P(), P(None, 'tp', None), P('tp', None), P(None, 'tp', None), P(None, 'tp', None), P('tp', None), P('tp', None, None), P(), P(), P(), P(None, 'tp'), P('tp'), P('tp', None), P(), P('dp', None))
OUT_SPECS = (P('dp', None), P('dp', 'sp', None), P('dp'), P('dp', 'tp', None), P('dp', 'tp', None), P('dp', 'tp', None), P(('dp', 'tp'), None, None), P('dp', 'tp'), P(('dp', 'tp'), None))
LANES = 128
SUB = 8
GELU_C = 0.7978845608028654
GELU_A = 0.044715


def nn(a, b):
    return lax.dot_general(a, b, (((1,), (0,)), ((), ())), preferred_element_type=F32)


def nt(a, b):
    return lax.dot_general(a, b, (((1,), (1,)), ((), ())), preferred_element_type=F32)


def tn(a, b):
    return lax.dot_general(a, b, (((0,), (0,)), ((), ())), preferred_element_type=F32)


def hi_lo(a):
    hi = a.astype(BF16)
    return hi, (a - hi.astype(F32)).astype(BF16)


def iota(shape, dim):
    return lax.broadcasted_iota(jnp.int32, shape, dim)


def by_head(parts, width):
    rows, cols = parts[0].shape[0], len(parts) * width
    block = iota((rows, cols), 1) // width
    out = jnp.zeros((rows, cols), F32)
    for h, part in enumerate(parts):
        out = jnp.where(block == h, part, out)
    return out


def row(ref):
    return ref[...].reshape(1, -1)


def flat(ref):
    heads, width = ref.shape
    wide = jnp.concatenate([ref[...]] * heads, axis=1)
    keep = iota(wide.shape, 0) == iota(wide.shape, 1) // width
    return jnp.sum(jnp.where(keep, wide, 0.0), axis=0, keepdims=True)


def gelu_parts(pre):
    t = jnp.tanh(GELU_C * (pre + GELU_A * pre * pre * pre))
    value = 0.5 * pre * (1.0 + t)
    slope = 0.5 * (1.0 + t) + 0.5 * pre * (1.0 - t * t) * (GELU_C * (1.0 + 3.0 * GELU_A * pre * pre))
    return value, slope


def centre(rows):
    mean = jnp.mean(rows, axis=-1, keepdims=True)
    centred = rows - mean
    inv = lax.rsqrt(jnp.mean(centred * centred, axis=-1, keepdims=True) + NORM_EPS)
    return centred * inv, inv, mean


def norm_back(hat, inv, cot):
    return inv * (cot - jnp.mean(cot, axis=-1, keepdims=True) - hat * jnp.mean(cot * hat, axis=-1, keepdims=True))


def barrier_all(peers):
    sem = pltpu.get_barrier_semaphore()
    for axis, dev in peers:
        pl.semaphore_signal(sem, inc=1, device_id={axis: dev}, device_id_type=MESH)
    pl.semaphore_wait(sem, len(peers))


def peers_of(axis, n):
    me = lax.axis_index(axis)
    return me, [lax.rem(me + k, n) for k in range(1, n)]


def remote(src, dst, send_sem, recv_sem, axis, dev):
    return pltpu.make_async_remote_copy(src_ref=src, dst_ref=dst, send_sem=send_sem, recv_sem=recv_sem, device_id={axis: dev}, device_id_type=MESH)


def gather_start(buf, me, peers, send_sems, recv_sems, axis):
    for k, dev in enumerate(peers):
        remote(buf.at[me], buf.at[me], send_sems.at[k], recv_sems.at[me], axis, dev).start()


def gather_wait(buf, me, peers, send_sems, recv_sems, axis):
    for k, dev in enumerate(peers):
        remote(buf.at[dev], buf.at[dev], send_sems.at[k], recv_sems.at[dev], axis, dev).wait_recv()
    for k, dev in enumerate(peers):
        remote(buf.at[me], buf.at[me], send_sems.at[k], recv_sems.at[me], axis, dev).wait_send()


class ChipRing:
    def __init__(self, nsp):
        me = lax.axis_index('sp')
        self.me, self.core = me, lax.rem(me, 2)
        self.mate = me + 1 - 2 * self.core
        self.up, self.down, self.far = (lax.rem(me + k, nsp) for k in (2, nsp - 2, 4))
        self.mates = [lax.rem(self.mate + k, nsp) for k in (2, nsp - 2, 4)]
        self.around = [self.mate, self.up, self.down, self.far] + self.mates

    def start(self, buf, send, recv):
        for k, dev in enumerate((self.mate, self.up, self.down)):
            remote(buf.at[self.me], buf.at[self.me], send.at[k], recv.at[self.me], 'sp', dev).start()

    def relay(self, buf, send, recv, upward):
        for k, dev in ((3, self.down), (4, self.up)):
            remote(buf.at[dev], buf.at[dev], send.at[k], recv.at[dev], 'sp', dev).wait_recv()
            if upward == (k == 3):
                remote(buf.at[dev], buf.at[dev], send.at[5], recv.at[dev], 'sp', self.up if upward else self.down).start()
            remote(buf.at[dev], buf.at[dev], send.at[k], recv.at[dev], 'sp', self.mate).start()

    def finish(self, buf, send, recv, upward):
        far = self.far
        remote(buf.at[far], buf.at[far], send.at[6], recv.at[far], 'sp', self.mate).wait_recv()
        remote(buf.at[far], buf.at[far], send.at[6], recv.at[far], 'sp', self.mate).start()
        for dev in [self.mate] + self.mates:
            remote(buf.at[dev], buf.at[dev], send.at[0], recv.at[dev], 'sp', self.mate).wait_recv()
        via = self.down if upward else self.up
        for k, slot in ((0, self.me), (1, self.me), (2, self.me), (3, self.down), (4, self.up), (5, via), (6, far)):
            remote(buf.at[slot], buf.at[slot], send.at[k], recv.at[slot], 'sp', self.mate).wait_send()


RING_SEMS = 7


def scan_kernel(heads, scale, x_ref, gain_ref, bias_ref, probe_ref, wq_ref, bq_ref, wk_ref, wv_ref, bv_ref, pk_ref, hb_ref, qk_ref, q_ref, h_ref, ms_ref, qkr, hball):
    rows = heads * SUB
    width = wq_ref.shape[0] // heads

    @pl.when(pl.program_id(0) == 0)
    def _():
        probe8 = jnp.broadcast_to(row(probe_ref), (SUB, probe_ref.shape[0])).astype(BF16)
        q8 = (nt(probe8, wq_ref[...]) + flat(bq_ref)).astype(BF16)
        q_ref[...] = q8.astype(F32)
        qs = jnp.concatenate([q8.astype(F32)] * heads, axis=0)
        qs = jnp.where(iota(qs.shape, 0) // SUB == iota(qs.shape, 1) // width, qs, 0.0).astype(BF16)
        qk = nn(qs, wk_ref[...])
        hi, lo = hi_lo(qk)
        qkr[...] = jnp.zeros(qkr.shape, BF16)
        qkr[0:rows, :] = hi
        qkr[LANES // 2:LANES // 2 + rows, :] = lo
        for h in range(heads):
            qk_ref[h:h + 1, :] = qk[SUB * h:SUB * h + 1, :]

    step = pl.program_id(0)
    images, tokens = SUB, x_ref.shape[0] // SUB
    hat, inv, mean = centre(x_ref[...].astype(F32))
    hid = (hat * row(gain_ref) + row(bias_ref)).astype(BF16)
    h_ref[...] = hid
    which = iota((x_ref.shape[0], LANES), 1)
    ms_ref[...] = jnp.where(which == 0, mean, inv)
    r = nt(hid, qkr[...])
    s = ((r + pltpu.roll(r, LANES // 2, 1)) * scale).reshape(images, tokens, LANES)
    m = jnp.max(s, axis=1)
    e = jnp.exp(s - m[:, None, :])
    l = jnp.sum(e, axis=1)
    lane, img = iota(e.shape, 2), iota(e.shape, 0)
    ebd = jnp.where((lane % SUB == img) & (lane < rows), e, 0.0).astype(BF16).reshape(images * tokens, LANES)
    hb = tn(ebd, hid)[0:rows, :]
    hb_ref[0, :, :] = hb
    hball[step] = hb
    cols = wq_ref.shape[0]
    mine = pl.ds(pl.multiple_of(step * SUB, SUB), SUB)
    pk_ref[mine, cols:cols + LANES] = m
    pk_ref[mine, cols + LANES:cols + 2 * LANES] = l

    @pl.when(step == pl.num_programs(0) - 1)
    def _():
        groups = hball.shape[0]
        every = groups * rows
        hi, lo = hi_lo(hball[...].reshape(every, hball.shape[2]))
        v = nt(hi, wv_ref[...]) + nt(lo, wv_ref[...])
        bias = flat(bv_ref)
        for g in range(groups):
            vs = by_head([v[g * rows + SUB * h:g * rows + SUB * h + SUB] for h in range(heads)], width)
            tot = pk_ref[g * SUB:g * SUB + SUB, cols + LANES:cols + 2 * LANES]
            pk_ref[g * SUB:g * SUB + SUB, 0:cols] = vs + by_head([tot[:, SUB * h:SUB * h + 1] for h in range(heads)], width) * bias


def scan_tokens(heads, images, scale, x, gain, bias, probe, wq, bq, wk, wv, bv):
    tokens_all, width = x.shape
    hd = wq.shape[0]
    groups = images // SUB
    block = tokens_all // groups
    full = lambda a: pl.BlockSpec(a.shape, lambda g: (0,) * a.ndim)
    return pl.pallas_call(
        functools.partial(scan_kernel, heads, scale),
        grid=(groups,),
        in_specs=[pl.BlockSpec((block, width), lambda g: (g, 0))] + [full(a) for a in (gain, bias, probe, wq, bq, wk, wv, bv)],
        out_specs=[pl.BlockSpec((images, hd + 2 * LANES), lambda g: (0, 0)), pl.BlockSpec((1, heads * SUB, width), lambda g: (g, 0, 0)), pl.BlockSpec((heads, width), lambda g: (0, 0)), pl.BlockSpec((SUB, hd), lambda g: (0, 0)), pl.BlockSpec((block, width), lambda g: (g, 0)), pl.BlockSpec((block, LANES), lambda g: (g, 0))],
        out_shape=[jax.ShapeDtypeStruct((images, hd + 2 * LANES), F32), jax.ShapeDtypeStruct((groups, heads * SUB, width), F32), jax.ShapeDtypeStruct((heads, width), F32), jax.ShapeDtypeStruct((SUB, hd), F32), jax.ShapeDtypeStruct(x.shape, BF16), jax.ShapeDtypeStruct((tokens_all, LANES), F32)],
        scratch_shapes=[pltpu.VMEM((LANES, width), BF16), pltpu.VMEM((groups, heads * SUB, width), F32)],
        name='scan_tokens',
    )(x, gain, bias, probe, wq, bq, wk, wv, bv)


def middle_kernel(heads, nsp, ntp, scale, pk_ref, og_ref, qk_ref, bo_ref, hg_ref, hb_ref, bu_ref, bd_ref, bv_ref, hb_hbm, x_hbm, wo_hbm, wu_hbm, wd_hbm, wv_hbm, wk_hbm, wq_hbm,
                  gv_out, hbar_out, st_out, qk_out, gp_out, y_out, ga_out, pool_out, pb_out, hid_out, gpre_out, u_out, gq_out, gpr_out,
                  wo, wu, wd, wv, wk, wq, rbuf, ta, tg, td, ag, hr, relay, pa, ha, sg, xb, rhs, uacc, ub, prb, ghb,
                  wsem, xsem, rs_send, rs_recv, ta_s, ta_r, tg_s, tg_r, td_s, td_r, ag_s, ag_r, hr_s, hr_r, rl_r, gv_s, gv_r, fw_s, fw_r, pa_s, pa_r, ha_s, ha_r, st_s, st_r, qk_s, qk_r, ub_s, ub_r, pr_s, pr_r, sy_s, sy_r, sg_s, sg_r):
    sp, sp_peers = peers_of('sp', nsp)
    tp, tp_peers = peers_of('tp', ntp)
    ring = ChipRing(nsp)
    core, mate = ring.core, ring.mate
    loads = [pltpu.make_async_copy(a, b, wsem.at[i]) for i, (a, b) in enumerate(((wd_hbm, wd), (wo_hbm, wo), (wu_hbm, wu), (hb_hbm.at[sp], hr.at[sp]), (wv_hbm, wv), (wk_hbm, wk), (wq_hbm, wq)))]
    for load in loads:
        load.start()
    sem = pltpu.get_barrier_semaphore()
    for axis, devs in (('sp', sp_peers), ('tp', tp_peers)):
        for dev in devs:
            pl.semaphore_signal(sem, inc=1, device_id={axis: dev}, device_id_type=MESH)

    def x_load(g):
        return pltpu.make_async_copy(x_hbm.at[g], xb.at[g % 2], xsem.at[g % 2])

    x_load(0).start()
    x_load(1).start()
    hd = wo.shape[0]
    width = hd // heads
    model = wu.shape[0]
    rows = heads * SUB
    images = nsp * SUB
    qk_out[tp] = qk_ref[...]
    rbuf[sp] = pk_ref[sp]
    for h in range(heads):
        hi, lo = hi_lo(jnp.broadcast_to(qk_ref[h:h + 1, :], (SUB, model)))
        rhs[h * SUB:h * SUB + SUB, :] = hi.astype(F32)
        rhs[2 * rows + h * SUB:2 * rows + h * SUB + SUB, :] = lo.astype(F32)
    og = og_ref[sp]
    pl.semaphore_wait(sem, len(sp_peers) + len(tp_peers))

    sends = []
    for k, dev in enumerate(sp_peers):
        sends.append(remote(pk_ref.at[dev], rbuf.at[sp], rs_send.at[k], rs_recv.at[sp], 'sp', dev))
        sends[-1].start()
    far0, far1 = ring.far - core, ring.far - core + 1
    late = [remote(hb_hbm.at[far0], relay.at[0], hr_s.at[0], rl_r.at[0], 'sp', ring.up), remote(hb_hbm.at[far1], relay.at[1], hr_s.at[1], rl_r.at[1], 'sp', ring.down)]
    for k, dev in enumerate((ring.up, ring.down, ring.mates[0], ring.mates[1], mate)):
        late.append(remote(hb_hbm.at[dev], hr.at[sp], hr_s.at[2 + k], hr_r.at[sp], 'sp', dev))
    for send in late:
        send.start()
    gather_start(qk_out, tp, tp_peers, qk_s, qk_r, 'tp')
    loads[0].wait()
    gh = nt(og, wd[...])
    for k, dev in enumerate(sp_peers):
        remote(rbuf.at[dev], rbuf.at[dev], rs_send.at[k], rs_recv.at[dev], 'sp', dev).wait_recv()
    for send in sends:
        send.wait_send()
    m = rbuf[0, :, hd:hd + LANES]
    for j in range(1, nsp):
        m = jnp.maximum(m, rbuf[j, :, hd:hd + LANES])
    l = jnp.zeros_like(m)
    v = jnp.zeros((SUB, hd), F32)
    for j in range(nsp):
        w = jnp.exp(rbuf[j, :, hd:hd + LANES] - m)
        l = l + w * rbuf[j, :, hd + LANES:hd + 2 * LANES]
        v = v + by_head([w[:, SUB * h:SUB * h + 1] for h in range(heads)], width) * rbuf[j, :, 0:hd]
    o = v / by_head([l[:, SUB * h:SUB * h + 1] for h in range(heads)], width)
    pooled_bf = o.astype(BF16)
    lse = m + jnp.log(l)

    loads[1].wait()
    ta[tp] = nn(pooled_bf, wo[...])
    gather_start(ta, tp, tp_peers, ta_s, ta_r, 'tp')
    for k, (src, dst) in enumerate(((ring.down, ring.up - core), (ring.up, ring.down - core + 1))):
        remote(relay.at[k], relay.at[k], hr_s.at[k], rl_r.at[k], 'sp', src).wait_recv()
        late.append(remote(relay.at[k], hr.at[src], hr_s.at[7 + k], hr_r.at[src], 'sp', dst))
        late[-1].start()
    loads[2].wait()
    gather_wait(ta, tp, tp_peers, ta_s, ta_r, 'tp')
    attn = ta[0]
    for t in range(1, ntp):
        attn = attn + ta[t]
    attn = attn + row(bo_ref)
    hat, inv, _ = centre(attn)
    gain = row(hg_ref)
    y = (hat * gain + row(hb_ref)).astype(BF16)
    value, slope = gelu_parts(nn(y, wu[...]) + row(bu_ref))
    tg[tp] = nt((gh * slope).astype(BF16), wu[...])
    gather_start(tg, tp, tp_peers, tg_s, tg_r, 'tp')
    td[tp] = nn(value.astype(BF16), wd[...])
    gather_start(td, tp, tp_peers, td_s, td_r, 'tp')
    gather_wait(tg, tp, tp_peers, tg_s, tg_r, 'tp')
    gno = tg[0]
    for t in range(1, ntp):
        gno = gno + tg[t]
    ga = (og.astype(F32) + norm_back(hat, inv, gno * gain)).astype(BF16)
    gp = nt(ga, wo[...]).astype(BF16).astype(F32)
    prod = gp * (o - flat(bv_ref))
    head_of = iota(prod.shape, 1) // width
    delta = by_head([jnp.sum(jnp.where(head_of == h, prod, 0.0), axis=1, keepdims=True) for h in range(heads)], SUB)
    ag[sp, :, 0:hd] = gp
    ag[sp, :, hd:hd + LANES] = jnp.concatenate([lse[:, 0:rows], delta, jnp.zeros((SUB, LANES - 2 * rows), F32)], axis=1)
    gather_start(ag, sp, sp_peers, ag_s, ag_r, 'sp')

    gather_wait(td, tp, tp_peers, td_s, td_r, 'tp')
    down = td[0]
    for t in range(1, ntp):
        down = down + td[t]
    pa[sp, :, 0:model] = y.astype(F32)
    pa[sp, :, model:2 * model] = (attn + down + row(bd_ref)).astype(BF16).astype(F32)
    pa[sp, :, 2 * model:3 * model] = ga.astype(F32)
    pa[sp, :, 3 * model:3 * model + hd] = pooled_bf.astype(F32)
    gather_wait(ag, sp, sp_peers, ag_s, ag_r, 'sp')
    ring.start(pa, pa_s, pa_r)

    loads[4].wait()
    st_out[tp] = ag[:, :, hd:hd + LANES]
    near_up, near_down, far_tp = lax.rem(tp + 1, ntp), lax.rem(tp + ntp - 1, ntp), lax.rem(tp + 2, ntp)
    half = nsp // 2
    direct = half - sg.shape[2]
    gp_out[...] = ag[:, :, 0:hd].astype(BF16)

    def make_gv(first):
        part = jnp.concatenate([ag[first + i, :, 0:hd] for i in range(half) for _ in range(heads)], axis=0)
        keep = (iota(part.shape, 0) // SUB) % heads == iota(part.shape, 1) // width
        gv_out[tp, pl.ds(first, half)] = nn(jnp.where(keep, part, 0.0).astype(BF16), wv[...]).reshape(half, rows, model)

    def piece(i, owner):
        return gv_out.at[owner, core * half + i]

    def send_gv(i, k, owner, dev):
        return remote(piece(i, owner), piece(i, owner), gv_s.at[k, i], gv_r.at[owner, i], 'tp', dev)

    def forward(i, k, owner):
        return remote(piece(i, owner), piece(i, owner), fw_s.at[k, i], fw_r.at[owner, i], 'sp', mate)

    def near(i):
        for k, owner in ((0, near_down), (1, near_up)):
            send_gv(i, k, owner, owner).wait_recv()
            if k == i % 2:
                send_gv(i, 2, owner, near_down if k else near_up).start()
            forward(i, k, owner).start()

    def beyond(i):
        send_gv(i, 2, far_tp, far_tp).wait_recv()
        forward(i, 2, far_tp).start()

    def send_shared(k):
        block = pl.ds(pl.multiple_of((sp // 2) * SUB, SUB), SUB)
        return remote(gv_out.at[tp, pl.ds(core * half + direct, half - direct), block], sg.at[sp, ntp - 1 - k], sy_s.at[k - 1], sy_r.at[ntp - 1 - k], 'tp', lax.rem(tp + k, ntp))

    make_gv(core * half)
    for k in range(1, ntp):
        send_shared(k).start()
    for i in range(direct):
        send_gv(i, 0, tp, near_up).start()
        send_gv(i, 1, tp, near_down).start()
        if i == 0:
            gather_start(st_out, tp, tp_peers, st_s, st_r, 'tp')
    make_gv((1 - core) * half)
    loads[3].wait()
    for k, dev in enumerate(sp_peers):
        remote(hr.at[dev], hr.at[dev], hr_s.at[k], hr_r.at[dev], 'sp', dev).wait_recv()
    for send in late:
        send.wait_send()
    hbar = jnp.zeros(hr.shape[1:], F32)
    for j in range(nsp):
        w = jnp.exp(rbuf[j, :, hd:hd + LANES] - lse)
        hbar = hbar + hr[j] * jnp.concatenate([w[:, SUB * h:SUB * h + 1] for h in range(heads)], axis=0)
    ha[sp] = hbar
    ring.start(ha, ha_s, ha_r)

    uacc[...] = jnp.zeros(uacc.shape, F32)

    def u_step(g):
        x_load(g).wait()
        tokens = xb.shape[1] // SUB
        hidden = xb[g % 2]
        hi, lo = hi_lo(gv_out[tp, g])
        rhs[rows:2 * rows, :] = hi.astype(F32)
        rhs[3 * rows:4 * rows, :] = lo.astype(F32)
        r = nt(hidden, rhs[...].astype(BF16))
        r = (r + pltpu.roll(r, LANES // 2, 1)).reshape(SUB, tokens, LANES)
        lane, img = iota(r.shape, 2), iota(r.shape, 0)
        r = r * jnp.where(lane < rows, scale, 1.0) - ag[g, :, hd:hd + LANES][:, None, :]
        r = r.reshape(SUB * tokens, LANES)
        grad = (jnp.exp(r) * pltpu.roll(r, LANES - rows, 1) * scale).reshape(SUB, tokens, LANES)
        ds = jnp.where((lane % SUB == img) & (lane < rows), grad, 0.0).astype(BF16).reshape(SUB * tokens, LANES)
        uacc[...] += tn(ds, hidden)[0:rows, :]
        if g + 2 < nsp:
            x_load(g + 2).start()

    u_step(0)
    u_step(1)
    u_step(2)
    ring.relay(pa, pa_s, pa_r, False)
    for k in range(1, ntp):
        remote(sg.at[sp, k - 1], sg.at[sp, k - 1], sy_s.at[0], sy_r.at[k - 1], 'tp', near_up).wait_recv()
    ring.start(sg, sg_s, sg_r)
    u_step(3)
    u_step(4)
    near(0)
    u_step(5)
    u_step(6)
    ring.finish(pa, pa_s, pa_r, False)
    ring.relay(ha, ha_s, ha_r, True)
    u_step(7)
    for h in range(heads):
        ub[sp, h:h + 1, :] = jnp.sum(uacc[SUB * h:SUB * h + SUB, :], axis=0, keepdims=True)
    gather_start(ub, sp, sp_peers, ub_s, ub_r, 'sp')

    near(1)
    ghb[...] = nt(og_ref[...].reshape(images, model), wd[...])
    y_all = pa[:, :, 0:model].astype(BF16)
    y_out[...] = y_all
    pool_out[...] = pa[:, :, model:2 * model].astype(BF16)
    ga_out[...] = pa[:, :, 2 * model:3 * model].astype(BF16)
    pb_out[...] = pa[:, :, 3 * model:3 * model + hd].astype(BF16)
    value, slope = gelu_parts(nn(y_all.reshape(images, model), wu[...]) + row(bu_ref))
    gpre_out[...] = (ghb[...] * slope).astype(BF16)
    hid_out[...] = value.astype(BF16)
    ring.relay(sg, sg_s, sg_r, False)
    near(2)

    gather_wait(ub, sp, sp_peers, ub_s, ub_r, 'sp')
    u = ub[0]
    for j in range(1, nsp):
        u = u + ub[j]
    u_out[...] = u
    loads[5].wait()
    loads[6].wait()
    hi, lo = hi_lo(u)
    gq = nt(jnp.concatenate([hi, lo], axis=0), wk[...])
    gq = gq[0:heads] + gq[heads:2 * heads]
    gq = jnp.sum(jnp.where(iota(gq.shape, 0) == iota(gq.shape, 1) // width, gq, 0.0), axis=0, keepdims=True)
    gq_out[...] = gq
    hi, lo = hi_lo(gq)
    gpr = nn(jnp.concatenate([hi, lo], axis=0), wq[...])
    prb[tp] = gpr[0:1] + gpr[1:2]
    gather_start(prb, tp, tp_peers, pr_s, pr_r, 'tp')
    beyond(0)
    ring.finish(ha, ha_s, ha_r, True)
    hbar_out[...] = ha[...].astype(BF16)
    beyond(1)
    ring.finish(sg, sg_s, sg_r, False)
    for j in range(nsp):
        for k in range(1, ntp):
            gv_out[lax.rem(tp + k, ntp), (j % 2) * half + direct:(j % 2) * half + half, (j // 2) * SUB:(j // 2) * SUB + SUB, :] = sg[j, k - 1]
    beyond(2)
    for k in range(1, ntp):
        send_shared(k).wait_send()
    for i in range(direct):
        other = (1 - core) * half + i
        for k, (owner, dev) in enumerate(((tp, near_up), (tp, near_down), (near_up if i % 2 else near_down, near_down if i % 2 else near_up))):
            send_gv(i, k, owner, dev).wait_send()
        for k, owner in enumerate((near_down, near_up, far_tp)):
            forward(i, k, owner).wait_send()
            remote(gv_out.at[owner, other], gv_out.at[owner, other], fw_s.at[k, i], fw_r.at[owner, i], 'sp', mate).wait_recv()
    gather_wait(st_out, tp, tp_peers, st_s, st_r, 'tp')
    gather_wait(qk_out, tp, tp_peers, qk_s, qk_r, 'tp')
    gather_wait(prb, tp, tp_peers, pr_s, pr_r, 'tp')
    total = prb[0]
    for t in range(1, ntp):
        total = total + prb[t]
    gpr_out[...] = total


def middle(heads, nsp, ntp, scale, pk, og3, qk, vectors, hb, x3, wo, wu, wd, wv, wk, wq):
    own, model = og3.shape[1:]
    hd = wo.shape[0]
    rows = hb.shape[1]
    images = nsp * own
    half = nsp // 2
    pk3 = pk.reshape(nsp, own, pk.shape[1])
    vm, hbm = pl.BlockSpec(memory_space=pltpu.VMEM), pl.BlockSpec(memory_space=pl.ANY)
    dma = pltpu.SemaphoreType.DMA
    sds = jax.ShapeDtypeStruct
    part = pltpu.VMEM((ntp, own, model), F32)
    wide = [pltpu.VMEM(w.shape, BF16) for w in (wo, wu, wd, wv, wk, wq)]
    ring, tps, tpr = [dma((RING_SEMS,)), dma((nsp,))], dma((ntp - 1,)), dma((ntp,))
    return pl.pallas_call(
        functools.partial(middle_kernel, heads, nsp, ntp, scale),
        in_specs=[vm] * 9 + [hbm] * 8,
        out_specs=[vm] * 14,
        out_shape=[sds((ntp, nsp, rows, model), F32), sds((nsp, rows, model), BF16), sds((ntp, nsp, own, LANES), F32), sds((ntp,) + qk.shape, F32), sds((nsp, own, hd), BF16),
                   sds((nsp, own, model), BF16), sds((nsp, own, model), BF16), sds((nsp, own, model), BF16), sds((nsp, own, hd), BF16), sds((images, model), BF16), sds((images, model), BF16), sds(qk.shape, F32), sds((1, hd), F32), sds((1, model), F32)],
        scratch_shapes=wide + [pltpu.VMEM(pk3.shape, F32), part, part, part, pltpu.VMEM((nsp, own, hd + LANES), F32), pltpu.VMEM(hb.shape, F32), pltpu.VMEM((2,) + hb.shape[1:], F32), pltpu.VMEM((nsp, own, 3 * model + hd), F32), pltpu.VMEM(hb.shape, F32), pltpu.VMEM((nsp, ntp - 1, 1, own, model), F32),
                               pltpu.VMEM((2,) + x3.shape[1:], BF16), pltpu.VMEM((LANES, model), F32), pltpu.VMEM((rows, model), F32), pltpu.VMEM((nsp,) + qk.shape, F32), pltpu.VMEM((ntp, 1, model), F32), pltpu.VMEM((images, model), F32),
                               dma((7,)), dma((2,)), dma((nsp - 1,)), dma((nsp,)), tps, tpr, tps, tpr, tps, tpr, dma((nsp - 1,)), dma((nsp,))] + [dma((9,)), dma((nsp,)), dma((2,)), dma((3, half)), dma((ntp, half)), dma((3, half)), dma((ntp, half))] + ring + ring + [tps, tpr, tps, tpr, dma((nsp - 1,)), dma((nsp,)), tps, tpr, tps, tpr] + ring,
        compiler_params=pltpu.CompilerParams(collective_id=0, has_side_effects=True),
        name='middle',
    )(pk3, og3, qk, *vectors, hb, x3, wo, wu, wd, wv, wk, wq)


def products_kernel(heads, parts, y_ref, gpre_ref, hid_ref, og_ref, pb_ref, ga_ref, gp_ref, hbar_ref, q_ref, u_ref, gq_ref, probe_ref, pool_ref, gpr_ref, gup_ref, gdown_ref, gwo_ref, gwv_ref, gwk_ref, gwq_ref, pool_out, gpr_out):
    step = pl.program_id(0)
    gup_ref[...] = tn(y_ref[...], gpre_ref[...])
    gdown_ref[...] = tn(hid_ref[...], og_ref[...])
    tile, model = gwo_ref.shape
    width = parts * tile // heads
    part = lax.rem(step, parts)
    groups = gp_ref.shape[0]

    @pl.when(step == 0)
    def _():
        pool_out[...] = pool_ref[...]
        gpr_out[...] = gpr_ref[...].reshape(gpr_out.shape)

    @pl.when(step < parts)
    def _():
        gwo_ref[...] = tn(pb_ref[...], ga_ref[...])
        gp = jnp.concatenate([gp_ref[g].astype(F32) for g in range(groups) for _ in range(heads)], axis=0)
        keep = (iota(gp.shape, 0) // SUB) % heads == (part * tile + iota(gp.shape, 1)) // width
        gwv_ref[...] = tn(jnp.where(keep, gp, 0.0).astype(BF16), hbar_ref[...].reshape(gp.shape[0], model))

    @pl.when(step >= parts)
    def _():
        q = jnp.transpose(q_ref[...])[:, 0:1]
        head_of = (part * tile + iota((tile, model), 0)) // width
        u = jnp.zeros((tile, model), F32)
        for h in range(heads):
            u = jnp.where(head_of == h, u_ref[h:h + 1, :], u)
        gwk_ref[...] = q * u
        gq = jnp.transpose(jnp.broadcast_to(gq_ref[...], (SUB, tile)))[:, 0:1]
        gwq_ref[...] = gq * row(probe_ref)


def products(heads, y, gpre, hid, og, pb, ga, gp3, hbar, q8, u, gq, probe, pool, gpr):
    images, model = y.shape
    cols, hd = gpre.shape[1], pb.shape[1]
    parts = hd // LANES
    steps = 2 * parts
    tile = model // steps
    at = lambda a: lambda i: jnp.clip(i - parts * a, 0, parts - 1)
    lane = lambda i: lax.rem(i, parts)
    part = pl.BlockSpec((images, tile), lambda i: (0, i))
    full = lambda a: pl.BlockSpec(a.shape, lambda i: (0,) * a.ndim)
    out = pl.BlockSpec((tile, cols), lambda i: (i, 0))
    small = [pl.BlockSpec((LANES, model), lambda i, f=at(a): (f(i), 0)) for a in (0, 0, 1, 1)]
    sds = jax.ShapeDtypeStruct
    return pl.pallas_call(
        functools.partial(products_kernel, heads, parts),
        grid=(steps,),
        in_specs=[part, full(gpre), part, full(og), pl.BlockSpec((images, LANES), lambda i: (0, lane(i))), full(ga), pl.BlockSpec(gp3.shape[:2] + (LANES,), lambda i: (0, 0, lane(i))), full(hbar), pl.BlockSpec((SUB, LANES), lambda i: (0, lane(i))), full(u), pl.BlockSpec((1, LANES), lambda i: (0, lane(i))), full(probe), full(pool), full(gpr)],
        out_specs=[out, out] + small + [full(pool), full(probe)],
        out_shape=[sds((model, cols), F32), sds((cols, model), F32)] + [sds((hd, model), F32)] * 4 + [sds(pool.shape, pool.dtype), sds(probe.shape, F32)],
        name='products',
    )(y, gpre, hid, og, pb, ga, gp3, hbar, q8, u, gq, probe, pool, gpr)


def back_kernel(heads, ntp, scale, x_ref, h_ref, ms_ref, gain_ref, gv_ref, qk_ref, st_ref, gx_ref, qkr):
    step = pl.program_id(0)
    rows = heads * SUB
    model = x_ref.shape[1]

    @pl.when(step == 0)
    def _():
        for t in range(ntp):
            for h in range(heads):
                hi, lo = hi_lo(jnp.broadcast_to(qk_ref[t, h:h + 1, :], (SUB, model)))
                at = (t * heads + h) * SUB
                qkr[at:at + SUB, :] = hi.astype(F32)
                qkr[LANES + at:LANES + at + SUB, :] = lo.astype(F32)

    images, tokens = SUB, x_ref.shape[0] // SUB
    inv = ms_ref[:, 1:2]
    hat = (x_ref[...].astype(F32) - ms_ref[:, 0:1]) * inv
    gain = row(gain_ref)
    hid = h_ref[...]
    qkb = qkr[...].astype(BF16)
    gv_hi, gv_lo = hi_lo(gv_ref[...].reshape(ntp * rows, model))
    r = nt(hid, qkb)
    s = (r[:, 0:LANES] + r[:, LANES:2 * LANES]) * scale
    d = nt(hid, jnp.concatenate([gv_hi, gv_lo], axis=0))
    d = d[:, 0:LANES] + d[:, LANES:2 * LANES]
    lse = jnp.concatenate([st_ref[t, 0, :, 0:rows] for t in range(ntp)], axis=1)
    delta = jnp.concatenate([st_ref[t, 0, :, rows:2 * rows] for t in range(ntp)], axis=1)
    shape = (images, tokens, LANES)
    keep = iota(shape, 2) % SUB == iota(shape, 0)
    p = jnp.where(keep, jnp.exp(s.reshape(shape) - lse[:, None, :]), 0.0)
    ds = p * (d.reshape(shape) - delta[:, None, :]) * scale
    pb = p.astype(BF16).reshape(images * tokens, LANES)
    db = ds.astype(BF16).reshape(images * tokens, LANES)
    gh = nn(jnp.concatenate([pb, db], axis=1), jnp.concatenate([gv_hi, qkb[0:LANES]], axis=0))
    gx_ref[...] = norm_back(hat, inv, gh * gain).astype(BF16)


def back_tokens(heads, ntp, scale, x, h, ms, gain, gv, qk, st):
    tokens_all, model = x.shape
    groups, rows = gv.shape[1], gv.shape[2]
    block = tokens_all // groups
    full = lambda a: pl.BlockSpec(a.shape, lambda g: (0,) * a.ndim)
    return pl.pallas_call(
        functools.partial(back_kernel, heads, ntp, scale),
        grid=(groups,),
        in_specs=[pl.BlockSpec((block, model), lambda g: (g, 0)), pl.BlockSpec((block, model), lambda g: (g, 0)), pl.BlockSpec((block, LANES), lambda g: (g, 0)), full(gain), pl.BlockSpec((ntp, 1, rows, model), lambda g: (0, g, 0, 0)), full(qk), pl.BlockSpec((ntp, 1) + st.shape[2:], lambda g: (0, g, 0, 0))],
        out_specs=pl.BlockSpec((block, model), lambda g: (g, 0)),
        out_shape=jax.ShapeDtypeStruct((tokens_all, model), BF16),
        scratch_shapes=[pltpu.VMEM((2 * LANES, model), F32)],
        name='back_tokens',
    )(x, h, ms, gain, gv, qk, st)


def local_head(nsp, ntp, encoded, enc_gain, enc_bias, probe, w_query, b_query, w_key, w_value, b_value, w_out, b_out, head_gain, head_bias, w_up, b_up, w_down, b_down, out_grad):
    images, tokens, model = encoded.shape
    heads, head_dim = b_query.shape
    hd = heads * head_dim
    scale = head_dim ** -0.5
    x = encoded.reshape(images * tokens, model)
    wq, wk, wv = (jnp.transpose(w, (1, 2, 0)).reshape(hd, model) for w in (w_query, w_key, w_value))
    wo = w_out.reshape(hd, model)
    og3 = out_grad.reshape(nsp, images // nsp, model)
    pk, hb, qk, q8, h, ms = scan_tokens(heads, images, scale, x, enc_gain, enc_bias, probe, wq, b_query, wk, wv, b_value)
    gv, hbar, st, qk_all, gp3, y3, ga3, pool3, pb3, hidden, grad_pre, u, gq, gpr = middle(heads, nsp, ntp, scale, pk, og3, qk, (b_out, head_gain, head_bias, b_up, b_down, b_value), hb, h.reshape(nsp, -1, model), wo, w_up, w_down, wv, wk, wq)
    gx = back_tokens(heads, ntp, scale, x, h, ms, enc_gain, gv, qk_all, st)
    y, ga, pool, pooled_bf = (a.reshape(images, -1) for a in (y3, ga3, pool3, pb3))
    grad_w_up, grad_w_down, *small, pooled, grad_probe = products(heads, y, grad_pre, hidden, out_grad, pooled_bf, ga, gp3, hbar, q8, u, gq, probe, pool, gpr)
    grad_w_out, grad_wv, grad_wk, grad_wq = (a.reshape(heads, head_dim, model) for a in small)
    back = lambda a: jnp.transpose(a, (2, 0, 1))
    return (pooled, gx.reshape(encoded.shape), grad_probe, back(grad_wq), back(grad_wk), back(grad_wv), grad_w_out, grad_w_up, grad_w_down)


def solution(mesh):
    body = functools.partial(local_head, mesh.shape['sp'], mesh.shape['tp'])
    return jax.shard_map(body, mesh=mesh, in_specs=IN_SPECS, out_specs=OUT_SPECS, check_vma=False)
```

```python
import functools
import jax
import jax.numpy as jnp
from jax import lax
from jax.experimental import pallas as pl
from jax.experimental.pallas import tpu as pltpu
from jax.sharding import PartitionSpec as P

NORM_EPS = 1e-6
MESH = pl.DeviceIdType.MESH
F32, BF16 = jnp.float32, jnp.bfloat16
IN_SPECS = (P('dp', 'sp', None), P(), P(), P(), P(None, 'tp', None), P('tp', None), P(None, 'tp', None), P(None, 'tp', None), P('tp', None), P('tp', None, None), P(), P(), P(), P(None, 'tp'), P('tp'), P('tp', None), P(), P('dp', None))
OUT_SPECS = (P('dp', None), P('dp', 'sp', None), P('dp'), P('dp', 'tp', None), P('dp', 'tp', None), P('dp', 'tp', None), P(('dp', 'tp'), None, None), P('dp', 'tp'), P(('dp', 'tp'), None))
LANES = 128
SUB = 8
PER = 2
GELU_C = 0.7978845608028654
GELU_A = 0.044715


def nn(a, b):
    return lax.dot_general(a, b, (((1,), (0,)), ((), ())), preferred_element_type=F32)


def nt(a, b):
    return lax.dot_general(a, b, (((1,), (1,)), ((), ())), preferred_element_type=F32)


def tn(a, b):
    return lax.dot_general(a, b, (((0,), (0,)), ((), ())), preferred_element_type=F32)


def hi_lo(a):
    hi = a.astype(BF16)
    return hi, (a - hi.astype(F32)).astype(BF16)


def iota(shape, dim):
    return lax.broadcasted_iota(jnp.int32, shape, dim)


def by_head(parts, width):
    rows, cols = parts[0].shape[0], len(parts) * width
    block = iota((rows, cols), 1) // width
    out = jnp.zeros((rows, cols), F32)
    for h, part in enumerate(parts):
        out = jnp.where(block == h, part, out)
    return out


def row(ref):
    return ref[...].reshape(1, -1)


def flat(ref):
    heads, width = ref.shape
    wide = jnp.concatenate([ref[...]] * heads, axis=1)
    keep = iota(wide.shape, 0) == iota(wide.shape, 1) // width
    return jnp.sum(jnp.where(keep, wide, 0.0), axis=0, keepdims=True)


def gelu_parts(pre):
    t = jnp.tanh(GELU_C * (pre + GELU_A * pre * pre * pre))
    value = 0.5 * pre * (1.0 + t)
    slope = 0.5 * (1.0 + t) + 0.5 * pre * (1.0 - t * t) * (GELU_C * (1.0 + 3.0 * GELU_A * pre * pre))
    return value, slope


def centre(rows):
    mean = jnp.mean(rows, axis=-1, keepdims=True)
    centred = rows - mean
    inv = lax.rsqrt(jnp.mean(centred * centred, axis=-1, keepdims=True) + NORM_EPS)
    return centred * inv, inv, mean


def norm_back(hat, inv, cot):
    return inv * (cot - jnp.mean(cot, axis=-1, keepdims=True) - hat * jnp.mean(cot * hat, axis=-1, keepdims=True))


def barrier_all(peers):
    sem = pltpu.get_barrier_semaphore()
    for axis, dev in peers:
        pl.semaphore_signal(sem, inc=1, device_id={axis: dev}, device_id_type=MESH)
    pl.semaphore_wait(sem, len(peers))


def peers_of(axis, n):
    me = lax.axis_index(axis)
    return me, [lax.rem(me + k, n) for k in range(1, n)]


def remote(src, dst, send_sem, recv_sem, axis, dev):
    return pltpu.make_async_remote_copy(src_ref=src, dst_ref=dst, send_sem=send_sem, recv_sem=recv_sem, device_id={axis: dev}, device_id_type=MESH)


def gather_start(buf, me, peers, send_sems, recv_sems, axis):
    for k, dev in enumerate(peers):
        remote(buf.at[me], buf.at[me], send_sems.at[k], recv_sems.at[me], axis, dev).start()


def gather_wait(buf, me, peers, send_sems, recv_sems, axis):
    for k, dev in enumerate(peers):
        remote(buf.at[dev], buf.at[dev], send_sems.at[k], recv_sems.at[dev], axis, dev).wait_recv()
    for k, dev in enumerate(peers):
        remote(buf.at[me], buf.at[me], send_sems.at[k], recv_sems.at[me], axis, dev).wait_send()


class ChipRing:
    def __init__(self, nsp):
        me = lax.axis_index('sp')
        self.me, self.core = me, lax.rem(me, 2)
        self.mate = me + 1 - 2 * self.core
        self.up, self.down, self.far = (lax.rem(me + k, nsp) for k in (2, nsp - 2, 4))
        self.mates = [lax.rem(self.mate + k, nsp) for k in (2, nsp - 2, 4)]
        self.around = [self.mate, self.up, self.down, self.far] + self.mates

    def start(self, buf, send, recv):
        for k, dev in enumerate((self.mate, self.up, self.down)):
            remote(buf.at[self.me], buf.at[self.me], send.at[k], recv.at[self.me], 'sp', dev).start()

    def relay(self, buf, send, recv, upward):
        for k, dev in ((3, self.down), (4, self.up)):
            remote(buf.at[dev], buf.at[dev], send.at[k], recv.at[dev], 'sp', dev).wait_recv()
            if upward == (k == 3):
                remote(buf.at[dev], buf.at[dev], send.at[5], recv.at[dev], 'sp', self.up if upward else self.down).start()
            remote(buf.at[dev], buf.at[dev], send.at[k], recv.at[dev], 'sp', self.mate).start()

    def finish(self, buf, send, recv, upward):
        far = self.far
        remote(buf.at[far], buf.at[far], send.at[6], recv.at[far], 'sp', self.mate).wait_recv()
        remote(buf.at[far], buf.at[far], send.at[6], recv.at[far], 'sp', self.mate).start()
        for dev in [self.mate] + self.mates:
            remote(buf.at[dev], buf.at[dev], send.at[0], recv.at[dev], 'sp', self.mate).wait_recv()
        via = self.down if upward else self.up
        for k, slot in ((0, self.me), (1, self.me), (2, self.me), (3, self.down), (4, self.up), (5, via), (6, far)):
            remote(buf.at[slot], buf.at[slot], send.at[k], recv.at[slot], 'sp', self.mate).wait_send()


RING_SEMS = 7


def scan_kernel(heads, scale, x_ref, gain_ref, bias_ref, probe_ref, wq_ref, bq_ref, wk_ref, wv_ref, bv_ref, pk_ref, hb_ref, qk_ref, q_ref, h_ref, ms_ref, qkr, hball):
    rows = heads * SUB
    width = wq_ref.shape[0] // heads

    @pl.when(pl.program_id(0) == 0)
    def _():
        probe8 = jnp.broadcast_to(row(probe_ref), (SUB, probe_ref.shape[0])).astype(BF16)
        q8 = (nt(probe8, wq_ref[...]) + flat(bq_ref)).astype(BF16)
        q_ref[...] = q8.astype(F32)
        qs = jnp.concatenate([q8.astype(F32)] * heads, axis=0)
        qs = jnp.where(iota(qs.shape, 0) // SUB == iota(qs.shape, 1) // width, qs, 0.0).astype(BF16)
        qk = nn(qs, wk_ref[...])
        hi, lo = hi_lo(qk)
        qkr[...] = jnp.zeros(qkr.shape, BF16)
        qkr[0:rows, :] = hi
        qkr[LANES // 2:LANES // 2 + rows, :] = lo
        for h in range(heads):
            qk_ref[h:h + 1, :] = qk[SUB * h:SUB * h + 1, :]

    step = pl.program_id(0)
    block = x_ref.shape[0] // PER
    images, tokens = SUB, block // SUB
    cols = wq_ref.shape[0]
    for j in range(PER):
        at = slice(j * block, j * block + block)
        hat, inv, mean = centre(x_ref[at, :].astype(F32))
        hid = (hat * row(gain_ref) + row(bias_ref)).astype(BF16)
        h_ref[at, :] = hid
        ms_ref[at, :] = jnp.where(iota((block, LANES), 1) == 0, mean, inv)
        r = nt(hid, qkr[...])
        s = ((r + pltpu.roll(r, LANES // 2, 1)) * scale).reshape(images, tokens, LANES)
        m = jnp.max(s, axis=1)
        e = jnp.exp(s - m[:, None, :])
        l = jnp.sum(e, axis=1)
        lane, img = iota(e.shape, 2), iota(e.shape, 0)
        ebd = jnp.where((lane % SUB == img) & (lane < rows), e, 0.0).astype(BF16).reshape(images * tokens, LANES)
        hb = tn(ebd, hid)[0:rows, :]
        hb_ref[j, :, :] = hb
        hball[step * PER + j] = hb
        mine = pl.ds(pl.multiple_of((step * PER + j) * SUB, SUB), SUB)
        pk_ref[mine, cols:cols + LANES] = m
        pk_ref[mine, cols + LANES:cols + 2 * LANES] = l

    @pl.when(step == pl.num_programs(0) - 1)
    def _():
        groups = hball.shape[0]
        every = groups * rows
        hi, lo = hi_lo(hball[...].reshape(every, hball.shape[2]))
        v = nt(hi, wv_ref[...]) + nt(lo, wv_ref[...])
        bias = flat(bv_ref)
        for g in range(groups):
            vs = by_head([v[g * rows + SUB * h:g * rows + SUB * h + SUB] for h in range(heads)], width)
            tot = pk_ref[g * SUB:g * SUB + SUB, cols + LANES:cols + 2 * LANES]
            pk_ref[g * SUB:g * SUB + SUB, 0:cols] = vs + by_head([tot[:, SUB * h:SUB * h + 1] for h in range(heads)], width) * bias


def scan_tokens(heads, images, scale, x, gain, bias, probe, wq, bq, wk, wv, bv):
    tokens_all, width = x.shape
    hd = wq.shape[0]
    groups = images // SUB
    block = tokens_all // groups * PER
    full = lambda a: pl.BlockSpec(a.shape, lambda g: (0,) * a.ndim)
    return pl.pallas_call(
        functools.partial(scan_kernel, heads, scale),
        grid=(groups // PER,),
        in_specs=[pl.BlockSpec((block, width), lambda g: (g, 0))] + [full(a) for a in (gain, bias, probe, wq, bq, wk, wv, bv)],
        out_specs=[pl.BlockSpec((images, hd + 2 * LANES), lambda g: (0, 0)), pl.BlockSpec((PER, heads * SUB, width), lambda g: (g, 0, 0)), pl.BlockSpec((heads, width), lambda g: (0, 0)), pl.BlockSpec((SUB, hd), lambda g: (0, 0)), pl.BlockSpec((block, width), lambda g: (g, 0)), pl.BlockSpec((block, LANES), lambda g: (g, 0))],
        out_shape=[jax.ShapeDtypeStruct((images, hd + 2 * LANES), F32), jax.ShapeDtypeStruct((groups, heads * SUB, width), F32), jax.ShapeDtypeStruct((heads, width), F32), jax.ShapeDtypeStruct((SUB, hd), F32), jax.ShapeDtypeStruct(x.shape, BF16), jax.ShapeDtypeStruct((tokens_all, LANES), F32)],
        scratch_shapes=[pltpu.VMEM((LANES, width), BF16), pltpu.VMEM((groups, heads * SUB, width), F32)],
        name='scan_tokens',
    )(x, gain, bias, probe, wq, bq, wk, wv, bv)


def middle_kernel(heads, nsp, ntp, scale, pk_ref, og_ref, qk_ref, bo_ref, hg_ref, hb_ref, bu_ref, bd_ref, bv_ref, hb_hbm, x_hbm, wo_hbm, wu_hbm, wd_hbm, wv_hbm, wk_hbm, wq_hbm,
                  gv_out, hbar_out, st_out, qk_out, gp_out, y_out, ga_out, pool_out, pb_out, hid_out, gpre_out, u_out, gq_out, gpr_out,
                  wo, wu, wd, wv, wk, wq, rbuf, ta, tg, td, ag, hr, relay, pa, ha, sg, xb, rhs, uacc, ub, prb, ghb,
                  wsem, xsem, rs_send, rs_recv, ta_s, ta_r, tg_s, tg_r, td_s, td_r, ag_s, ag_r, hr_s, hr_r, rl_r, gv_s, gv_r, fw_s, fw_r, pa_s, pa_r, ha_s, ha_r, st_s, st_r, qk_s, qk_r, ub_s, ub_r, pr_s, pr_r, sy_s, sy_r, sg_s, sg_r):
    sp, sp_peers = peers_of('sp', nsp)
    tp, tp_peers = peers_of('tp', ntp)
    ring = ChipRing(nsp)
    core, mate = ring.core, ring.mate
    loads = [pltpu.make_async_copy(a, b, wsem.at[i]) for i, (a, b) in enumerate(((wd_hbm, wd), (wo_hbm, wo), (wu_hbm, wu), (hb_hbm.at[sp], hr.at[sp]), (wv_hbm, wv), (wk_hbm, wk), (wq_hbm, wq)))]
    for load in loads:
        load.start()
    sem = pltpu.get_barrier_semaphore()
    for axis, devs in (('sp', sp_peers), ('tp', tp_peers)):
        for dev in devs:
            pl.semaphore_signal(sem, inc=1, device_id={axis: dev}, device_id_type=MESH)

    def x_load(g):
        return pltpu.make_async_copy(x_hbm.at[g], xb.at[g % 2], xsem.at[g % 2])

    x_load(0).start()
    x_load(1).start()
    hd = wo.shape[0]
    width = hd // heads
    model = wu.shape[0]
    rows = heads * SUB
    images = nsp * SUB
    qk_out[tp] = qk_ref[...]
    rbuf[sp] = pk_ref[sp]
    for h in range(heads):
        hi, lo = hi_lo(jnp.broadcast_to(qk_ref[h:h + 1, :], (SUB, model)))
        rhs[h * SUB:h * SUB + SUB, :] = hi.astype(F32)
        rhs[2 * rows + h * SUB:2 * rows + h * SUB + SUB, :] = lo.astype(F32)
    og = og_ref[sp]
    pl.semaphore_wait(sem, len(sp_peers) + len(tp_peers))

    sends = []
    for k, dev in enumerate(sp_peers):
        sends.append(remote(pk_ref.at[dev], rbuf.at[sp], rs_send.at[k], rs_recv.at[sp], 'sp', dev))
        sends[-1].start()
    far0, far1 = ring.far - core, ring.far - core + 1
    late = [remote(hb_hbm.at[far0], relay.at[0], hr_s.at[0], rl_r.at[0], 'sp', ring.up), remote(hb_hbm.at[far1], relay.at[1], hr_s.at[1], rl_r.at[1], 'sp', ring.down)]
    for k, dev in enumerate((ring.up, ring.down, ring.mates[0], ring.mates[1], mate)):
        late.append(remote(hb_hbm.at[dev], hr.at[sp], hr_s.at[2 + k], hr_r.at[sp], 'sp', dev))
    for send in late:
        send.start()
    gather_start(qk_out, tp, tp_peers, qk_s, qk_r, 'tp')
    loads[0].wait()
    gh = nt(og, wd[...])
    for k, dev in enumerate(sp_peers):
        remote(rbuf.at[dev], rbuf.at[dev], rs_send.at[k], rs_recv.at[dev], 'sp', dev).wait_recv()
    for send in sends:
        send.wait_send()
    m = rbuf[0, :, hd:hd + LANES]
    for j in range(1, nsp):
        m = jnp.maximum(m, rbuf[j, :, hd:hd + LANES])
    l = jnp.zeros_like(m)
    v = jnp.zeros((SUB, hd), F32)
    for j in range(nsp):
        w = jnp.exp(rbuf[j, :, hd:hd + LANES] - m)
        l = l + w * rbuf[j, :, hd + LANES:hd + 2 * LANES]
        v = v + by_head([w[:, SUB * h:SUB * h + 1] for h in range(heads)], width) * rbuf[j, :, 0:hd]
    o = v / by_head([l[:, SUB * h:SUB * h + 1] for h in range(heads)], width)
    pooled_bf = o.astype(BF16)
    lse = m + jnp.log(l)

    loads[1].wait()
    ta[tp] = nn(pooled_bf, wo[...])
    gather_start(ta, tp, tp_peers, ta_s, ta_r, 'tp')
    for k, (src, dst) in enumerate(((ring.down, ring.up - core), (ring.up, ring.down - core + 1))):
        remote(relay.at[k], relay.at[k], hr_s.at[k], rl_r.at[k], 'sp', src).wait_recv()
        late.append(remote(relay.at[k], hr.at[src], hr_s.at[7 + k], hr_r.at[src], 'sp', dst))
        late[-1].start()
    loads[2].wait()
    gather_wait(ta, tp, tp_peers, ta_s, ta_r, 'tp')
    attn = ta[0]
    for t in range(1, ntp):
        attn = attn + ta[t]
    attn = attn + row(bo_ref)
    hat, inv, _ = centre(attn)
    gain = row(hg_ref)
    y = (hat * gain + row(hb_ref)).astype(BF16)
    value, slope = gelu_parts(nn(y, wu[...]) + row(bu_ref))
    tg[tp] = nt((gh * slope).astype(BF16), wu[...])
    gather_start(tg, tp, tp_peers, tg_s, tg_r, 'tp')
    td[tp] = nn(value.astype(BF16), wd[...])
    gather_start(td, tp, tp_peers, td_s, td_r, 'tp')
    gather_wait(tg, tp, tp_peers, tg_s, tg_r, 'tp')
    gno = tg[0]
    for t in range(1, ntp):
        gno = gno + tg[t]
    ga = (og.astype(F32) + norm_back(hat, inv, gno * gain)).astype(BF16)
    gp = nt(ga, wo[...]).astype(BF16).astype(F32)
    prod = gp * (o - flat(bv_ref))
    head_of = iota(prod.shape, 1) // width
    delta = by_head([jnp.sum(jnp.where(head_of == h, prod, 0.0), axis=1, keepdims=True) for h in range(heads)], SUB)
    ag[sp, :, 0:hd] = gp
    ag[sp, :, hd:hd + LANES] = jnp.concatenate([lse[:, 0:rows], delta, jnp.zeros((SUB, LANES - 2 * rows), F32)], axis=1)
    gather_start(ag, sp, sp_peers, ag_s, ag_r, 'sp')

    gather_wait(td, tp, tp_peers, td_s, td_r, 'tp')
    down = td[0]
    for t in range(1, ntp):
        down = down + td[t]
    pa[sp, :, 0:model] = y.astype(F32)
    pa[sp, :, model:2 * model] = (attn + down + row(bd_ref)).astype(BF16).astype(F32)
    pa[sp, :, 2 * model:3 * model] = ga.astype(F32)
    pa[sp, :, 3 * model:3 * model + hd] = pooled_bf.astype(F32)
    gather_wait(ag, sp, sp_peers, ag_s, ag_r, 'sp')
    ring.start(pa, pa_s, pa_r)

    loads[4].wait()
    st_out[tp] = ag[:, :, hd:hd + LANES]
    near_up, near_down, far_tp = lax.rem(tp + 1, ntp), lax.rem(tp + ntp - 1, ntp), lax.rem(tp + 2, ntp)
    half = nsp // 2
    direct = half - sg.shape[2]
    gp_out[...] = ag[:, :, 0:hd].astype(BF16)

    def make_gv(first):
        part = jnp.concatenate([ag[first + i, :, 0:hd] for i in range(half) for _ in range(heads)], axis=0)
        keep = (iota(part.shape, 0) // SUB) % heads == iota(part.shape, 1) // width
        gv_out[tp, pl.ds(first, half)] = nn(jnp.where(keep, part, 0.0).astype(BF16), wv[...]).reshape(half, rows, model)

    def piece(i, owner):
        return gv_out.at[owner, core * half + i]

    def send_gv(i, k, owner, dev):
        return remote(piece(i, owner), piece(i, owner), gv_s.at[k, i], gv_r.at[owner, i], 'tp', dev)

    def forward(i, k, owner):
        return remote(piece(i, owner), piece(i, owner), fw_s.at[k, i], fw_r.at[owner, i], 'sp', mate)

    def near(i):
        for k, owner in ((0, near_down), (1, near_up)):
            send_gv(i, k, owner, owner).wait_recv()
            if k == i % 2:
                send_gv(i, 2, owner, near_down if k else near_up).start()
            forward(i, k, owner).start()

    def beyond(i):
        send_gv(i, 2, far_tp, far_tp).wait_recv()
        forward(i, 2, far_tp).start()

    def send_shared(k):
        block = pl.ds(pl.multiple_of((sp // 2) * SUB, SUB), SUB)
        return remote(gv_out.at[tp, pl.ds(core * half + direct, half - direct), block], sg.at[sp, ntp - 1 - k], sy_s.at[k - 1], sy_r.at[ntp - 1 - k], 'tp', lax.rem(tp + k, ntp))

    make_gv(core * half)
    for k in range(1, ntp):
        send_shared(k).start()
    for i in range(direct):
        send_gv(i, 0, tp, near_up).start()
        send_gv(i, 1, tp, near_down).start()
        if i == 0:
            gather_start(st_out, tp, tp_peers, st_s, st_r, 'tp')
    make_gv((1 - core) * half)
    loads[3].wait()
    for k, dev in enumerate(sp_peers):
        remote(hr.at[dev], hr.at[dev], hr_s.at[k], hr_r.at[dev], 'sp', dev).wait_recv()
    for send in late:
        send.wait_send()
    hbar = jnp.zeros(hr.shape[1:], F32)
    for j in range(nsp):
        w = jnp.exp(rbuf[j, :, hd:hd + LANES] - lse)
        hbar = hbar + hr[j] * jnp.concatenate([w[:, SUB * h:SUB * h + 1] for h in range(heads)], axis=0)
    ha[sp] = hbar
    ring.start(ha, ha_s, ha_r)

    uacc[...] = jnp.zeros(uacc.shape, F32)

    def u_step(g):
        x_load(g).wait()
        tokens = xb.shape[1] // SUB
        hidden = xb[g % 2]
        hi, lo = hi_lo(gv_out[tp, g])
        rhs[rows:2 * rows, :] = hi.astype(F32)
        rhs[3 * rows:4 * rows, :] = lo.astype(F32)
        r = nt(hidden, rhs[...].astype(BF16))
        r = (r + pltpu.roll(r, LANES // 2, 1)).reshape(SUB, tokens, LANES)
        lane, img = iota(r.shape, 2), iota(r.shape, 0)
        r = r * jnp.where(lane < rows, scale, 1.0) - ag[g, :, hd:hd + LANES][:, None, :]
        r = r.reshape(SUB * tokens, LANES)
        grad = (jnp.exp(r) * pltpu.roll(r, LANES - rows, 1) * scale).reshape(SUB, tokens, LANES)
        ds = jnp.where((lane % SUB == img) & (lane < rows), grad, 0.0).astype(BF16).reshape(SUB * tokens, LANES)
        uacc[...] += tn(ds, hidden)[0:rows, :]
        if g + 2 < nsp:
            x_load(g + 2).start()

    u_step(0)
    u_step(1)
    u_step(2)
    ring.relay(pa, pa_s, pa_r, False)
    for k in range(1, ntp):
        remote(sg.at[sp, k - 1], sg.at[sp, k - 1], sy_s.at[0], sy_r.at[k - 1], 'tp', near_up).wait_recv()
    ring.start(sg, sg_s, sg_r)
    u_step(3)
    u_step(4)
    near(0)
    u_step(5)
    u_step(6)
    ring.finish(pa, pa_s, pa_r, False)
    ring.relay(ha, ha_s, ha_r, True)
    u_step(7)
    for h in range(heads):
        ub[sp, h:h + 1, :] = jnp.sum(uacc[SUB * h:SUB * h + SUB, :], axis=0, keepdims=True)
    gather_start(ub, sp, sp_peers, ub_s, ub_r, 'sp')

    near(1)
    ghb[...] = nt(og_ref[...].reshape(images, model), wd[...])
    y_all = pa[:, :, 0:model].astype(BF16)
    y_out[...] = y_all
    pool_out[...] = pa[:, :, model:2 * model].astype(BF16)
    ga_out[...] = pa[:, :, 2 * model:3 * model].astype(BF16)
    pb_out[...] = pa[:, :, 3 * model:3 * model + hd].astype(BF16)
    value, slope = gelu_parts(nn(y_all.reshape(images, model), wu[...]) + row(bu_ref))
    gpre_out[...] = (ghb[...] * slope).astype(BF16)
    hid_out[...] = value.astype(BF16)
    ring.relay(sg, sg_s, sg_r, False)
    near(2)

    gather_wait(ub, sp, sp_peers, ub_s, ub_r, 'sp')
    u = ub[0]
    for j in range(1, nsp):
        u = u + ub[j]
    u_out[...] = u
    loads[5].wait()
    loads[6].wait()
    hi, lo = hi_lo(u)
    gq = nt(jnp.concatenate([hi, lo], axis=0), wk[...])
    gq = gq[0:heads] + gq[heads:2 * heads]
    gq = jnp.sum(jnp.where(iota(gq.shape, 0) == iota(gq.shape, 1) // width, gq, 0.0), axis=0, keepdims=True)
    gq_out[...] = gq
    hi, lo = hi_lo(gq)
    gpr = nn(jnp.concatenate([hi, lo], axis=0), wq[...])
    prb[tp] = gpr[0:1] + gpr[1:2]
    gather_start(prb, tp, tp_peers, pr_s, pr_r, 'tp')
    beyond(0)
    ring.finish(ha, ha_s, ha_r, True)
    hbar_out[...] = ha[...].astype(BF16)
    beyond(1)
    ring.finish(sg, sg_s, sg_r, False)
    for j in range(nsp):
        for k in range(1, ntp):
            gv_out[lax.rem(tp + k, ntp), (j % 2) * half + direct:(j % 2) * half + half, (j // 2) * SUB:(j // 2) * SUB + SUB, :] = sg[j, k - 1]
    beyond(2)
    for k in range(1, ntp):
        send_shared(k).wait_send()
    for i in range(direct):
        other = (1 - core) * half + i
        for k, (owner, dev) in enumerate(((tp, near_up), (tp, near_down), (near_up if i % 2 else near_down, near_down if i % 2 else near_up))):
            send_gv(i, k, owner, dev).wait_send()
        for k, owner in enumerate((near_down, near_up, far_tp)):
            forward(i, k, owner).wait_send()
            remote(gv_out.at[owner, other], gv_out.at[owner, other], fw_s.at[k, i], fw_r.at[owner, i], 'sp', mate).wait_recv()
    gather_wait(st_out, tp, tp_peers, st_s, st_r, 'tp')
    gather_wait(qk_out, tp, tp_peers, qk_s, qk_r, 'tp')
    gather_wait(prb, tp, tp_peers, pr_s, pr_r, 'tp')
    total = prb[0]
    for t in range(1, ntp):
        total = total + prb[t]
    gpr_out[...] = total


def middle(heads, nsp, ntp, scale, pk, og3, qk, vectors, hb, x3, wo, wu, wd, wv, wk, wq):
    own, model = og3.shape[1:]
    hd = wo.shape[0]
    rows = hb.shape[1]
    images = nsp * own
    half = nsp // 2
    pk3 = pk.reshape(nsp, own, pk.shape[1])
    vm, hbm = pl.BlockSpec(memory_space=pltpu.VMEM), pl.BlockSpec(memory_space=pl.ANY)
    dma = pltpu.SemaphoreType.DMA
    sds = jax.ShapeDtypeStruct
    part = pltpu.VMEM((ntp, own, model), F32)
    wide = [pltpu.VMEM(w.shape, BF16) for w in (wo, wu, wd, wv, wk, wq)]
    ring, tps, tpr = [dma((RING_SEMS,)), dma((nsp,))], dma((ntp - 1,)), dma((ntp,))
    return pl.pallas_call(
        functools.partial(middle_kernel, heads, nsp, ntp, scale),
        in_specs=[vm] * 9 + [hbm] * 8,
        out_specs=[vm] * 14,
        out_shape=[pltpu.VMEM((ntp, nsp, rows, model), F32), sds((nsp, rows, model), BF16), sds((ntp, nsp, own, LANES), F32), sds((ntp,) + qk.shape, F32), sds((nsp, own, hd), BF16),
                   sds((nsp, own, model), BF16), sds((nsp, own, model), BF16), sds((nsp, own, model), BF16), sds((nsp, own, hd), BF16), sds((images, model), BF16), sds((images, model), BF16), sds(qk.shape, F32), sds((1, hd), F32), sds((1, model), F32)],
        scratch_shapes=wide + [pltpu.VMEM(pk3.shape, F32), part, part, part, pltpu.VMEM((nsp, own, hd + LANES), F32), pltpu.VMEM(hb.shape, F32), pltpu.VMEM((2,) + hb.shape[1:], F32), pltpu.VMEM((nsp, own, 3 * model + hd), F32), pltpu.VMEM(hb.shape, F32), pltpu.VMEM((nsp, ntp - 1, 1, own, model), F32),
                               pltpu.VMEM((2,) + x3.shape[1:], BF16), pltpu.VMEM((LANES, model), F32), pltpu.VMEM((rows, model), F32), pltpu.VMEM((nsp,) + qk.shape, F32), pltpu.VMEM((ntp, 1, model), F32), pltpu.VMEM((images, model), F32),
                               dma((7,)), dma((2,)), dma((nsp - 1,)), dma((nsp,)), tps, tpr, tps, tpr, tps, tpr, dma((nsp - 1,)), dma((nsp,))] + [dma((9,)), dma((nsp,)), dma((2,)), dma((3, half)), dma((ntp, half)), dma((3, half)), dma((ntp, half))] + ring + ring + [tps, tpr, tps, tpr, dma((nsp - 1,)), dma((nsp,)), tps, tpr, tps, tpr] + ring,
        compiler_params=pltpu.CompilerParams(collective_id=0, has_side_effects=True, vmem_limit_bytes=57 << 20),
        name='middle',
    )(pk3, og3, qk, *vectors, hb, x3, wo, wu, wd, wv, wk, wq)


def products_kernel(heads, parts, y_ref, gpre_ref, hid_ref, og_ref, pb_ref, ga_ref, gp_ref, hbar_ref, q_ref, u_ref, gq_ref, probe_ref, pool_ref, gpr_ref, gup_ref, gdown_ref, gwo_ref, gwv_ref, gwk_ref, gwq_ref, pool_out, gpr_out):
    step = pl.program_id(0)
    gup_ref[...] = tn(y_ref[...], gpre_ref[...])
    gdown_ref[...] = tn(hid_ref[...], og_ref[...])
    tile, model = gwo_ref.shape
    width = parts * tile // heads
    part = lax.rem(step, parts)
    groups = gp_ref.shape[0]

    @pl.when(step == 0)
    def _():
        pool_out[...] = pool_ref[...]
        gpr_out[...] = gpr_ref[...].reshape(gpr_out.shape)

    @pl.when(step < parts)
    def _():
        gwo_ref[...] = tn(pb_ref[...], ga_ref[...])
        gp = jnp.concatenate([gp_ref[g].astype(F32) for g in range(groups) for _ in range(heads)], axis=0)
        keep = (iota(gp.shape, 0) // SUB) % heads == (part * tile + iota(gp.shape, 1)) // width
        gwv_ref[...] = tn(jnp.where(keep, gp, 0.0).astype(BF16), hbar_ref[...].reshape(gp.shape[0], model))

    @pl.when(step >= parts)
    def _():
        q = jnp.transpose(q_ref[...])[:, 0:1]
        head_of = (part * tile + iota((tile, model), 0)) // width
        u = jnp.zeros((tile, model), F32)
        for h in range(heads):
            u = jnp.where(head_of == h, u_ref[h:h + 1, :], u)
        gwk_ref[...] = q * u
        gq = jnp.transpose(jnp.broadcast_to(gq_ref[...], (SUB, tile)))[:, 0:1]
        gwq_ref[...] = gq * row(probe_ref)


def products(heads, y, gpre, hid, og, pb, ga, gp3, hbar, q8, u, gq, probe, pool, gpr):
    images, model = y.shape
    cols, hd = gpre.shape[1], pb.shape[1]
    parts = hd // LANES
    steps = 2 * parts
    tile = model // steps
    at = lambda a: lambda i: jnp.clip(i - parts * a, 0, parts - 1)
    lane = lambda i: lax.rem(i, parts)
    part = pl.BlockSpec((images, tile), lambda i: (0, i))
    full = lambda a: pl.BlockSpec(a.shape, lambda i: (0,) * a.ndim)
    out = pl.BlockSpec((tile, cols), lambda i: (i, 0))
    small = [pl.BlockSpec((LANES, model), lambda i, f=at(a): (f(i), 0)) for a in (0, 0, 1, 1)]
    sds = jax.ShapeDtypeStruct
    return pl.pallas_call(
        functools.partial(products_kernel, heads, parts),
        grid=(steps,),
        in_specs=[part, full(gpre), part, full(og), pl.BlockSpec((images, LANES), lambda i: (0, lane(i))), full(ga), pl.BlockSpec(gp3.shape[:2] + (LANES,), lambda i: (0, 0, lane(i))), full(hbar), pl.BlockSpec((SUB, LANES), lambda i: (0, lane(i))), full(u), pl.BlockSpec((1, LANES), lambda i: (0, lane(i))), full(probe), full(pool), full(gpr)],
        out_specs=[out, out] + small + [full(pool), full(probe)],
        out_shape=[sds((model, cols), F32), sds((cols, model), F32)] + [sds((hd, model), F32)] * 4 + [sds(pool.shape, pool.dtype), sds(probe.shape, F32)],
        name='products',
    )(y, gpre, hid, og, pb, ga, gp3, hbar, q8, u, gq, probe, pool, gpr)


def back_kernel(heads, ntp, scale, x_ref, h_ref, ms_ref, gain_ref, gv_ref, qk_ref, st_ref, gx_ref, qkr):
    step = pl.program_id(0)
    rows = heads * SUB
    model = x_ref.shape[1]

    @pl.when(step == 0)
    def _():
        for t in range(ntp):
            for h in range(heads):
                hi, lo = hi_lo(jnp.broadcast_to(qk_ref[t, h:h + 1, :], (SUB, model)))
                at = (t * heads + h) * SUB
                qkr[at:at + SUB, :] = hi.astype(F32)
                qkr[LANES + at:LANES + at + SUB, :] = lo.astype(F32)

    block = x_ref.shape[0] // PER
    images, tokens = SUB, block // SUB
    gain = row(gain_ref)
    qkb = qkr[...].astype(BF16)
    for j in range(PER):
        at = slice(j * block, j * block + block)
        hid = h_ref[at, :]
        gv_hi, gv_lo = hi_lo(jnp.concatenate([gv_ref[t, step * PER + j] for t in range(ntp)], axis=0))
        r = nt(hid, qkb)
        s = (r[:, 0:LANES] + r[:, LANES:2 * LANES]) * scale
        d = nt(hid, jnp.concatenate([gv_hi, gv_lo], axis=0))
        d = d[:, 0:LANES] + d[:, LANES:2 * LANES]
        lse = jnp.concatenate([st_ref[t, j, :, 0:rows] for t in range(ntp)], axis=1)
        delta = jnp.concatenate([st_ref[t, j, :, rows:2 * rows] for t in range(ntp)], axis=1)
        shape = (images, tokens, LANES)
        keep = iota(shape, 2) % SUB == iota(shape, 0)
        p = jnp.where(keep, jnp.exp(s.reshape(shape) - lse[:, None, :]), 0.0)
        ds = p * (d.reshape(shape) - delta[:, None, :]) * scale
        pb = p.astype(BF16).reshape(images * tokens, LANES)
        db = ds.astype(BF16).reshape(images * tokens, LANES)
        gh = nn(jnp.concatenate([pb, db], axis=1), jnp.concatenate([gv_hi, qkb[0:LANES]], axis=0))
        inv = ms_ref[at, 1:2]
        hat = (x_ref[at, :].astype(F32) - ms_ref[at, 0:1]) * inv
        gx_ref[at, :] = norm_back(hat, inv, gh * gain).astype(BF16)


def back_tokens(heads, ntp, scale, x, h, ms, gain, gv, qk, st):
    tokens_all, model = x.shape
    groups, rows = gv.shape[1], gv.shape[2]
    block = tokens_all // groups * PER
    full = lambda a: pl.BlockSpec(a.shape, lambda g: (0,) * a.ndim)
    return pl.pallas_call(
        functools.partial(back_kernel, heads, ntp, scale),
        grid=(groups // PER,),
        in_specs=[pl.BlockSpec((block, model), lambda g: (g, 0)), pl.BlockSpec((block, model), lambda g: (g, 0)), pl.BlockSpec((block, LANES), lambda g: (g, 0)), full(gain), pl.BlockSpec(memory_space=pltpu.VMEM), full(qk), pl.BlockSpec((ntp, PER) + st.shape[2:], lambda g: (0, g, 0, 0))],
        out_specs=pl.BlockSpec((block, model), lambda g: (g, 0)),
        out_shape=jax.ShapeDtypeStruct((tokens_all, model), BF16),
        scratch_shapes=[pltpu.VMEM((2 * LANES, model), F32)],
        compiler_params=pltpu.CompilerParams(vmem_limit_bytes=57 << 20),
        name='back_tokens',
    )(x, h, ms, gain, gv, qk, st)


def local_head(nsp, ntp, encoded, enc_gain, enc_bias, probe, w_query, b_query, w_key, w_value, b_value, w_out, b_out, head_gain, head_bias, w_up, b_up, w_down, b_down, out_grad):
    images, tokens, model = encoded.shape
    heads, head_dim = b_query.shape
    hd = heads * head_dim
    scale = head_dim ** -0.5
    x = encoded.reshape(images * tokens, model)
    wq, wk, wv = (jnp.transpose(w, (1, 2, 0)).reshape(hd, model) for w in (w_query, w_key, w_value))
    wo = w_out.reshape(hd, model)
    og3 = out_grad.reshape(nsp, images // nsp, model)
    pk, hb, qk, q8, h, ms = scan_tokens(heads, images, scale, x, enc_gain, enc_bias, probe, wq, b_query, wk, wv, b_value)
    gv, hbar, st, qk_all, gp3, y3, ga3, pool3, pb3, hidden, grad_pre, u, gq, gpr = middle(heads, nsp, ntp, scale, pk, og3, qk, (b_out, head_gain, head_bias, b_up, b_down, b_value), hb, h.reshape(nsp, -1, model), wo, w_up, w_down, wv, wk, wq)
    gv = pltpu.with_memory_space_constraint(gv, pltpu.VMEM)
    gx = back_tokens(heads, ntp, scale, x, h, ms, enc_gain, gv, qk_all, st)
    y, ga, pool, pooled_bf = (a.reshape(images, -1) for a in (y3, ga3, pool3, pb3))
    grad_w_up, grad_w_down, *small, pooled, grad_probe = products(heads, y, grad_pre, hidden, out_grad, pooled_bf, ga, gp3, hbar, q8, u, gq, probe, pool, gpr)
    grad_w_out, grad_wv, grad_wk, grad_wq = (a.reshape(heads, head_dim, model) for a in small)
    back = lambda a: jnp.transpose(a, (2, 0, 1))
    return (pooled, gx.reshape(encoded.shape), grad_probe, back(grad_wq), back(grad_wk), back(grad_wv), grad_w_out, grad_w_up, grad_w_down)


def solution(mesh):
    body = functools.partial(local_head, mesh.shape['sp'], mesh.shape['tp'])
    return jax.shard_map(body, mesh=mesh, in_specs=IN_SPECS, out_specs=OUT_SPECS, check_vma=False)
```

```python
import functools
import jax
import jax.numpy as jnp
from jax import lax
from jax.experimental import pallas as pl
from jax.experimental.pallas import tpu as pltpu
from jax.sharding import PartitionSpec as P

NORM_EPS = 1e-6
MESH = pl.DeviceIdType.MESH
F32, BF16 = jnp.float32, jnp.bfloat16
IN_SPECS = (P('dp', 'sp', None), P(), P(), P(), P(None, 'tp', None), P('tp', None), P(None, 'tp', None), P(None, 'tp', None), P('tp', None), P('tp', None, None), P(), P(), P(), P(None, 'tp'), P('tp'), P('tp', None), P(), P('dp', None))
OUT_SPECS = (P('dp', None), P('dp', 'sp', None), P('dp'), P('dp', 'tp', None), P('dp', 'tp', None), P('dp', 'tp', None), P(('dp', 'tp'), None, None), P('dp', 'tp'), P(('dp', 'tp'), None))
LANES = 128
SUB = 8
PER = 2
GELU_C = 0.7978845608028654
GELU_A = 0.044715


def nn(a, b):
    return lax.dot_general(a, b, (((1,), (0,)), ((), ())), preferred_element_type=F32)


def nt(a, b):
    return lax.dot_general(a, b, (((1,), (1,)), ((), ())), preferred_element_type=F32)


def tn(a, b):
    return lax.dot_general(a, b, (((0,), (0,)), ((), ())), preferred_element_type=F32)


def hi_lo(a):
    hi = a.astype(BF16)
    return hi, (a - hi.astype(F32)).astype(BF16)


def iota(shape, dim):
    return lax.broadcasted_iota(jnp.int32, shape, dim)


def by_head(parts, width):
    rows, cols = parts[0].shape[0], len(parts) * width
    block = iota((rows, cols), 1) // width
    out = jnp.zeros((rows, cols), F32)
    for h, part in enumerate(parts):
        out = jnp.where(block == h, part, out)
    return out


def row(ref):
    return ref[...].reshape(1, -1)


def flat(ref):
    heads, width = ref.shape
    wide = jnp.concatenate([ref[...]] * heads, axis=1)
    keep = iota(wide.shape, 0) == iota(wide.shape, 1) // width
    return jnp.sum(jnp.where(keep, wide, 0.0), axis=0, keepdims=True)


def gelu_parts(pre):
    t = jnp.tanh(GELU_C * (pre + GELU_A * pre * pre * pre))
    value = 0.5 * pre * (1.0 + t)
    slope = 0.5 * (1.0 + t) + 0.5 * pre * (1.0 - t * t) * (GELU_C * (1.0 + 3.0 * GELU_A * pre * pre))
    return value, slope


def centre(rows):
    mean = jnp.mean(rows, axis=-1, keepdims=True)
    centred = rows - mean
    inv = lax.rsqrt(jnp.mean(centred * centred, axis=-1, keepdims=True) + NORM_EPS)
    return centred * inv, inv, mean


def norm_back(hat, inv, cot):
    return inv * (cot - jnp.mean(cot, axis=-1, keepdims=True) - hat * jnp.mean(cot * hat, axis=-1, keepdims=True))


def barrier_all(peers):
    sem = pltpu.get_barrier_semaphore()
    for axis, dev in peers:
        pl.semaphore_signal(sem, inc=1, device_id={axis: dev}, device_id_type=MESH)
    pl.semaphore_wait(sem, len(peers))


def peers_of(axis, n):
    me = lax.axis_index(axis)
    return me, [lax.rem(me + k, n) for k in range(1, n)]


def remote(src, dst, send_sem, recv_sem, axis, dev):
    return pltpu.make_async_remote_copy(src_ref=src, dst_ref=dst, send_sem=send_sem, recv_sem=recv_sem, device_id={axis: dev}, device_id_type=MESH)


def gather_start(buf, me, peers, send_sems, recv_sems, axis):
    for k, dev in enumerate(peers):
        remote(buf.at[me], buf.at[me], send_sems.at[k], recv_sems.at[me], axis, dev).start()


def gather_wait(buf, me, peers, send_sems, recv_sems, axis):
    for k, dev in enumerate(peers):
        remote(buf.at[dev], buf.at[dev], send_sems.at[k], recv_sems.at[dev], axis, dev).wait_recv()
    for k, dev in enumerate(peers):
        remote(buf.at[me], buf.at[me], send_sems.at[k], recv_sems.at[me], axis, dev).wait_send()


class ChipRing:
    def __init__(self, nsp):
        me = lax.axis_index('sp')
        self.me, self.core = me, lax.rem(me, 2)
        self.mate = me + 1 - 2 * self.core
        self.up, self.down, self.far = (lax.rem(me + k, nsp) for k in (2, nsp - 2, 4))
        self.mates = [lax.rem(self.mate + k, nsp) for k in (2, nsp - 2, 4)]
        self.around = [self.mate, self.up, self.down, self.far] + self.mates

    def start(self, buf, send, recv):
        for k, dev in enumerate((self.mate, self.up, self.down)):
            remote(buf.at[self.me], buf.at[self.me], send.at[k], recv.at[self.me], 'sp', dev).start()

    def relay(self, buf, send, recv, upward):
        for k, dev in ((3, self.down), (4, self.up)):
            remote(buf.at[dev], buf.at[dev], send.at[k], recv.at[dev], 'sp', dev).wait_recv()
            if upward == (k == 3):
                remote(buf.at[dev], buf.at[dev], send.at[5], recv.at[dev], 'sp', self.up if upward else self.down).start()
            remote(buf.at[dev], buf.at[dev], send.at[k], recv.at[dev], 'sp', self.mate).start()

    def finish(self, buf, send, recv, upward):
        far = self.far
        remote(buf.at[far], buf.at[far], send.at[6], recv.at[far], 'sp', self.mate).wait_recv()
        remote(buf.at[far], buf.at[far], send.at[6], recv.at[far], 'sp', self.mate).start()
        for dev in [self.mate] + self.mates:
            remote(buf.at[dev], buf.at[dev], send.at[0], recv.at[dev], 'sp', self.mate).wait_recv()
        via = self.down if upward else self.up
        for k, slot in ((0, self.me), (1, self.me), (2, self.me), (3, self.down), (4, self.up), (5, via), (6, far)):
            remote(buf.at[slot], buf.at[slot], send.at[k], recv.at[slot], 'sp', self.mate).wait_send()


RING_SEMS = 7


def scan_kernel(heads, scale, x_ref, gain_ref, bias_ref, probe_ref, wq_ref, bq_ref, wk_ref, wv_hbm, bv_ref, pk_ref, hb_ref, qk_ref, q_ref, h_ref, ms_ref, qkr, hball, wv_ref, wv_sem):
    rows = heads * SUB
    width = wq_ref.shape[0] // heads

    load = pltpu.make_async_copy(wv_hbm, wv_ref, wv_sem)

    @pl.when(pl.program_id(0) == 0)
    def _():
        load.start()
        probe8 = jnp.broadcast_to(row(probe_ref), (SUB, probe_ref.shape[0])).astype(BF16)
        q8 = (nt(probe8, wq_ref[...]) + flat(bq_ref)).astype(BF16)
        q_ref[...] = q8.astype(F32)
        qs = jnp.concatenate([q8.astype(F32)] * heads, axis=0)
        qs = jnp.where(iota(qs.shape, 0) // SUB == iota(qs.shape, 1) // width, qs, 0.0).astype(BF16)
        qk = nn(qs, wk_ref[...])
        hi, lo = hi_lo(qk)
        qkr[...] = jnp.zeros(qkr.shape, BF16)
        qkr[0:rows, :] = hi
        qkr[LANES // 2:LANES // 2 + rows, :] = lo
        for h in range(heads):
            qk_ref[h:h + 1, :] = qk[SUB * h:SUB * h + 1, :]

    step = pl.program_id(0)
    block = x_ref.shape[0] // PER
    images, tokens = SUB, block // SUB
    cols = wq_ref.shape[0]
    for j in range(PER):
        at = slice(j * block, j * block + block)
        hat, inv, mean = centre(x_ref[at, :].astype(F32))
        hid = (hat * row(gain_ref) + row(bias_ref)).astype(BF16)
        h_ref[at, :] = hid
        ms_ref[at, :] = jnp.where(iota((block, LANES), 1) == 0, mean, inv)
        r = nt(hid, qkr[...])
        s = ((r + pltpu.roll(r, LANES // 2, 1)) * scale).reshape(images, tokens, LANES)
        m = jnp.max(s, axis=1)
        e = jnp.exp(s - m[:, None, :])
        l = jnp.sum(e, axis=1)
        lane, img = iota(e.shape, 2), iota(e.shape, 0)
        ebd = jnp.where((lane % SUB == img) & (lane < rows), e, 0.0).astype(BF16).reshape(images * tokens, LANES)
        hb = tn(ebd, hid)[0:rows, :]
        hb_ref[j, :, :] = hb
        hball[step * PER + j] = hb
        mine = pl.ds(pl.multiple_of((step * PER + j) * SUB, SUB), SUB)
        pk_ref[mine, cols:cols + LANES] = m
        pk_ref[mine, cols + LANES:cols + 2 * LANES] = l

    @pl.when(step == pl.num_programs(0) - 1)
    def _():
        groups = hball.shape[0]
        every = groups * rows
        load.wait()
        hi, lo = hi_lo(hball[...].reshape(every, hball.shape[2]))
        v = nt(hi, wv_ref[...]) + nt(lo, wv_ref[...])
        bias = flat(bv_ref)
        for g in range(groups):
            vs = by_head([v[g * rows + SUB * h:g * rows + SUB * h + SUB] for h in range(heads)], width)
            tot = pk_ref[g * SUB:g * SUB + SUB, cols + LANES:cols + 2 * LANES]
            pk_ref[g * SUB:g * SUB + SUB, 0:cols] = vs + by_head([tot[:, SUB * h:SUB * h + 1] for h in range(heads)], width) * bias


def scan_tokens(heads, images, scale, x, gain, bias, probe, wq, bq, wk, wv, bv):
    tokens_all, width = x.shape
    hd = wq.shape[0]
    groups = images // SUB
    block = tokens_all // groups * PER
    full = lambda a: pl.BlockSpec(a.shape, lambda g: (0,) * a.ndim)
    return pl.pallas_call(
        functools.partial(scan_kernel, heads, scale),
        grid=(groups // PER,),
        in_specs=[pl.BlockSpec((block, width), lambda g: (g, 0))] + [full(a) for a in (gain, bias, probe, wq, bq, wk)] + [pl.BlockSpec(memory_space=pl.ANY), full(bv)],
        out_specs=[pl.BlockSpec((images, hd + 2 * LANES), lambda g: (0, 0)), pl.BlockSpec((PER, heads * SUB, width), lambda g: (g, 0, 0)), pl.BlockSpec((heads, width), lambda g: (0, 0)), pl.BlockSpec((SUB, hd), lambda g: (0, 0)), pl.BlockSpec((block, width), lambda g: (g, 0)), pl.BlockSpec((block, LANES), lambda g: (g, 0))],
        out_shape=[jax.ShapeDtypeStruct((images, hd + 2 * LANES), F32), jax.ShapeDtypeStruct((groups, heads * SUB, width), F32), jax.ShapeDtypeStruct((heads, width), F32), jax.ShapeDtypeStruct((SUB, hd), F32), jax.ShapeDtypeStruct(x.shape, BF16), jax.ShapeDtypeStruct((tokens_all, LANES), F32)],
        scratch_shapes=[pltpu.VMEM((LANES, width), BF16), pltpu.VMEM((groups, heads * SUB, width), F32), pltpu.VMEM(wv.shape, BF16), pltpu.SemaphoreType.DMA(())],
        name='scan_tokens',
    )(x, gain, bias, probe, wq, bq, wk, wv, bv)


def middle_kernel(heads, nsp, ntp, scale, pk_ref, og_ref, qk_ref, bo_ref, hg_ref, hb_ref, bu_ref, bd_ref, bv_ref, hb_hbm, x_hbm, wo_hbm, wu_hbm, wd_hbm, wv_hbm, wk_hbm, wq_hbm,
                  gv_out, hbar_out, st_out, qk_out, gp_out, y_out, ga_out, pool_out, pb_out, hid_out, gpre_out, u_out, gq_out, gpr_out,
                  wo, wu, wd, wv, wk, wq, rbuf, ta, tg, td, ag, hr, relay, pa, ha, sg, xb, rhs, uacc, ub, prb, ghb,
                  wsem, xsem, rs_send, rs_recv, ta_s, ta_r, tg_s, tg_r, td_s, td_r, ag_s, ag_r, hr_s, hr_r, rl_r, gv_s, gv_r, fw_s, fw_r, pa_s, pa_r, ha_s, ha_r, st_s, st_r, qk_s, qk_r, ub_s, ub_r, pr_s, pr_r, sy_s, sy_r, sg_s, sg_r):
    sp, sp_peers = peers_of('sp', nsp)
    tp, tp_peers = peers_of('tp', ntp)
    ring = ChipRing(nsp)
    core, mate = ring.core, ring.mate
    loads = [pltpu.make_async_copy(a, b, wsem.at[i]) for i, (a, b) in enumerate(((wd_hbm, wd), (wo_hbm, wo), (wu_hbm, wu), (hb_hbm.at[sp], hr.at[sp]), (wv_hbm, wv), (wk_hbm, wk), (wq_hbm, wq)))]
    for load in loads:
        load.start()
    sem = pltpu.get_barrier_semaphore()
    for axis, devs in (('sp', sp_peers), ('tp', tp_peers)):
        for dev in devs:
            pl.semaphore_signal(sem, inc=1, device_id={axis: dev}, device_id_type=MESH)

    def x_load(g):
        return pltpu.make_async_copy(x_hbm.at[g], xb.at[g % 2], xsem.at[g % 2])

    x_load(0).start()
    x_load(1).start()
    hd = wo.shape[0]
    width = hd // heads
    model = wu.shape[0]
    rows = heads * SUB
    images = nsp * SUB
    qk_out[tp] = qk_ref[...]
    rbuf[sp] = pk_ref[sp]
    for h in range(heads):
        hi, lo = hi_lo(jnp.broadcast_to(qk_ref[h:h + 1, :], (SUB, model)))
        rhs[h * SUB:h * SUB + SUB, :] = hi.astype(F32)
        rhs[2 * rows + h * SUB:2 * rows + h * SUB + SUB, :] = lo.astype(F32)
    og = og_ref[sp]
    pl.semaphore_wait(sem, len(sp_peers) + len(tp_peers))

    sends = []
    for k, dev in enumerate(sp_peers):
        sends.append(remote(pk_ref.at[dev], rbuf.at[sp], rs_send.at[k], rs_recv.at[sp], 'sp', dev))
        sends[-1].start()
    far0, far1 = ring.far - core, ring.far - core + 1
    late = [remote(hb_hbm.at[far0], relay.at[0], hr_s.at[0], rl_r.at[0], 'sp', ring.up), remote(hb_hbm.at[far1], relay.at[1], hr_s.at[1], rl_r.at[1], 'sp', ring.down)]
    for k, dev in enumerate((ring.up, ring.down, ring.mates[0], ring.mates[1], mate)):
        late.append(remote(hb_hbm.at[dev], hr.at[sp], hr_s.at[2 + k], hr_r.at[sp], 'sp', dev))
    for send in late:
        send.start()
    gather_start(qk_out, tp, tp_peers, qk_s, qk_r, 'tp')
    loads[0].wait()
    gh = nt(og, wd[...])
    for k, dev in enumerate(sp_peers):
        remote(rbuf.at[dev], rbuf.at[dev], rs_send.at[k], rs_recv.at[dev], 'sp', dev).wait_recv()
    for send in sends:
        send.wait_send()
    m = rbuf[0, :, hd:hd + LANES]
    for j in range(1, nsp):
        m = jnp.maximum(m, rbuf[j, :, hd:hd + LANES])
    l = jnp.zeros_like(m)
    v = jnp.zeros((SUB, hd), F32)
    for j in range(nsp):
        w = jnp.exp(rbuf[j, :, hd:hd + LANES] - m)
        l = l + w * rbuf[j, :, hd + LANES:hd + 2 * LANES]
        v = v + by_head([w[:, SUB * h:SUB * h + 1] for h in range(heads)], width) * rbuf[j, :, 0:hd]
    o = v / by_head([l[:, SUB * h:SUB * h + 1] for h in range(heads)], width)
    pooled_bf = o.astype(BF16)
    lse = m + jnp.log(l)

    loads[1].wait()
    ta[tp] = nn(pooled_bf, wo[...])
    gather_start(ta, tp, tp_peers, ta_s, ta_r, 'tp')
    for k, (src, dst) in enumerate(((ring.down, ring.up - core), (ring.up, ring.down - core + 1))):
        remote(relay.at[k], relay.at[k], hr_s.at[k], rl_r.at[k], 'sp', src).wait_recv()
        late.append(remote(relay.at[k], hr.at[src], hr_s.at[7 + k], hr_r.at[src], 'sp', dst))
        late[-1].start()
    loads[2].wait()
    gather_wait(ta, tp, tp_peers, ta_s, ta_r, 'tp')
    attn = ta[0]
    for t in range(1, ntp):
        attn = attn + ta[t]
    attn = attn + row(bo_ref)
    hat, inv, _ = centre(attn)
    gain = row(hg_ref)
    y = (hat * gain + row(hb_ref)).astype(BF16)
    value, slope = gelu_parts(nn(y, wu[...]) + row(bu_ref))
    tg[tp] = nt((gh * slope).astype(BF16), wu[...])
    gather_start(tg, tp, tp_peers, tg_s, tg_r, 'tp')
    td[tp] = nn(value.astype(BF16), wd[...])
    gather_start(td, tp, tp_peers, td_s, td_r, 'tp')
    gather_wait(tg, tp, tp_peers, tg_s, tg_r, 'tp')
    gno = tg[0]
    for t in range(1, ntp):
        gno = gno + tg[t]
    ga = (og.astype(F32) + norm_back(hat, inv, gno * gain)).astype(BF16)
    gp = nt(ga, wo[...]).astype(BF16).astype(F32)
    prod = gp * (o - flat(bv_ref))
    head_of = iota(prod.shape, 1) // width
    delta = by_head([jnp.sum(jnp.where(head_of == h, prod, 0.0), axis=1, keepdims=True) for h in range(heads)], SUB)
    ag[sp, :, 0:hd] = gp
    ag[sp, :, hd:hd + LANES] = jnp.concatenate([lse[:, 0:rows], delta, jnp.zeros((SUB, LANES - 2 * rows), F32)], axis=1)
    gather_start(ag, sp, sp_peers, ag_s, ag_r, 'sp')

    gather_wait(td, tp, tp_peers, td_s, td_r, 'tp')
    down = td[0]
    for t in range(1, ntp):
        down = down + td[t]
    pa[sp, :, 0:model] = y.astype(F32)
    pa[sp, :, model:2 * model] = (attn + down + row(bd_ref)).astype(BF16).astype(F32)
    pa[sp, :, 2 * model:3 * model] = ga.astype(F32)
    pa[sp, :, 3 * model:3 * model + hd] = pooled_bf.astype(F32)
    gather_wait(ag, sp, sp_peers, ag_s, ag_r, 'sp')
    ring.start(pa, pa_s, pa_r)

    loads[4].wait()
    st_out[tp] = ag[:, :, hd:hd + LANES]
    near_up, near_down, far_tp = lax.rem(tp + 1, ntp), lax.rem(tp + ntp - 1, ntp), lax.rem(tp + 2, ntp)
    half = nsp // 2
    direct = half - sg.shape[2]
    gp_out[...] = ag[:, :, 0:hd].astype(BF16)

    def make_gv(first):
        part = jnp.concatenate([ag[first + i, :, 0:hd] for i in range(half) for _ in range(heads)], axis=0)
        keep = (iota(part.shape, 0) // SUB) % heads == iota(part.shape, 1) // width
        gv_out[tp, pl.ds(first, half)] = nn(jnp.where(keep, part, 0.0).astype(BF16), wv[...]).reshape(half, rows, model)

    def piece(i, owner):
        return gv_out.at[owner, core * half + i]

    def send_gv(i, k, owner, dev):
        return remote(piece(i, owner), piece(i, owner), gv_s.at[k, i], gv_r.at[owner, i], 'tp', dev)

    def forward(i, k, owner):
        return remote(piece(i, owner), piece(i, owner), fw_s.at[k, i], fw_r.at[owner, i], 'sp', mate)

    def near(i):
        for k, owner in ((0, near_down), (1, near_up)):
            send_gv(i, k, owner, owner).wait_recv()
            if k == i % 2:
                send_gv(i, 2, owner, near_down if k else near_up).start()
            forward(i, k, owner).start()

    def beyond(i):
        send_gv(i, 2, far_tp, far_tp).wait_recv()
        forward(i, 2, far_tp).start()

    def send_shared(k):
        block = pl.ds(pl.multiple_of((sp // 2) * SUB, SUB), SUB)
        return remote(gv_out.at[tp, pl.ds(core * half + direct, half - direct), block], sg.at[sp, ntp - 1 - k], sy_s.at[k - 1], sy_r.at[ntp - 1 - k], 'tp', lax.rem(tp + k, ntp))

    make_gv(core * half)
    for k in range(1, ntp):
        send_shared(k).start()
    for i in range(direct):
        send_gv(i, 0, tp, near_up).start()
        send_gv(i, 1, tp, near_down).start()
        if i == 0:
            gather_start(st_out, tp, tp_peers, st_s, st_r, 'tp')
    make_gv((1 - core) * half)
    loads[3].wait()
    for k, dev in enumerate(sp_peers):
        remote(hr.at[dev], hr.at[dev], hr_s.at[k], hr_r.at[dev], 'sp', dev).wait_recv()
    for send in late:
        send.wait_send()
    hbar = jnp.zeros(hr.shape[1:], F32)
    for j in range(nsp):
        w = jnp.exp(rbuf[j, :, hd:hd + LANES] - lse)
        hbar = hbar + hr[j] * jnp.concatenate([w[:, SUB * h:SUB * h + 1] for h in range(heads)], axis=0)
    ha[sp] = hbar
    ring.start(ha, ha_s, ha_r)

    uacc[...] = jnp.zeros(uacc.shape, F32)

    def u_step(g):
        x_load(g).wait()
        tokens = xb.shape[1] // SUB
        hidden = xb[g % 2]
        hi, lo = hi_lo(gv_out[tp, g])
        rhs[rows:2 * rows, :] = hi.astype(F32)
        rhs[3 * rows:4 * rows, :] = lo.astype(F32)
        r = nt(hidden, rhs[...].astype(BF16))
        r = (r + pltpu.roll(r, LANES // 2, 1)).reshape(SUB, tokens, LANES)
        lane, img = iota(r.shape, 2), iota(r.shape, 0)
        r = r * jnp.where(lane < rows, scale, 1.0) - ag[g, :, hd:hd + LANES][:, None, :]
        r = r.reshape(SUB * tokens, LANES)
        grad = (jnp.exp(r) * pltpu.roll(r, LANES - rows, 1) * scale).reshape(SUB, tokens, LANES)
        ds = jnp.where((lane % SUB == img) & (lane < rows), grad, 0.0).astype(BF16).reshape(SUB * tokens, LANES)
        uacc[...] += tn(ds, hidden)[0:rows, :]
        if g + 2 < nsp:
            x_load(g + 2).start()

    u_step(0)
    u_step(1)
    u_step(2)
    ring.relay(pa, pa_s, pa_r, False)
    for k in range(1, ntp):
        remote(sg.at[sp, k - 1], sg.at[sp, k - 1], sy_s.at[0], sy_r.at[k - 1], 'tp', near_up).wait_recv()
    ring.start(sg, sg_s, sg_r)
    u_step(3)
    u_step(4)
    near(0)
    u_step(5)
    u_step(6)
    ring.finish(pa, pa_s, pa_r, False)
    ring.relay(ha, ha_s, ha_r, True)
    u_step(7)
    for h in range(heads):
        ub[sp, h:h + 1, :] = jnp.sum(uacc[SUB * h:SUB * h + SUB, :], axis=0, keepdims=True)
    gather_start(ub, sp, sp_peers, ub_s, ub_r, 'sp')

    near(1)
    ghb[...] = nt(og_ref[...].reshape(images, model), wd[...])
    y_all = pa[:, :, 0:model].astype(BF16)
    y_out[...] = y_all
    pool_out[...] = pa[:, :, model:2 * model].astype(BF16)
    ga_out[...] = pa[:, :, 2 * model:3 * model].astype(BF16)
    pb_out[...] = pa[:, :, 3 * model:3 * model + hd].astype(BF16)
    value, slope = gelu_parts(nn(y_all.reshape(images, model), wu[...]) + row(bu_ref))
    gpre_out[...] = (ghb[...] * slope).astype(BF16)
    hid_out[...] = value.astype(BF16)
    ring.relay(sg, sg_s, sg_r, False)
    near(2)

    gather_wait(ub, sp, sp_peers, ub_s, ub_r, 'sp')
    u = ub[0]
    for j in range(1, nsp):
        u = u + ub[j]
    u_out[...] = u
    loads[5].wait()
    loads[6].wait()
    hi, lo = hi_lo(u)
    gq = nt(jnp.concatenate([hi, lo], axis=0), wk[...])
    gq = gq[0:heads] + gq[heads:2 * heads]
    gq = jnp.sum(jnp.where(iota(gq.shape, 0) == iota(gq.shape, 1) // width, gq, 0.0), axis=0, keepdims=True)
    gq_out[...] = gq
    hi, lo = hi_lo(gq)
    gpr = nn(jnp.concatenate([hi, lo], axis=0), wq[...])
    prb[tp] = gpr[0:1] + gpr[1:2]
    gather_start(prb, tp, tp_peers, pr_s, pr_r, 'tp')
    beyond(0)
    ring.finish(ha, ha_s, ha_r, True)
    hbar_out[...] = ha[...].astype(BF16)
    beyond(1)
    ring.finish(sg, sg_s, sg_r, False)
    for j in range(nsp):
        for k in range(1, ntp):
            gv_out[lax.rem(tp + k, ntp), (j % 2) * half + direct:(j % 2) * half + half, (j // 2) * SUB:(j // 2) * SUB + SUB, :] = sg[j, k - 1]
    beyond(2)
    for k in range(1, ntp):
        send_shared(k).wait_send()
    for i in range(direct):
        other = (1 - core) * half + i
        for k, (owner, dev) in enumerate(((tp, near_up), (tp, near_down), (near_up if i % 2 else near_down, near_down if i % 2 else near_up))):
            send_gv(i, k, owner, dev).wait_send()
        for k, owner in enumerate((near_down, near_up, far_tp)):
            forward(i, k, owner).wait_send()
            remote(gv_out.at[owner, other], gv_out.at[owner, other], fw_s.at[k, i], fw_r.at[owner, i], 'sp', mate).wait_recv()
    gather_wait(st_out, tp, tp_peers, st_s, st_r, 'tp')
    gather_wait(qk_out, tp, tp_peers, qk_s, qk_r, 'tp')
    gather_wait(prb, tp, tp_peers, pr_s, pr_r, 'tp')
    total = prb[0]
    for t in range(1, ntp):
        total = total + prb[t]
    gpr_out[...] = total


def middle(heads, nsp, ntp, scale, pk, og3, qk, vectors, hb, x3, wo, wu, wd, wv, wk, wq):
    own, model = og3.shape[1:]
    hd = wo.shape[0]
    rows = hb.shape[1]
    images = nsp * own
    half = nsp // 2
    pk3 = pk.reshape(nsp, own, pk.shape[1])
    vm, hbm = pl.BlockSpec(memory_space=pltpu.VMEM), pl.BlockSpec(memory_space=pl.ANY)
    dma = pltpu.SemaphoreType.DMA
    sds = jax.ShapeDtypeStruct
    part = pltpu.VMEM((ntp, own, model), F32)
    wide = [pltpu.VMEM(w.shape, BF16) for w in (wo, wu, wd, wv, wk, wq)]
    ring, tps, tpr = [dma((RING_SEMS,)), dma((nsp,))], dma((ntp - 1,)), dma((ntp,))
    return pl.pallas_call(
        functools.partial(middle_kernel, heads, nsp, ntp, scale),
        in_specs=[vm] * 9 + [hbm] * 8,
        out_specs=[vm] * 14,
        out_shape=[pltpu.VMEM((ntp, nsp, rows, model), F32), sds((nsp, rows, model), BF16), sds((ntp, nsp, own, LANES), F32), sds((ntp,) + qk.shape, F32), sds((nsp, own, hd), BF16),
                   sds((nsp, own, model), BF16), sds((nsp, own, model), BF16), sds((nsp, own, model), BF16), sds((nsp, own, hd), BF16), sds((images, model), BF16), sds((images, model), BF16), sds(qk.shape, F32), sds((1, hd), F32), sds((1, model), F32)],
        scratch_shapes=wide + [pltpu.VMEM(pk3.shape, F32), part, part, part, pltpu.VMEM((nsp, own, hd + LANES), F32), pltpu.VMEM(hb.shape, F32), pltpu.VMEM((2,) + hb.shape[1:], F32), pltpu.VMEM((nsp, own, 3 * model + hd), F32), pltpu.VMEM(hb.shape, F32), pltpu.VMEM((nsp, ntp - 1, 1, own, model), F32),
                               pltpu.VMEM((2,) + x3.shape[1:], BF16), pltpu.VMEM((LANES, model), F32), pltpu.VMEM((rows, model), F32), pltpu.VMEM((nsp,) + qk.shape, F32), pltpu.VMEM((ntp, 1, model), F32), pltpu.VMEM((images, model), F32),
                               dma((7,)), dma((2,)), dma((nsp - 1,)), dma((nsp,)), tps, tpr, tps, tpr, tps, tpr, dma((nsp - 1,)), dma((nsp,))] + [dma((9,)), dma((nsp,)), dma((2,)), dma((3, half)), dma((ntp, half)), dma((3, half)), dma((ntp, half))] + ring + ring + [tps, tpr, tps, tpr, dma((nsp - 1,)), dma((nsp,)), tps, tpr, tps, tpr] + ring,
        compiler_params=pltpu.CompilerParams(collective_id=0, has_side_effects=True, vmem_limit_bytes=57 << 20),
        name='middle',
    )(pk3, og3, qk, *vectors, hb, x3, wo, wu, wd, wv, wk, wq)


def products_kernel(heads, parts, y_ref, gpre_ref, hid_ref, og_ref, pb_ref, ga_ref, gp_ref, hbar_ref, q_ref, u_ref, gq_ref, probe_ref, pool_ref, gpr_ref, gup_ref, gdown_ref, gwo_ref, gwv_ref, gwk_ref, gwq_ref, pool_out, gpr_out):
    step = pl.program_id(0)
    gup_ref[...] = tn(y_ref[...], gpre_ref[...])
    gdown_ref[...] = tn(hid_ref[...], og_ref[...])
    tile, model = gwo_ref.shape
    width = parts * tile // heads
    part = lax.rem(step, parts)
    groups = gp_ref.shape[0]

    @pl.when(step == 0)
    def _():
        pool_out[...] = pool_ref[...]
        gpr_out[...] = gpr_ref[...].reshape(gpr_out.shape)

    @pl.when(step < parts)
    def _():
        gwo_ref[...] = tn(pb_ref[...], ga_ref[...])
        gp = jnp.concatenate([gp_ref[g].astype(F32) for g in range(groups) for _ in range(heads)], axis=0)
        keep = (iota(gp.shape, 0) // SUB) % heads == (part * tile + iota(gp.shape, 1)) // width
        gwv_ref[...] = tn(jnp.where(keep, gp, 0.0).astype(BF16), hbar_ref[...].reshape(gp.shape[0], model))

    @pl.when(step >= parts)
    def _():
        q = jnp.transpose(q_ref[...])[:, 0:1]
        head_of = (part * tile + iota((tile, model), 0)) // width
        u = jnp.zeros((tile, model), F32)
        for h in range(heads):
            u = jnp.where(head_of == h, u_ref[h:h + 1, :], u)
        gwk_ref[...] = q * u
        gq = jnp.transpose(jnp.broadcast_to(gq_ref[...], (SUB, tile)))[:, 0:1]
        gwq_ref[...] = gq * row(probe_ref)


def products(heads, y, gpre, hid, og, pb, ga, gp3, hbar, q8, u, gq, probe, pool, gpr):
    images, model = y.shape
    cols, hd = gpre.shape[1], pb.shape[1]
    parts = hd // LANES
    steps = 2 * parts
    tile = model // steps
    at = lambda a: lambda i: jnp.clip(i - parts * a, 0, parts - 1)
    lane = lambda i: lax.rem(i, parts)
    part = pl.BlockSpec((images, tile), lambda i: (0, i))
    full = lambda a: pl.BlockSpec(a.shape, lambda i: (0,) * a.ndim)
    out = pl.BlockSpec((tile, cols), lambda i: (i, 0))
    small = [pl.BlockSpec((LANES, model), lambda i, f=at(a): (f(i), 0)) for a in (0, 0, 1, 1)]
    sds = jax.ShapeDtypeStruct
    return pl.pallas_call(
        functools.partial(products_kernel, heads, parts),
        grid=(steps,),
        in_specs=[part, full(gpre), part, full(og), pl.BlockSpec((images, LANES), lambda i: (0, lane(i))), full(ga), pl.BlockSpec(gp3.shape[:2] + (LANES,), lambda i: (0, 0, lane(i))), full(hbar), pl.BlockSpec((SUB, LANES), lambda i: (0, lane(i))), full(u), pl.BlockSpec((1, LANES), lambda i: (0, lane(i))), full(probe), full(pool), full(gpr)],
        out_specs=[out, out] + small + [full(pool), full(probe)],
        out_shape=[sds((model, cols), F32), sds((cols, model), F32)] + [sds((hd, model), F32)] * 4 + [sds(pool.shape, pool.dtype), sds(probe.shape, F32)],
        name='products',
    )(y, gpre, hid, og, pb, ga, gp3, hbar, q8, u, gq, probe, pool, gpr)


def back_kernel(heads, ntp, scale, x_ref, h_ref, ms_ref, gain_ref, gv_ref, qk_ref, st_ref, gx_ref, qkr):
    step = pl.program_id(0)
    rows = heads * SUB
    model = x_ref.shape[1]

    @pl.when(step == 0)
    def _():
        for t in range(ntp):
            for h in range(heads):
                hi, lo = hi_lo(jnp.broadcast_to(qk_ref[t, h:h + 1, :], (SUB, model)))
                at = (t * heads + h) * SUB
                qkr[at:at + SUB, :] = hi.astype(F32)
                qkr[LANES + at:LANES + at + SUB, :] = lo.astype(F32)

    block = x_ref.shape[0] // PER
    images, tokens = SUB, block // SUB
    gain = row(gain_ref)
    qkb = qkr[...].astype(BF16)
    for j in range(PER):
        at = slice(j * block, j * block + block)
        hid = h_ref[at, :]
        gv_hi, gv_lo = hi_lo(jnp.concatenate([gv_ref[t, step * PER + j] for t in range(ntp)], axis=0))
        r = nt(hid, qkb)
        s = (r[:, 0:LANES] + r[:, LANES:2 * LANES]) * scale
        d = nt(hid, jnp.concatenate([gv_hi, gv_lo], axis=0))
        d = d[:, 0:LANES] + d[:, LANES:2 * LANES]
        lse = jnp.concatenate([st_ref[t, j, :, 0:rows] for t in range(ntp)], axis=1)
        delta = jnp.concatenate([st_ref[t, j, :, rows:2 * rows] for t in range(ntp)], axis=1)
        shape = (images, tokens, LANES)
        keep = iota(shape, 2) % SUB == iota(shape, 0)
        p = jnp.where(keep, jnp.exp(s.reshape(shape) - lse[:, None, :]), 0.0)
        ds = p * (d.reshape(shape) - delta[:, None, :]) * scale
        pb = p.astype(BF16).reshape(images * tokens, LANES)
        db = ds.astype(BF16).reshape(images * tokens, LANES)
        gh = nn(jnp.concatenate([pb, db], axis=1), jnp.concatenate([gv_hi, qkb[0:LANES]], axis=0))
        inv = ms_ref[at, 1:2]
        hat = (x_ref[at, :].astype(F32) - ms_ref[at, 0:1]) * inv
        gx_ref[at, :] = norm_back(hat, inv, gh * gain).astype(BF16)


def back_tokens(heads, ntp, scale, x, h, ms, gain, gv, qk, st):
    tokens_all, model = x.shape
    groups, rows = gv.shape[1], gv.shape[2]
    block = tokens_all // groups * PER
    full = lambda a: pl.BlockSpec(a.shape, lambda g: (0,) * a.ndim)
    return pl.pallas_call(
        functools.partial(back_kernel, heads, ntp, scale),
        grid=(groups // PER,),
        in_specs=[pl.BlockSpec((block, model), lambda g: (g, 0)), pl.BlockSpec((block, model), lambda g: (g, 0)), pl.BlockSpec((block, LANES), lambda g: (g, 0)), full(gain), pl.BlockSpec(memory_space=pltpu.VMEM), full(qk), pl.BlockSpec((ntp, PER) + st.shape[2:], lambda g: (0, g, 0, 0))],
        out_specs=pl.BlockSpec((block, model), lambda g: (g, 0)),
        out_shape=jax.ShapeDtypeStruct((tokens_all, model), BF16),
        scratch_shapes=[pltpu.VMEM((2 * LANES, model), F32)],
        compiler_params=pltpu.CompilerParams(vmem_limit_bytes=57 << 20),
        name='back_tokens',
    )(x, h, ms, gain, gv, qk, st)


def local_head(nsp, ntp, encoded, enc_gain, enc_bias, probe, w_query, b_query, w_key, w_value, b_value, w_out, b_out, head_gain, head_bias, w_up, b_up, w_down, b_down, out_grad):
    images, tokens, model = encoded.shape
    heads, head_dim = b_query.shape
    hd = heads * head_dim
    scale = head_dim ** -0.5
    x = encoded.reshape(images * tokens, model)
    wq, wk, wv = (jnp.transpose(w, (1, 2, 0)).reshape(hd, model) for w in (w_query, w_key, w_value))
    wo = w_out.reshape(hd, model)
    og3 = out_grad.reshape(nsp, images // nsp, model)
    pk, hb, qk, q8, h, ms = scan_tokens(heads, images, scale, x, enc_gain, enc_bias, probe, wq, b_query, wk, wv, b_value)
    gv, hbar, st, qk_all, gp3, y3, ga3, pool3, pb3, hidden, grad_pre, u, gq, gpr = middle(heads, nsp, ntp, scale, pk, og3, qk, (b_out, head_gain, head_bias, b_up, b_down, b_value), hb, h.reshape(nsp, -1, model), wo, w_up, w_down, wv, wk, wq)
    gv = pltpu.with_memory_space_constraint(gv, pltpu.VMEM)
    gx = back_tokens(heads, ntp, scale, x, h, ms, enc_gain, gv, qk_all, st)
    y, ga, pool, pooled_bf = (a.reshape(images, -1) for a in (y3, ga3, pool3, pb3))
    grad_w_up, grad_w_down, *small, pooled, grad_probe = products(heads, y, grad_pre, hidden, out_grad, pooled_bf, ga, gp3, hbar, q8, u, gq, probe, pool, gpr)
    grad_w_out, grad_wv, grad_wk, grad_wq = (a.reshape(heads, head_dim, model) for a in small)
    back = lambda a: jnp.transpose(a, (2, 0, 1))
    return (pooled, gx.reshape(encoded.shape), grad_probe, back(grad_wq), back(grad_wk), back(grad_wv), grad_w_out, grad_w_up, grad_w_down)


def solution(mesh):
    body = functools.partial(local_head, mesh.shape['sp'], mesh.shape['tp'])
    return jax.shard_map(body, mesh=mesh, in_specs=IN_SPECS, out_specs=OUT_SPECS, check_vma=False)
```
